512 devices in a mesh: cls: 8 (over y_hi, core), img: 64 (over y_lo, z, x).
Axes of the slice: x: 4, y: 8 (y_hi: 4, y_lo: 2; y = y_hi * 2 + y_lo), z: 8, core: 2. Of those that a mesh axis runs over, the one named last changes fastest.
Arguments:
- images: bfloat16 [28672, 7200], P(('cls', 'img')), may hold values from -8 to 8
- projections: bfloat16 [1024, 7200], P('cls'), may hold values from -0.42426407 to 0.42426407
- noise_power: float32 [32, 7200], replicated, may hold values from 0.5 to 4
- class_logprior: float32 [4], replicated, may hold values from -1.5 to 1.5
- groups: int32 [28672], P(('cls', 'img')), may hold values from 0 to 31
- offsets: int32 [28672], P(('cls', 'img')), may hold values from 0 to 3
Outputs:
- weighted_sums: float32 [1024, 7200], P(('cls', 'img'))
- log_evidence: float32 [28672], P(('cls', 'img'))
The draws below stay inside these ranges and needn't reach their ends.
All inputs are finite; a program needn't handle non-finite values.
Results may differ from the reference program's by a relative error of at most 0.0064.
Values may be sent and summed in bfloat16 or wider, within the bound.
A program may use at most 64 MiB of HBM per device.

```python
import math
import jax
import jax.numpy as jnp
from jax import lax

F = 7200
CLASSES = 4
GROUPS = 32
IMG_DEV = 56
PROJS = 1024
IMAGES = 28672
N_CLS = 8


aligned_pairs = 8


mean_inverse = 1.75 / math.log(8.0)


def shared_layout(key):
    layout_key = jax.random.fold_in(key, 911)
    pair_order = jax.random.permutation(jax.random.fold_in(layout_key, 1), PROJS // 2)
    image_order = jax.random.permutation(jax.random.fold_in(layout_key, 2), IMAGES)
    first_rows = 2 * pair_order[:aligned_pairs]
    return (first_rows, first_rows + 1, image_order[:aligned_pairs])


def base_rows(key):
    base_key = jax.random.fold_in(key, 913)
    values = jnp.clip(jax.random.normal(base_key, (PROJS, F), jnp.float32), -6.0, 6.0)
    return values


def drawn_base(key):
    return jax.random.uniform(jax.random.fold_in(key, 917), (aligned_pairs, F), jnp.float32, -math.sqrt(3.0), math.sqrt(3.0))


def targets():
    return 200.0 + 60.0 * (jnp.arange(aligned_pairs) % 4).astype(jnp.float32)


def projection_level():
    return 18.0 / math.sqrt(F)


def image_level():
    level = projection_level()
    return (targets() + 0.5 * level * level * F * mean_inverse) / (level * F * mean_inverse)


def draw_projections(key, part):
    values = base_rows(key)
    row_scale = jnp.exp(jax.random.uniform(jax.random.fold_in(key, 914), (PROJS,), jnp.float32, math.log(0.5), math.log(2.0)))
    result = 3.0 * row_scale[:, None] * values / math.sqrt(F)
    first_rows, second_rows, image_rows = shared_layout(key)
    shared = drawn_base(key)
    level = projection_level()
    half_quadratic = 0.5 * level * level * F * mean_inverse
    epsilon = 2.0 / (targets() - half_quadratic)
    result = result.at[first_rows].set(level * shared)
    result = result.at[second_rows].set(level * (1.0 - epsilon)[:, None] * shared)
    return result.astype(jnp.bfloat16)


def draw_images(key, part):
    image_key = jax.random.fold_in(key, 915)
    values = jnp.clip(jax.random.normal(image_key, (IMAGES, F), jnp.float32), -6.0, 6.0)
    first_rows, second_rows, image_rows = shared_layout(key)
    shared = drawn_base(key)
    values = values.at[image_rows].set(image_level()[:, None] * shared)
    return values.astype(jnp.bfloat16)


def touch_ends(values, stream_key, smallest, high):
    spot = [jax.random.randint(jax.random.fold_in(stream_key, axis), (), 0, length) for axis, length in enumerate(values.shape)]
    longest = values.shape.index(max(values.shape))
    next_to = spot[:longest] + [(spot[longest] + 1) % values.shape[longest]] + spot[longest + 1:]
    return values.at[tuple(spot)].set(smallest).at[tuple(next_to)].set(high)


def setup_inputs(seed: int = 0) -> dict:
    keys = jax.random.split(jax.random.key(seed), 7)
    images = draw_images(jax.random.fold_in(keys[6], 71), 0)
    projections = draw_projections(jax.random.fold_in(keys[6], 71), 0)
    noise_power = jnp.clip(jnp.exp(jax.random.uniform(keys[2], (GROUPS, F), jnp.float32, math.log(0.5), math.log(4.0))), 0.5, 4.0)
    class_logprior = jnp.clip(jax.random.uniform(keys[3], (CLASSES,), jnp.float32, -1.5, 1.5), -1.5, 1.5)
    groups = touch_ends(jax.random.randint(keys[4], (IMAGES,), 0, GROUPS), jax.random.fold_in(keys[4], 1), 0, GROUPS - 1).astype(jnp.int32)
    offsets = touch_ends(jax.random.randint(keys[5], (IMAGES,), 0, CLASSES), jax.random.fold_in(keys[5], 1), 0, CLASSES - 1).astype(jnp.int32)
    return {"images": images, "projections": projections, "noise_power": noise_power, "class_logprior": class_logprior, "groups": groups, "offsets": offsets}


def reference(images, projections, noise_power, class_logprior, groups, offsets):
    inverse = 1.0 / noise_power
    whitened = (images.astype(jnp.float32) * inverse[groups]).astype(jnp.bfloat16)
    proj_float = projections.astype(jnp.float32)
    quadratic = jnp.dot(inverse, (proj_float * proj_float).T, precision=lax.Precision.HIGHEST)
    per_class = PROJS // CLASSES
    class_of = jnp.arange(PROJS, dtype=jnp.int32) // per_class
    class_shift = (class_of[None, :] - jnp.arange(CLASSES, dtype=jnp.int32)[:, None]) % CLASSES
    prior_table = class_logprior[class_shift]
    block_rows = IMG_DEV * N_CLS
    blocks = IMAGES // block_rows
    white_blocks = whitened.reshape(blocks, block_rows, F)
    group_blocks = groups.reshape(blocks, block_rows)
    offset_blocks = offsets.reshape(blocks, block_rows)

    def one_block(summed, inputs):
        batch_rows, group_ids, offset_ids = inputs
        scores = jnp.dot(batch_rows, projections.T, preferred_element_type=jnp.float32)
        scores = scores + (-0.5 * quadratic[group_ids] + prior_table[offset_ids])
        peak = jnp.max(scores, axis=1)
        evidence = peak + jnp.log(jnp.sum(jnp.exp(scores - peak[:, None]), axis=1))
        posterior = jnp.exp(scores - evidence[:, None]).astype(jnp.bfloat16)
        summed = summed + jnp.einsum("bp,bf->pf", posterior.astype(jnp.float32), batch_rows.astype(jnp.float32))
        return summed, evidence

    start_sums = jnp.zeros((PROJS, F), jnp.float32)
    weighted_sums, evidence = lax.scan(one_block, start_sums, (white_blocks, group_blocks, offset_blocks))
    return weighted_sums, evidence.reshape(IMAGES)
```

```python
import jax
import jax.numpy as jnp
from jax import lax
from jax.experimental import pallas as pl
from jax.experimental.pallas import tpu as pltpu
from jax.sharding import PartitionSpec as P

NX, NY, NZ = 4, 8, 8
F = 7200
W = 1920
TAG = 128
ROWS = 56
BLOCK = 128
CHUNKS = 4
CHUNK = BLOCK // CHUNKS
WA = 1024
WB = W - WA
GROUPS = 32
CLASSES = 4
OWN = 8
R_ORDER = (0, 1, 2, 3)
L_ORDER = (2, 3, 0, 1)
NT = (((1,), (1,)), ((), ()))
TN = (((0,), (0,)), ((), ()))
f32 = jnp.float32
bf16 = jnp.bfloat16


def kernel(
    img_ref, proj_ref, inv_ref, prior_ref, out_ref, ev_ref,
    xin, white, inv3, pbuf, qbuf, sc_send, sc_recv, post_send, post_recv,
    sum_a, sum_b, r1a, r1b, mid_a, mid_b, r2a, r2b, fin_send, fin_recv,
    img_s, img_r, ring_s, ring_r, sc_s, sc_r, post_s, post_r, rs_s, rs_r, fin_s, fin_r,
):
    cls = lax.axis_index("cls")
    img = lax.axis_index("img")
    h, c = cls // 2, cls % 2
    lo, z, x = img // (NZ * NX), (img // NX) % NZ, img % NX
    y = 2 * h + lo

    def device(y_, z_, x_, c_):
        return {"cls": (y_ // 2) * 2 + c_, "img": ((y_ % 2) * NZ + z_) * NX + x_}

    def group(dx, dc):
        return device(y, z, (x + dx) % NX, (c + dc) % 2)

    def along_y(d):
        return device((y + d) % NY, z, x, c)

    def along_z(d):
        return device(y, (z + d) % NZ, x, c)

    def copy(src, dst, send, recv, to):
        return pltpu.make_async_remote_copy(
            src_ref=src, dst_ref=dst, send_sem=send, recv_sem=recv,
            device_id=to, device_id_type=pl.DeviceIdType.MESH,
        )

    barrier = pltpu.get_barrier_semaphore()
    partners = [group(s // 2, s % 2) for s in range(1, 2 * NX)]
    partners += [along_y(d) for d in range(1, NY)] + [along_z(d) for d in range(1, NZ)]
    for to in partners:
        pl.semaphore_signal(barrier, inc=1, device_id=to, device_id_type=pl.DeviceIdType.MESH)
    pl.semaphore_wait(barrier, len(partners))

    def ring(way, m, src, rel, chunk):
        return copy(
            src, pbuf.at[rel, chunk], ring_s.at[way, m], ring_r.at[way, m],
            along_y(1 if way == 0 else NY - 1),
        )

    def ring_slot(way, m):
        order = R_ORDER if way == 0 else L_ORDER
        if m < CHUNKS:
            return (3 if way == 0 else 1), order[m]
        return 2, order[m - CHUNKS]

    for way in (0, 1):
        @pl.when(lo == 1 - way)
        def _(way=way):
            for m in range(CHUNKS):
                rel, chunk = ring_slot(way, m)
                ring(way, m, proj_ref.at[chunk], rel, chunk).start()

    def image(dx):
        return copy(
            img_ref.at[(x + dx) % NX], xin.at[2 * dx], img_s.at[2 * dx], img_r.at[2 * dx],
            group(dx, 0),
        )

    def to_sibling(dx):
        src = img_ref.at[x] if dx == 0 else xin.at[2 * dx]
        s = 2 * dx + 1
        return copy(src, xin.at[s], img_s.at[s], img_r.at[s], group(0, 1))

    for dx in (2, 1, 3):
        image(dx).start()
    to_sibling(0).start()
    xin[0] = img_ref[x]

    inv = inv_ref[...]
    hi = inv.astype(bf16)
    rest = inv - hi.astype(f32)
    mid = rest.astype(bf16)
    low = (rest - mid.astype(f32)).astype(bf16)
    inv3[0:GROUPS] = hi
    inv3[GROUPS : 2 * GROUPS] = mid
    inv3[2 * GROUPS : 3 * GROUPS] = low
    inv3[3 * GROUPS :] = jnp.zeros((TAG - 3 * GROUPS, W), bf16)

    lane = lax.broadcasted_iota(jnp.int32, (BLOCK, TAG), 1)
    piece = jnp.where(lane < 96, lane // 32, jnp.minimum((lane - 96) // 4, 3))

    def block_of(rel):
        return (proj_ref if rel == 0 else pbuf.at[rel])[...].reshape(BLOCK, W)

    def columns(rel):
        p = block_of(rel).astype(f32)
        square = p * p
        s_hi = square.astype(bf16)
        s_lo = (square - s_hi.astype(f32)).astype(bf16)
        q = lax.dot_general(s_hi, inv3[...], NT, preferred_element_type=f32)
        q += lax.dot_general(s_lo, inv3[...], NT, preferred_element_type=f32)
        q = q + pltpu.roll(q, 32, 1) + pltpu.roll(q, 64, 1) + pltpu.roll(q, 96, 1)
        value = jnp.where(lane < 96, -0.5 * q, prior_ref[rel : rel + 1, :])
        v_hi = value.astype(bf16).astype(f32)
        v_mid = (value - v_hi).astype(bf16).astype(f32)
        v_lo = value - v_hi - v_mid
        both = jnp.where(piece == 0, v_hi, jnp.where(piece == 1, v_mid, jnp.where(piece == 2, v_lo, 0.0)))
        qbuf[rel] = both.astype(bf16)

    def arrived(way, m):
        rel, chunk = ring_slot(way, m)
        ring(way, m, pbuf.at[rel, chunk], rel, chunk).wait_recv()

        @pl.when(lo == way)
        def _():
            ring(way, m, pbuf.at[rel, chunk], rel, chunk).start()

        if m < 2:
            @pl.when(lo == 1 - way)
            def _():
                ring(way, CHUNKS + m, pbuf.at[rel, chunk], 2, chunk).start()

    def image_arrived(dx):
        image(dx).wait_recv()
        to_sibling(dx).start()

    def score_copy(rel, s):
        return copy(
            sc_send.at[rel, s], sc_recv.at[rel, s], sc_s.at[rel, s], sc_r.at[rel, s],
            group((NX - s // 2) % NX, s % 2),
        )

    def scores(rel):
        columns(rel)
        tags = xin[:, :, W:].reshape(2 * NX * ROWS, TAG)
        part = lax.dot_general(
            white[...].reshape(2 * NX * ROWS, W), block_of(rel), NT, preferred_element_type=f32
        )
        part += lax.dot_general(tags, qbuf[rel], NT, preferred_element_type=f32)
        sc_send[rel] = part.reshape(2 * NX, ROWS, BLOCK)
        for s in (4, 5, 2, 3, 6, 7, 1):
            score_copy(rel, s).start()

    def whiten(s):
        inverse = jnp.dot(xin[s, :, W:], inv3[...], preferred_element_type=f32)
        white[s] = (xin[s, :, :W].astype(f32) * inverse).astype(bf16)

    whiten(0)
    arrived(0, 0)
    arrived(1, 0)
    image_arrived(1)
    image_arrived(3)
    arrived(0, 1)
    arrived(1, 1)
    image_arrived(2)
    for s in (2, 6, 4):
        whiten(s)
    arrived(0, 2)
    arrived(1, 2)
    for s in (1, 3, 7, 5):
        to_sibling(s // 2).wait_recv()
        whiten(s)
    scores(0)
    arrived(0, 3)
    arrived(1, 3)
    scores(3)
    arrived(0, 4)
    arrived(1, 4)
    scores(1)
    arrived(0, 5)
    arrived(1, 5)
    scores(2)

    total = {}
    for rel in (0, 3, 1, 2):
        for s in range(1, 2 * NX):
            score_copy(rel, s).wait_recv()
        for dc in (0, 1):
            parts = [sc_send[rel, 0]] if dc == 0 else [sc_recv[rel, 1]]
            parts += [sc_recv[rel, 2 * dx + dc] for dx in range(1, NX)]
            total[rel, dc] = (parts[0] + parts[1]) + (parts[2] + parts[3])
    peak = None
    for value in total.values():
        peak = value if peak is None else jnp.maximum(peak, value)
    peak = jnp.max(peak, axis=1, keepdims=True)
    mass = None
    for value in total.values():
        term = jnp.exp(value - peak)
        mass = term if mass is None else mass + term
    evidence = peak + jnp.log(jnp.sum(mass, axis=1, keepdims=True))
    ev_ref[...] = evidence
    for (rel, dc), value in total.items():
        post_send[dc, rel] = jnp.exp(value - evidence).astype(bf16)

    def post_copy(s):
        return copy(
            post_send.at[s % 2], post_recv.at[s], post_s.at[s], post_r.at[s], group(s // 2, s % 2)
        )

    for s in (4, 5, 2, 3, 6, 7, 1):
        post_copy(s).start()
    post_recv[0] = post_send[0]
    for s in (1, 2, 3, 6, 7, 4, 5):
        post_copy(s).wait_recv()

    def weights(rel):
        return post_recv[:, rel].reshape(2 * NX * ROWS, BLOCK)

    def rs(which, d, src, dst, to):
        return copy(src, dst, rs_s.at[which, d], rs_r.at[which, d], to)

    def first_b(d):
        return rs(0, d, sum_b.at[(lo + d) % NY], r1b.at[d], along_y(d))

    def first_a(d):
        return rs(1, d, sum_a.at[(z + d) % NZ], r1a.at[d], along_z(d))

    def second_b(d):
        return rs(2, d, mid_b.at[(z + d) % NZ], r2b.at[d], along_z(d))

    def second_a(d):
        return rs(3, d, mid_a.at[(lo + d) % NY], r2a.at[d], along_y(d))

    far_first = (4, 3, 5, 2, 6, 1, 7)
    near_first = (1, 7, 2, 6, 3, 5, 4)
    for rel in range(4):
        part = lax.dot_general(
            weights(rel), white[:, :, WA:].reshape(2 * NX * ROWS, WB), TN, preferred_element_type=f32
        ).astype(bf16)
        for r in range(2 * NZ):
            sum_b[2 * rel + r // NZ, r % NZ] = part[OWN * r : OWN * (r + 1)]
    for d in far_first:
        first_b(d).start()
    for rel in range(4):
        part = lax.dot_general(
            weights(rel), white[:, :, :WA].reshape(2 * NX * ROWS, WA), TN, preferred_element_type=f32
        ).astype(bf16)
        for r in range(2 * NZ):
            sum_a[r % NZ, 2 * rel + r // NZ] = part[OWN * r : OWN * (r + 1)]
    for d in far_first:
        first_a(d).start()

    for d in near_first:
        first_b(d).wait_recv()
    for q in range(NZ):
        acc = sum_b[lo, q].astype(f32)
        for d in range(1, NY):
            acc += r1b[d, q].astype(f32)
        mid_b[q] = acc.astype(bf16)
    for d in far_first:
        second_b(d).start()
    for d in near_first:
        first_a(d).wait_recv()
    for q in range(NY):
        acc = sum_a[z, q].astype(f32)
        for d in range(1, NZ):
            acc += r1a[d, q].astype(f32)
        mid_a[q] = acc.astype(bf16)
    for d in far_first:
        second_a(d).start()

    for d in near_first:
        second_b(d).wait_recv()
    acc_b = mid_b[z].astype(f32)
    for d in range(1, NZ):
        acc_b += r2b[d].astype(f32)
    for d in near_first:
        second_a(d).wait_recv()
    acc_a = mid_a[lo].astype(f32)
    for d in range(1, NY):
        acc_a += r2a[d].astype(f32)

    def fin(d):
        return copy(
            fin_send.at[(x + d) % NX], fin_recv.at[x], fin_s.at[d], fin_r.at[d], group(d, 0)
        )

    def fin_in(d):
        return copy(
            fin_send.at[x], fin_recv.at[(x + NX - d) % NX], fin_s.at[d], fin_r.at[d], group(d, 0)
        )

    for k in range(NX):
        fin_send[k, :, :WA] = acc_a[2 * k : 2 * k + 2]
        fin_send[k, :, WA:] = acc_b[2 * k : 2 * k + 2]
    for d in (2, 1, 3):
        fin(d).start()
    fin_recv[x] = fin_send[x]
    for d in (1, 3, 2):
        fin_in(d).wait_recv()
    for k in range(NX):
        end = min(F, W * (k + 1))
        out_ref[:, W * k : end] = fin_recv[k, :, : end - W * k]

    for way in (0, 1):
        for m in range(6):
            rel, chunk = ring_slot(way, m)
            ring(way, m, pbuf.at[rel, chunk], rel, chunk).wait_send()
    for dx in range(NX):
        if dx:
            image(dx).wait_send()
        to_sibling(dx).wait_send()
    for s in range(1, 2 * NX):
        for rel in range(4):
            score_copy(rel, s).wait_send()
        post_copy(s).wait_send()
    for d in range(1, NY):
        first_a(d).wait_send()
        first_b(d).wait_send()
        second_a(d).wait_send()
        second_b(d).wait_send()
    for d in range(1, NX):
        fin(d).wait_send()


def body(images, projections, noise_power, class_logprior, groups, offsets):
    h = lax.axis_index("cls") // 2
    x = lax.axis_index("img") % NX
    lane = jnp.arange(TAG, dtype=jnp.int32)[None, :]
    is_group = (lane < 96) & (lane % 32 == groups[:, None])
    is_offset = (lane >= 96) & (lane < 108) & (lane % 4 == offsets[:, None])
    tags = (is_group | is_offset).astype(bf16)
    cut = jnp.pad(images, ((0, 0), (0, NX * W - F))).reshape(ROWS, NX, W)
    cut = jnp.concatenate([cut, jnp.broadcast_to(tags[:, None, :], (ROWS, NX, TAG))], axis=2)
    cut = jnp.transpose(cut, (1, 0, 2))
    mine = lax.dynamic_slice_in_dim(
        jnp.pad(projections, ((0, 0), (0, NX * W - F))), x * W, W, axis=1
    ).reshape(CHUNKS, CHUNK, W)
    noise = lax.dynamic_slice_in_dim(
        jnp.pad(noise_power, ((0, 0), (0, NX * W - F)), constant_values=1.0), x * W, W, axis=1
    )
    rel = jnp.arange(4, dtype=jnp.int32)[:, None]
    place = (h + rel + 128 - lane) % CLASSES
    prior = sum(jnp.where(place == n, class_logprior[n], 0.0) for n in range(CLASSES)) * (1.0 / NX)
    dma = pltpu.SemaphoreType.DMA
    out, evidence = pl.pallas_call(
        kernel,
        out_shape=(
            jax.ShapeDtypeStruct((2, F), f32),
            jax.ShapeDtypeStruct((ROWS, 1), f32),
        ),
        in_specs=[pl.BlockSpec(memory_space=pltpu.VMEM)] * 4,
        out_specs=(pl.BlockSpec(memory_space=pltpu.VMEM),) * 2,
        scratch_shapes=[
            pltpu.VMEM((2 * NX, ROWS, W + TAG), bf16),
            pltpu.VMEM((2 * NX, ROWS, W), bf16),
            pltpu.VMEM((TAG, W), bf16),
            pltpu.VMEM((4, CHUNKS, CHUNK, W), bf16),
            pltpu.VMEM((4, BLOCK, TAG), bf16),
            pltpu.VMEM((4, 2 * NX, ROWS, BLOCK), f32),
            pltpu.VMEM((4, 2 * NX, ROWS, BLOCK), f32),
            pltpu.VMEM((2, 4, ROWS, BLOCK), bf16),
            pltpu.VMEM((2 * NX, 4, ROWS, BLOCK), bf16),
            pltpu.VMEM((NZ, NY, OWN, WA), bf16),
            pltpu.VMEM((NY, NZ, OWN, WB), bf16),
            pltpu.VMEM((NZ, NY, OWN, WA), bf16),
            pltpu.VMEM((NY, NZ, OWN, WB), bf16),
            pltpu.VMEM((NY, OWN, WA), bf16),
            pltpu.VMEM((NZ, OWN, WB), bf16),
            pltpu.VMEM((NY, OWN, WA), bf16),
            pltpu.VMEM((NZ, OWN, WB), bf16),
            pltpu.VMEM((NX, 2, W), f32),
            pltpu.VMEM((NX, 2, W), f32),
            dma((2 * NX,)), dma((2 * NX,)),
            dma((2, 6)), dma((2, 6)),
            dma((4, 2 * NX)), dma((4, 2 * NX)),
            dma((2 * NX,)), dma((2 * NX,)),
            dma((4, 8)), dma((4, 8)),
            dma((NX,)), dma((NX,)),
        ],
        compiler_params=pltpu.CompilerParams(
            collective_id=0, has_side_effects=True, vmem_limit_bytes=58 * 1024 * 1024
        ),
        name="estep",
    )(cut, mine, 1.0 / noise, prior)
    return (out, evidence.reshape(ROWS))


def solution(mesh):
    in_specs = (
        P(("cls", "img"), None),
        P("cls", None),
        P(),
        P(),
        P(("cls", "img")),
        P(("cls", "img")),
    )
    out_specs = (P(("cls", "img"), None), P(("cls", "img")))
    return jax.shard_map(body, mesh=mesh, in_specs=in_specs, out_specs=out_specs, check_vma=False)
```

```python
import jax
import jax.numpy as jnp
from jax import lax
from jax.experimental import pallas as pl
from jax.experimental.pallas import tpu as pltpu
from jax.sharding import PartitionSpec as P

NX, NY, NZ = 4, 8, 8
F = 7200
W = 1920
TAG = 128
ROWS = 56
ALL = 2 * NX * ROWS
BLOCK = 128
CHUNKS = 4
CHUNK = W // CHUNKS
LAST = F - (NX - 1) * W
WA = 1024
WB = W - WA
GROUPS = 32
CLASSES = 4
OWN = 8
NN = (((1,), (0,)), ((), ()))
TN = (((0,), (0,)), ((), ()))
f32 = jnp.float32
bf16 = jnp.bfloat16


def kernel(
    img_hbm, proj_hbm, noise_hbm, prior_ref, group_ref, offset_ref, out_ref, ev_ref,
    img_v, noise_v, img_ref, xin, white, inv3, pbuf, qbuf, sc_send, sc_recv, post_send, post_recv,
    sum_a, sum_b, r1a, r1b, mid_a, mid_b, r2a, r2b, fin_send, fin_recv,
    load, img_s, img_r, cross_s, cross_r, pair_s, pair_r, sc_s, sc_r, post_s, post_r,
    rs_s, rs_r, fin_s, fin_r,
):
    cls = lax.axis_index("cls")
    img = lax.axis_index("img")
    h, c = cls // 2, cls % 2
    lo, z, x = img // (NZ * NX), (img // NX) % NZ, img % NX
    y = 2 * h + lo
    turn = (0, 3 - 2 * lo, 1 + 2 * lo, 2)

    def device(y_, z_, x_, c_):
        return {"cls": (y_ // 2) * 2 + c_, "img": ((y_ % 2) * NZ + z_) * NX + x_}

    def group(dx, dc):
        return device(y, z, (x + dx) % NX, (c + dc) % 2)

    def along_y(d):
        return device((y + d) % NY, z, x, c)

    def along_z(d):
        return device(y, (z + d) % NZ, x, c)

    across = device((y + NY - 1 + 2 * lo) % NY, z, x, c)
    beside = device(y + 1 - 2 * lo, z, x, c)

    def copy(src, dst, send, recv, to):
        return pltpu.make_async_remote_copy(
            src_ref=src, dst_ref=dst, send_sem=send, recv_sem=recv,
            device_id=to, device_id_type=pl.DeviceIdType.MESH,
        )

    load_img = pltpu.make_async_copy(img_hbm, img_v, load.at[0])
    load_noise = pltpu.make_async_copy(noise_hbm, noise_v, load.at[1])

    def load_proj(i):
        start = pl.multiple_of(x * W, 8) + i * CHUNK
        return pltpu.make_async_copy(
            proj_hbm.at[pl.ds(start, CHUNK)], pbuf.at[0, i], load.at[2 + i]
        )

    load_img.start()
    for i in range(CHUNKS - 1):
        load_proj(i).start()

    @pl.when(x < NX - 1)
    def _():
        load_proj(CHUNKS - 1).start()

    load_noise.start()

    barrier = pltpu.get_barrier_semaphore()
    partners = [group(s // 2, s % 2) for s in range(1, 2 * NX)]
    partners += [along_y(d) for d in range(1, NY)] + [along_z(d) for d in range(1, NZ)]
    for to in partners:
        pl.semaphore_signal(barrier, inc=1, device_id=to, device_id_type=pl.DeviceIdType.MESH)

    tag = lax.broadcasted_iota(jnp.int32, (TAG, ROWS), 0)
    is_group = (tag < 96) & (tag % 32 == group_ref[...])
    is_offset = (tag >= 96) & (tag < 108) & (tag % 4 == offset_ref[...])
    tags = jnp.transpose(jnp.where(is_group | is_offset, 1.0, 0.0).astype(f32)).astype(bf16)
    load_img.wait()
    for k in range(NX):
        end = min(F, W * (k + 1))
        img_ref[k, :, : end - W * k] = img_v[:, W * k : end]
        if end - W * k < W:
            img_ref[k, :, end - W * k : W] = jnp.zeros((ROWS, W * (k + 1) - end), bf16)
        img_ref[k, :, W:] = tags
    for i in range(CHUNKS - 1):
        load_proj(i).wait()

    @pl.when(x < NX - 1)
    def _():
        load_proj(CHUNKS - 1).wait()

    @pl.when(x == NX - 1)
    def _():
        pbuf[0, CHUNKS - 1] = jnp.zeros((CHUNK, BLOCK), bf16)

    pl.semaphore_wait(barrier, len(partners))

    def to_across(m):
        mine = (m + 2 * (1 - lo)) % CHUNKS
        src, dst = (pbuf.at[0, mine], pbuf.at[1, mine])
        if m >= CHUNKS:
            src, dst = (pbuf.at[2, mine], pbuf.at[3, mine])
        return copy(src, dst, cross_s.at[m], cross_r.at[m], across)

    def from_across(m):
        chunk = (m + 2 * lo) % CHUNKS
        return pbuf.at[1 if m < CHUNKS else 3, chunk]

    def to_beside(m):
        dst = pbuf.at[2 if m < CHUNKS else 3, (m + 2 * lo) % CHUNKS]
        return copy(from_across(m), dst, pair_s.at[m], pair_r.at[m], beside)

    def crossed(m):
        ref = from_across(m)
        copy(ref, ref, cross_s.at[m], cross_r.at[m], across).wait_recv()
        to_beside(m).start()

    def paired(m):
        ref = pbuf.at[2 if m < CHUNKS else 3, (m + 2 * (1 - lo)) % CHUNKS]
        copy(ref, ref, pair_s.at[m], pair_r.at[m], beside).wait_recv()
        if m < 2:
            to_across(CHUNKS + m).start()

    def image(dx):
        return copy(
            img_ref.at[(x + dx) % NX], xin.at[2 * dx], img_s.at[2 * dx], img_r.at[2 * dx],
            group(dx, 0),
        )

    def to_sibling(dx):
        src = img_ref.at[x] if dx == 0 else xin.at[2 * dx]
        s = 2 * dx + 1
        return copy(src, xin.at[s], img_s.at[s], img_r.at[s], group(0, 1))

    for m in range(CHUNKS):
        to_across(m).start()
    for dx in (2, 1, 3):
        image(dx).start()
    to_sibling(0).start()

    xin[0] = img_ref[x]
    load_noise.wait()

    def pieces(inv, width):
        hi = inv.astype(bf16)
        rest = inv - hi.astype(f32)
        mid = rest.astype(bf16)
        low = (rest - mid.astype(f32)).astype(bf16)
        inv3[0:GROUPS, :width] = hi
        inv3[GROUPS : 2 * GROUPS, :width] = mid
        inv3[2 * GROUPS : 3 * GROUPS, :width] = low

    inv3[3 * GROUPS :] = jnp.zeros((TAG - 3 * GROUPS, W), bf16)

    @pl.when(x < NX - 1)
    def _():
        pieces(1.0 / noise_v[:, pl.ds(pl.multiple_of(x * W, 128), W)], W)

    @pl.when(x == NX - 1)
    def _():
        pieces(1.0 / noise_v[:, F - LAST :], LAST)
        inv3[: 3 * GROUPS, LAST:] = jnp.zeros((3 * GROUPS, W - LAST), bf16)

    row = lax.broadcasted_iota(jnp.int32, (TAG, BLOCK), 0)
    piece = jnp.where(row < 96, row // 32, jnp.minimum((row - 96) // 4, 3))

    def block_of(slot):
        return pbuf[slot].reshape(W, BLOCK)

    def columns(slot):
        p = block_of(slot).astype(f32)
        square = p * p
        s_hi = square.astype(bf16)
        s_lo = (square - s_hi.astype(f32)).astype(bf16)
        q = lax.dot_general(inv3[...], s_hi, NN, preferred_element_type=f32)
        q += lax.dot_general(inv3[...], s_lo, NN, preferred_element_type=f32)
        q = q[0:32] + q[32:64] + q[64:96]
        prior = jnp.zeros((TAG, BLOCK), f32)
        for o in range(CLASSES):
            log_prior = prior_ref[0, (h + turn[slot] + CLASSES - o) % CLASSES]
            prior = jnp.where(row % CLASSES == o, log_prior * (1.0 / NX), prior)
        value = jnp.where(row < 96, -0.5 * jnp.concatenate([q] * 4, axis=0), prior)
        v_hi = value.astype(bf16).astype(f32)
        v_mid = (value - v_hi).astype(bf16).astype(f32)
        v_lo = value - v_hi - v_mid
        both = jnp.where(piece == 2, v_lo, 0.0)
        both = jnp.where(piece == 1, v_mid, both)
        qbuf[slot] = jnp.where(piece == 0, v_hi, both).astype(bf16)

    def image_arrived(dx):
        image(dx).wait_recv()
        to_sibling(dx).start()

    def score_copy(slot, s):
        return copy(
            sc_send.at[slot, s], sc_recv.at[slot, s], sc_s.at[slot, s], sc_r.at[slot, s],
            group((NX - s // 2) % NX, s % 2),
        )

    def scores(slot):
        part = lax.dot_general(
            white[...].reshape(ALL, W), block_of(slot), NN, preferred_element_type=f32
        )
        part += lax.dot_general(
            xin[:, :, W:].reshape(ALL, TAG), qbuf[slot], NN, preferred_element_type=f32
        )
        sc_send[slot] = part.reshape(2 * NX, ROWS, BLOCK)
        for s in (4, 5, 2, 3, 6, 7, 1):
            score_copy(slot, s).start()

    def whiten(s):
        inverse = jnp.dot(xin[s, :, W:], inv3[...], preferred_element_type=f32)
        white[s] = (xin[s, :, :W].astype(f32) * inverse).astype(bf16)

    whiten(0)
    columns(0)
    crossed(0)
    crossed(1)
    paired(0)
    image_arrived(1)
    image_arrived(3)
    crossed(2)
    paired(1)
    image_arrived(2)
    crossed(3)
    for s in (2, 6, 4):
        whiten(s)
    columns(1)
    for s in (1, 3, 7, 5):
        to_sibling(s // 2).wait_recv()
        whiten(s)
    scores(0)
    scores(1)
    crossed(4)
    paired(2)
    paired(3)
    columns(2)
    scores(2)
    crossed(5)
    paired(4)
    paired(5)
    columns(3)
    scores(3)

    total = {}
    for slot in range(4):
        for s in range(1, 2 * NX):
            score_copy(slot, s).wait_recv()
        for dc in (0, 1):
            parts = [sc_send[slot, 0]] if dc == 0 else [sc_recv[slot, 1]]
            parts += [sc_recv[slot, 2 * dx + dc] for dx in range(1, NX)]
            total[slot, dc] = (parts[0] + parts[1]) + (parts[2] + parts[3])
    peak = None
    for value in total.values():
        peak = value if peak is None else jnp.maximum(peak, value)
    peak = jnp.max(peak, axis=1, keepdims=True)
    mass = None
    for value in total.values():
        term = jnp.exp(value - peak)
        mass = term if mass is None else mass + term
    evidence = peak + jnp.log(jnp.sum(mass, axis=1, keepdims=True))
    ev_ref[...] = jnp.transpose(jnp.broadcast_to(evidence, (ROWS, TAG)))[0:1, :]
    for (slot, dc), value in total.items():
        post_send[dc, slot] = jnp.exp(value - evidence).astype(bf16)

    def post_copy(s):
        return copy(
            post_send.at[s % 2], post_recv.at[s], post_s.at[s], post_r.at[s], group(s // 2, s % 2)
        )

    for s in (4, 5, 2, 3, 6, 7, 1):
        post_copy(s).start()
    post_recv[0] = post_send[0]
    for s in (1, 2, 3, 6, 7, 4, 5):
        post_copy(s).wait_recv()

    def weights(slot):
        return post_recv[:, slot].reshape(ALL, BLOCK)

    def rs(which, d, src, dst, to):
        return copy(src, dst, rs_s.at[which, d], rs_r.at[which, d], to)

    def first_b(d):
        return rs(0, d, sum_b.at[(lo + d) % NY], r1b.at[d], along_y(d))

    def first_a(d):
        return rs(1, d, sum_a.at[(z + d) % NZ], r1a.at[d], along_z(d))

    def second_b(d):
        return rs(2, d, mid_b.at[(z + d) % NZ], r2b.at[d], along_z(d))

    def second_a(d):
        return rs(3, d, mid_a.at[(lo + d) % NY], r2a.at[d], along_y(d))

    far_first = (4, 3, 5, 2, 6, 1, 7)
    near_first = (1, 7, 2, 6, 3, 5, 4)
    for slot in range(4):
        part = lax.dot_general(
            weights(slot), white[:, :, WA:].reshape(ALL, WB), TN, preferred_element_type=f32
        ).astype(bf16)
        for r in range(2 * NZ):
            sum_b[2 * turn[slot] + r // NZ, r % NZ] = part[OWN * r : OWN * (r + 1)]
    for d in far_first:
        first_b(d).start()
    for slot in range(4):
        part = lax.dot_general(
            weights(slot), white[:, :, :WA].reshape(ALL, WA), TN, preferred_element_type=f32
        ).astype(bf16)
        for r in range(2 * NZ):
            sum_a[r % NZ, 2 * turn[slot] + r // NZ] = part[OWN * r : OWN * (r + 1)]
    for d in far_first:
        first_a(d).start()

    for d in near_first:
        first_b(d).wait_recv()
    for q in range(NZ):
        acc = sum_b[lo, q].astype(f32)
        for d in range(1, NY):
            acc += r1b[d, q].astype(f32)
        mid_b[q] = acc.astype(bf16)
    for d in far_first:
        second_b(d).start()
    for d in near_first:
        first_a(d).wait_recv()
    for q in range(NY):
        acc = sum_a[z, q].astype(f32)
        for d in range(1, NZ):
            acc += r1a[d, q].astype(f32)
        mid_a[q] = acc.astype(bf16)
    for d in far_first:
        second_a(d).start()

    for d in near_first:
        second_b(d).wait_recv()
    acc_b = mid_b[z].astype(f32)
    for d in range(1, NZ):
        acc_b += r2b[d].astype(f32)
    for d in near_first:
        second_a(d).wait_recv()
    acc_a = mid_a[lo].astype(f32)
    for d in range(1, NY):
        acc_a += r2a[d].astype(f32)

    def fin(d):
        return copy(
            fin_send.at[(x + d) % NX], fin_recv.at[x], fin_s.at[d], fin_r.at[d], group(d, 0)
        )

    def fin_in(d):
        return copy(
            fin_send.at[x], fin_recv.at[(x + NX - d) % NX], fin_s.at[d], fin_r.at[d], group(d, 0)
        )

    for k in range(NX):
        fin_send[k, :, :WA] = acc_a[2 * k : 2 * k + 2]
        fin_send[k, :, WA:] = acc_b[2 * k : 2 * k + 2]
    for d in (2, 1, 3):
        fin(d).start()
    fin_recv[x] = fin_send[x]
    for d in (1, 3, 2):
        fin_in(d).wait_recv()
    for k in range(NX):
        end = min(F, W * (k + 1))
        out_ref[:, W * k : end] = fin_recv[k, :, : end - W * k]

    for m in range(6):
        to_across(m).wait_send()
        to_beside(m).wait_send()
    for dx in range(NX):
        if dx:
            image(dx).wait_send()
        to_sibling(dx).wait_send()
    for s in range(1, 2 * NX):
        for slot in range(4):
            score_copy(slot, s).wait_send()
        post_copy(s).wait_send()
    for d in range(1, NY):
        first_a(d).wait_send()
        first_b(d).wait_send()
        second_a(d).wait_send()
        second_b(d).wait_send()
    for d in range(1, NX):
        fin(d).wait_send()


def body(images, projections, noise_power, class_logprior, groups, offsets):
    dma = pltpu.SemaphoreType.DMA
    anywhere = pl.BlockSpec(memory_space=pl.ANY)
    vmem = pl.BlockSpec(memory_space=pltpu.VMEM)
    out, evidence = pl.pallas_call(
        kernel,
        out_shape=(
            jax.ShapeDtypeStruct((2, F), f32),
            jax.ShapeDtypeStruct((1, ROWS), f32),
        ),
        in_specs=[anywhere] * 3 + [pl.BlockSpec(memory_space=pltpu.SMEM), vmem, vmem],
        out_specs=(vmem, vmem),
        scratch_shapes=[
            pltpu.VMEM((ROWS, F), bf16),
            pltpu.VMEM((GROUPS, F), f32),
            pltpu.VMEM((NX, ROWS, W + TAG), bf16),
            pltpu.VMEM((2 * NX, ROWS, W + TAG), bf16),
            pltpu.VMEM((2 * NX, ROWS, W), bf16),
            pltpu.VMEM((TAG, W), bf16),
            pltpu.VMEM((4, CHUNKS, CHUNK, BLOCK), bf16),
            pltpu.VMEM((4, TAG, BLOCK), bf16),
            pltpu.VMEM((4, 2 * NX, ROWS, BLOCK), f32),
            pltpu.VMEM((4, 2 * NX, ROWS, BLOCK), f32),
            pltpu.VMEM((2, 4, ROWS, BLOCK), bf16),
            pltpu.VMEM((2 * NX, 4, ROWS, BLOCK), bf16),
            pltpu.VMEM((NZ, NY, OWN, WA), bf16),
            pltpu.VMEM((NY, NZ, OWN, WB), bf16),
            pltpu.VMEM((NZ, NY, OWN, WA), bf16),
            pltpu.VMEM((NY, NZ, OWN, WB), bf16),
            pltpu.VMEM((NY, OWN, WA), bf16),
            pltpu.VMEM((NZ, OWN, WB), bf16),
            pltpu.VMEM((NY, OWN, WA), bf16),
            pltpu.VMEM((NZ, OWN, WB), bf16),
            pltpu.VMEM((NX, 2, W), f32),
            pltpu.VMEM((NX, 2, W), f32),
            dma((2 + CHUNKS,)),
            dma((2 * NX,)), dma((2 * NX,)),
            dma((6,)), dma((6,)),
            dma((6,)), dma((6,)),
            dma((4, 2 * NX)), dma((4, 2 * NX)),
            dma((2 * NX,)), dma((2 * NX,)),
            dma((4, 8)), dma((4, 8)),
            dma((NX,)), dma((NX,)),
        ],
        compiler_params=pltpu.CompilerParams(
            collective_id=0, has_side_effects=True, vmem_limit_bytes=58 * 1024 * 1024
        ),
        name="estep",
    )(
        images, projections.T, noise_power, class_logprior.reshape(1, CLASSES),
        groups.reshape(1, ROWS), offsets.reshape(1, ROWS),
    )
    return (out, evidence.reshape(ROWS))


def solution(mesh):
    in_specs = (
        P(("cls", "img"), None),
        P("cls", None),
        P(),
        P(),
        P(("cls", "img")),
        P(("cls", "img")),
    )
    out_specs = (P(("cls", "img"), None), P(("cls", "img")))
    return jax.shard_map(body, mesh=mesh, in_specs=in_specs, out_specs=out_specs, check_vma=False)
```

```python
import jax
import jax.numpy as jnp
from jax import lax
from jax.experimental import pallas as pl
from jax.experimental.pallas import tpu as pltpu
from jax.sharding import PartitionSpec as P

NX, NY, NZ = 4, 8, 8
F = 7200
W = 1920
TAG = 128
ROWS = 56
ALL = 2 * NX * ROWS
BLOCK = 128
CHUNKS = 4
PARTS = 2 * CHUNKS
CHUNK = W // PARTS
WHOLE = F // CHUNK - (NX - 1) * PARTS
STEPS = (0, 1, 3, 2)
EARLY = 6
LAST = F - (NX - 1) * W
WA = 1024
WB = W - WA
GROUPS = 32
CLASSES = 4
OWN = 8
NN = (((1,), (0,)), ((), ()))
TN = (((0,), (0,)), ((), ()))
f32 = jnp.float32
bf16 = jnp.bfloat16


def finish(fin_ref, ev_ref, out_ref, evidence_ref):
    for k in range(NX):
        end = min(F, W * (k + 1))
        out_ref[:, W * k : end] = fin_ref[k, :, : end - W * k]
    evidence_ref[...] = ev_ref[...]


def kernel(
    img_hbm, proj_hbm, noise_hbm, prior_ref, group_ref, offset_ref, out_ref, ev_ref,
    img_v, noise_v, img_ref, xin, white, inv3, pbuf, qbuf, sc_send, sc_recv, post_send, post_recv,
    sum_a, sum_b, r1a, r1b, mid_a, mid_b, r2a, r2b, fin_send, fin_recv,
    load, img_s, img_r, cross_s, cross_r, pair_s, pair_r, side_s, side_r, sc_s, sc_r, post_s, post_r,
    rs_s, rs_r, fin_s, fin_r,
):
    cls = lax.axis_index("cls")
    img = lax.axis_index("img")
    h, c = cls // 2, cls % 2
    lo, z, x = img // (NZ * NX), (img // NX) % NZ, img % NX
    y = 2 * h + lo
    turn = (0, 3 - 2 * lo, 1 + 2 * lo, 2)
    half = z % 2

    def device(y_, z_, x_, c_):
        return {"cls": (y_ // 2) * 2 + c_, "img": ((y_ % 2) * NZ + z_) * NX + x_}

    def group(dx, dc):
        return device(y, z, (x + dx) % NX, (c + dc) % 2)

    def along_y(d):
        return device((y + d) % NY, z, x, c)

    def along_z(d):
        return device(y, (z + d) % NZ, x, c)

    across = device((y + NY - 1 + 2 * lo) % NY, z, x, c)
    beside = device(y + 1 - 2 * lo, z, x, c)

    def copy(src, dst, send, recv, to):
        return pltpu.make_async_remote_copy(
            src_ref=src, dst_ref=dst, send_sem=send, recv_sem=recv,
            device_id=to, device_id_type=pl.DeviceIdType.MESH,
        )

    load_img = pltpu.make_async_copy(img_hbm, img_v, load.at[0])
    load_noise = pltpu.make_async_copy(noise_hbm, noise_v, load.at[1])

    load_proj = pltpu.make_async_copy(
        proj_hbm.at[pl.ds(x * PARTS, WHOLE)], pbuf.at[0, pl.ds(0, WHOLE)], load.at[2]
    )
    load_rest = pltpu.make_async_copy(
        proj_hbm.at[pl.ds((x % (NX - 1)) * PARTS + WHOLE, PARTS - WHOLE)],
        pbuf.at[0, pl.ds(WHOLE, PARTS - WHOLE)], load.at[3],
    )
    load_img.start()
    load_proj.start()

    @pl.when(x < NX - 1)
    def _():
        load_rest.start()

    load_noise.start()

    barrier = pltpu.get_barrier_semaphore()
    partners = [group(s // 2, s % 2) for s in range(1, 2 * NX)]
    partners += [along_y(d) for d in range(1, NY)] + [along_z(d) for d in range(1, NZ)]
    for to in partners:
        pl.semaphore_signal(barrier, inc=1, device_id=to, device_id_type=pl.DeviceIdType.MESH)

    tag = lax.broadcasted_iota(jnp.int32, (TAG, ROWS), 0)
    is_group = (tag < 96) & (tag % 32 == group_ref[...])
    is_offset = (tag >= 96) & (tag < 108) & (tag % 4 == offset_ref[...])
    tags = jnp.transpose(jnp.where(is_group | is_offset, 1.0, 0.0).astype(f32)).astype(bf16)
    load_img.wait()
    for k in range(NX):
        end = min(F, W * (k + 1))
        img_ref[k, :, : end - W * k] = img_v[:, W * k : end]
        if end - W * k < W:
            img_ref[k, :, end - W * k : W] = jnp.zeros((ROWS, W * (k + 1) - end), bf16)
        img_ref[k, :, W:] = tags
    load_proj.wait()

    @pl.when(x < NX - 1)
    def _():
        load_rest.wait()

    @pl.when(x == NX - 1)
    def _():
        pbuf[0, WHOLE:] = jnp.zeros((PARTS - WHOLE, CHUNK, BLOCK), bf16)

    pl.semaphore_wait(barrier, len(partners))

    def turned(m, low):
        return (m + 2 * low) % CHUNKS

    def to_across(m):
        mine = half * CHUNKS + turned(m, 1 - lo)
        src, dst = (pbuf.at[0, mine], pbuf.at[1, mine])
        if m >= CHUNKS:
            src, dst = (pbuf.at[2, mine], pbuf.at[3, mine])
        return copy(src, dst, cross_s.at[m], cross_r.at[m], across)

    def from_across(m):
        return pbuf.at[1 if m < CHUNKS else 3, half * CHUNKS + turned(m, lo)]

    def to_beside(m):
        dst = pbuf.at[2 if m < CHUNKS else 3, half * CHUNKS + turned(m, lo)]
        return copy(from_across(m), dst, pair_s.at[m], pair_r.at[m], beside)

    def from_beside(m):
        return pbuf.at[2 if m < CHUNKS else 3, half * CHUNKS + turned(m, 1 - lo)]

    def to_side(way, m):
        ref = from_across(m) if way == 0 else from_beside(m)
        up = 1 - 2 * (turned(m, lo if way == 0 else 1 - lo) // 2)
        to = device(y, (z + NZ + up) % NZ, x, c)
        return copy(ref, ref, side_s.at[way, m], side_r.at[way, m], to)

    def sided(way, m):
        chunk = (1 - half) * CHUNKS + turned(m, lo if way == 0 else 1 - lo)
        ref = pbuf.at[(1 + way) if m < CHUNKS else 3, chunk]
        copy(ref, ref, side_s.at[way, m], side_r.at[way, m], along_z(1)).wait_recv()

    def crossed(m):
        ref = from_across(m)
        copy(ref, ref, cross_s.at[m], cross_r.at[m], across).wait_recv()
        to_beside(m).start()
        to_side(0, m).start()

    def paired(m):
        ref = from_beside(m)
        copy(ref, ref, pair_s.at[m], pair_r.at[m], beside).wait_recv()
        if m < 2:
            to_across(CHUNKS + m).start()
        to_side(1, m).start()

    def image(p):
        return copy(
            img_ref.at[(x + STEPS[p]) % NX], xin.at[2 * p], img_s.at[2 * p], img_r.at[2 * p],
            group(STEPS[p], 0),
        )

    def to_sibling(p):
        src = img_ref.at[x] if p == 0 else xin.at[2 * p]
        s = 2 * p + 1
        return copy(src, xin.at[s], img_s.at[s], img_r.at[s], group(0, 1))

    for m in range(CHUNKS):
        to_across(m).start()
    for p in (1, 2, 3):
        image(p).start()
    to_sibling(0).start()

    xin[0] = img_ref[x]
    load_noise.wait()

    def pieces(inv, width):
        hi = inv.astype(bf16)
        rest = inv - hi.astype(f32)
        mid = rest.astype(bf16)
        low = (rest - mid.astype(f32)).astype(bf16)
        inv3[0:GROUPS, :width] = hi
        inv3[GROUPS : 2 * GROUPS, :width] = mid
        inv3[2 * GROUPS : 3 * GROUPS, :width] = low

    inv3[3 * GROUPS :] = jnp.zeros((TAG - 3 * GROUPS, W), bf16)

    @pl.when(x < NX - 1)
    def _():
        pieces(1.0 / noise_v[:, pl.ds(pl.multiple_of(x * W, 128), W)], W)

    @pl.when(x == NX - 1)
    def _():
        pieces(1.0 / noise_v[:, F - LAST :], LAST)
        inv3[: 3 * GROUPS, LAST:] = jnp.zeros((3 * GROUPS, W - LAST), bf16)

    row = lax.broadcasted_iota(jnp.int32, (TAG, BLOCK), 0)
    piece = jnp.where(row < 96, row // 32, jnp.minimum((row - 96) // 4, 3))

    def block_of(slot):
        return pbuf[slot].reshape(W, BLOCK)

    def columns(slot):
        p = block_of(slot).astype(f32)
        square = p * p
        s_hi = square.astype(bf16)
        s_lo = (square - s_hi.astype(f32)).astype(bf16)
        q = lax.dot_general(inv3[...], s_hi, NN, preferred_element_type=f32)
        q += lax.dot_general(inv3[...], s_lo, NN, preferred_element_type=f32)
        q = q[0:32] + q[32:64] + q[64:96]
        prior = jnp.zeros((TAG, BLOCK), f32)
        for o in range(CLASSES):
            log_prior = prior_ref[0, (h + turn[slot] + CLASSES - o) % CLASSES]
            prior = jnp.where(row % CLASSES == o, log_prior * (1.0 / NX), prior)
        value = jnp.where(row < 96, -0.5 * jnp.concatenate([q] * 4, axis=0), prior)
        v_hi = value.astype(bf16).astype(f32)
        v_mid = (value - v_hi).astype(bf16).astype(f32)
        v_lo = value - v_hi - v_mid
        both = jnp.where(piece == 2, v_lo, 0.0)
        both = jnp.where(piece == 1, v_mid, both)
        qbuf[slot] = jnp.where(piece == 0, v_hi, both).astype(bf16)

    def image_arrived(p):
        image(p).wait_recv()
        to_sibling(p).start()

    def score_copy(slot, s):
        return copy(
            sc_send.at[slot, s], sc_recv.at[slot, s], sc_s.at[slot, s], sc_r.at[slot, s],
            group((NX - STEPS[s // 2]) % NX, s % 2),
        )

    def scores(slot, first, last):
        rows = (last - first) * ROWS
        part = lax.dot_general(
            white[first:last].reshape(rows, W), block_of(slot), NN, preferred_element_type=f32
        )
        part += lax.dot_general(
            xin[first:last, :, W:].reshape(rows, TAG), qbuf[slot], NN, preferred_element_type=f32
        )
        sc_send[slot, first:last] = part.reshape(last - first, ROWS, BLOCK)
        for s in (6, 7, 2, 4, 3, 5, 1):
            if first <= s < last:
                score_copy(slot, s).start()

    def whiten(s):
        inverse = jnp.dot(xin[s, :, W:], inv3[...], preferred_element_type=f32)
        white[s] = (xin[s, :, :W].astype(f32) * inverse).astype(bf16)

    whiten(0)
    columns(0)
    crossed(0)
    crossed(1)
    crossed(2)
    paired(0)
    crossed(3)
    paired(1)
    image_arrived(1)
    image_arrived(2)
    whiten(2)
    whiten(4)
    paired(2)
    crossed(4)
    for s in (1, 3, 5):
        to_sibling(s // 2).wait_recv()
        whiten(s)
    paired(3)
    scores(0, 0, EARLY)
    crossed(5)
    for m in range(CHUNKS):
        sided(0, m)
    columns(1)
    scores(1, 0, EARLY)
    paired(4)
    image_arrived(3)
    whiten(6)
    for m in range(CHUNKS):
        sided(1, m)
    columns(2)
    paired(5)
    to_sibling(3).wait_recv()
    whiten(7)
    scores(0, EARLY, 2 * NX)
    scores(1, EARLY, 2 * NX)
    scores(2, 0, 2 * NX)
    for m in (CHUNKS, CHUNKS + 1):
        sided(0, m)
        sided(1, m)
    columns(3)
    scores(3, 0, 2 * NX)

    total = {}
    for slot in range(4):
        for s in range(1, 2 * NX):
            score_copy(slot, s).wait_recv()
        for dc in (0, 1):
            parts = [sc_send[slot, 0]] if dc == 0 else [sc_recv[slot, 1]]
            parts += [sc_recv[slot, 2 * dx + dc] for dx in range(1, NX)]
            total[slot, dc] = (parts[0] + parts[1]) + (parts[2] + parts[3])
    peak = None
    for value in total.values():
        peak = value if peak is None else jnp.maximum(peak, value)
    peak = jnp.max(peak, axis=1, keepdims=True)
    mass = None
    for value in total.values():
        term = jnp.exp(value - peak)
        mass = term if mass is None else mass + term
    evidence = peak + jnp.log(jnp.sum(mass, axis=1, keepdims=True))
    ev_ref[...] = jnp.transpose(jnp.broadcast_to(evidence, (ROWS, TAG)))[0:1, :]
    for (slot, dc), value in total.items():
        post_send[dc, slot] = jnp.exp(value - evidence).astype(bf16)

    def post_copy(s):
        return copy(
            post_send.at[s % 2], post_recv.at[s], post_s.at[s], post_r.at[s],
            group(STEPS[s // 2], s % 2),
        )

    for s in (6, 7, 2, 4, 3, 5, 1):
        post_copy(s).start()
    post_recv[0] = post_send[0]
    for s in (1, 2, 4, 3, 5, 6, 7):
        post_copy(s).wait_recv()

    def weights(slot):
        return post_recv[:, slot].reshape(ALL, BLOCK)

    def rs(which, d, src, dst, to):
        return copy(src, dst, rs_s.at[which, d], rs_r.at[which, d], to)

    def first_b(d):
        return rs(0, d, sum_b.at[(lo + d) % NY], r1b.at[d], along_y(d))

    def first_a(d):
        return rs(1, d, sum_a.at[(z + d) % NZ], r1a.at[d], along_z(d))

    def second_b(d):
        return rs(2, d, mid_b.at[(z + d) % NZ], r2b.at[d], along_z(d))

    def second_a(d):
        return rs(3, d, mid_a.at[(lo + d) % NY], r2a.at[d], along_y(d))

    far_first = (4, 3, 5, 2, 6, 1, 7)
    near_first = (1, 7, 2, 6, 3, 5, 4)
    for slot in range(4):
        part = lax.dot_general(
            weights(slot), white[:, :, WA:].reshape(ALL, WB), TN, preferred_element_type=f32
        ).astype(bf16)
        for r in range(2 * NZ):
            sum_b[2 * turn[slot] + r // NZ, r % NZ] = part[OWN * r : OWN * (r + 1)]
    for d in far_first:
        first_b(d).start()
    for slot in range(4):
        part = lax.dot_general(
            weights(slot), white[:, :, :WA].reshape(ALL, WA), TN, preferred_element_type=f32
        ).astype(bf16)
        for r in range(2 * NZ):
            sum_a[r % NZ, 2 * turn[slot] + r // NZ] = part[OWN * r : OWN * (r + 1)]
    for d in far_first:
        first_a(d).start()

    for d in near_first:
        first_b(d).wait_recv()
    for q in range(NZ):
        acc = sum_b[lo, q].astype(f32)
        for d in range(1, NY):
            acc += r1b[d, q].astype(f32)
        mid_b[q] = acc.astype(bf16)
    for d in far_first:
        second_b(d).start()
    for d in near_first:
        first_a(d).wait_recv()
    for q in range(NY):
        acc = sum_a[z, q].astype(f32)
        for d in range(1, NZ):
            acc += r1a[d, q].astype(f32)
        mid_a[q] = acc.astype(bf16)
    for d in far_first:
        second_a(d).start()

    for d in near_first:
        second_b(d).wait_recv()
    acc_b = mid_b[z].astype(f32)
    for d in range(1, NZ):
        acc_b += r2b[d].astype(f32)
    for d in near_first:
        second_a(d).wait_recv()
    acc_a = mid_a[lo].astype(f32)
    for d in range(1, NY):
        acc_a += r2a[d].astype(f32)

    def fin(d):
        return copy(
            fin_send.at[(x + d) % NX], fin_recv.at[x], fin_s.at[d], fin_r.at[d], group(d, 0)
        )

    def fin_in(d):
        return copy(
            fin_send.at[x], fin_recv.at[(x + NX - d) % NX], fin_s.at[d], fin_r.at[d], group(d, 0)
        )

    for k in range(NX):
        fin_send[k, :, :WA] = acc_a[2 * k : 2 * k + 2]
        fin_send[k, :, WA:] = acc_b[2 * k : 2 * k + 2]
    for d in (2, 1, 3):
        fin(d).start()
    fin_recv[x] = fin_send[x]
    for d in (1, 3, 2):
        fin_in(d).wait_recv()
    out_ref[...] = fin_recv[...]

    for m in range(6):
        to_across(m).wait_send()
        to_beside(m).wait_send()
        to_side(0, m).wait_send()
        to_side(1, m).wait_send()
    for p in range(NX):
        if p:
            image(p).wait_send()
        to_sibling(p).wait_send()
    for s in range(1, 2 * NX):
        for slot in range(4):
            score_copy(slot, s).wait_send()
        post_copy(s).wait_send()
    for d in range(1, NY):
        first_a(d).wait_send()
        first_b(d).wait_send()
        second_a(d).wait_send()
        second_b(d).wait_send()
    for d in range(1, NX):
        fin(d).wait_send()


def body(images, projections, noise_power, class_logprior, groups, offsets):
    dma = pltpu.SemaphoreType.DMA
    anywhere = pl.BlockSpec(memory_space=pl.ANY)
    vmem = pl.BlockSpec(memory_space=pltpu.VMEM)
    out, evidence = pl.pallas_call(
        kernel,
        out_shape=(
            jax.ShapeDtypeStruct((NX, 2, W), f32),
            jax.ShapeDtypeStruct((1, ROWS), f32),
        ),
        in_specs=[anywhere] * 3 + [pl.BlockSpec(memory_space=pltpu.SMEM), vmem, vmem],
        out_specs=(vmem, vmem),
        scratch_shapes=[
            pltpu.VMEM((ROWS, F), bf16),
            pltpu.VMEM((GROUPS, F), f32),
            pltpu.VMEM((NX, ROWS, W + TAG), bf16),
            pltpu.VMEM((2 * NX, ROWS, W + TAG), bf16),
            pltpu.VMEM((2 * NX, ROWS, W), bf16),
            pltpu.VMEM((TAG, W), bf16),
            pltpu.VMEM((4, PARTS, CHUNK, BLOCK), bf16),
            pltpu.VMEM((4, TAG, BLOCK), bf16),
            pltpu.VMEM((4, 2 * NX, ROWS, BLOCK), f32),
            pltpu.VMEM((4, 2 * NX, ROWS, BLOCK), f32),
            pltpu.VMEM((2, 4, ROWS, BLOCK), bf16),
            pltpu.VMEM((2 * NX, 4, ROWS, BLOCK), bf16),
            pltpu.VMEM((NZ, NY, OWN, WA), bf16),
            pltpu.VMEM((NY, NZ, OWN, WB), bf16),
            pltpu.VMEM((NZ, NY, OWN, WA), bf16),
            pltpu.VMEM((NY, NZ, OWN, WB), bf16),
            pltpu.VMEM((NY, OWN, WA), bf16),
            pltpu.VMEM((NZ, OWN, WB), bf16),
            pltpu.VMEM((NY, OWN, WA), bf16),
            pltpu.VMEM((NZ, OWN, WB), bf16),
            pltpu.VMEM((NX, 2, W), f32),
            pltpu.VMEM((NX, 2, W), f32),
            dma((4,)),
            dma((2 * NX,)), dma((2 * NX,)),
            dma((6,)), dma((6,)),
            dma((6,)), dma((6,)),
            dma((2, 6)), dma((2, 6)),
            dma((4, 2 * NX)), dma((4, 2 * NX)),
            dma((2 * NX,)), dma((2 * NX,)),
            dma((4, 8)), dma((4, 8)),
            dma((NX,)), dma((NX,)),
        ],
        compiler_params=pltpu.CompilerParams(
            collective_id=0, has_side_effects=True, vmem_limit_bytes=58 * 1024 * 1024
        ),
        name="estep",
    )(
        images, projections.T.reshape(F // CHUNK, CHUNK, BLOCK), noise_power, class_logprior.reshape(1, CLASSES),
        groups.reshape(1, ROWS), offsets.reshape(1, ROWS),
    )
    out, evidence = pl.pallas_call(
        finish,
        out_shape=(
            jax.ShapeDtypeStruct((2, F), f32),
            jax.ShapeDtypeStruct((1, ROWS), f32),
        ),
        in_specs=[vmem, vmem],
        out_specs=(vmem, vmem),
        name="finish",
    )(out, evidence)
    return (out, evidence.reshape(ROWS))


def solution(mesh):
    in_specs = (
        P(("cls", "img"), None),
        P("cls", None),
        P(),
        P(),
        P(("cls", "img")),
        P(("cls", "img")),
    )
    out_specs = (P(("cls", "img"), None), P(("cls", "img")))
    return jax.shard_map(body, mesh=mesh, in_specs=in_specs, out_specs=out_specs, check_vma=False)
```

```python
import jax
import jax.numpy as jnp
from jax import lax
from jax.experimental import pallas as pl
from jax.experimental.pallas import tpu as pltpu
from jax.sharding import PartitionSpec as P

NX, NY, NZ = 4, 8, 8
F = 7200
W = 1920
TAG = 128
ROWS = 56
ALL = 2 * NX * ROWS
BLOCK = 128
CHUNKS = 4
PARTS = 2 * CHUNKS
CHUNK = W // PARTS
WHOLE = F // CHUNK - (NX - 1) * PARTS
STEPS = (0, 1, 3, 2)
EARLY = 6
LAST = F - (NX - 1) * W
WA = 1024
WB = W - WA
GROUPS = 32
CLASSES = 4
OWN = 8
STREAMS = (
    ("z", 1, 0, 256), ("z", -1, 256, 256), ("y", 1, 1024, 256), ("y", -1, 1280, 256),
    ("z", 1, 512, 256), ("z", -1, 768, 256), ("y", 1, 1536, 256), ("y", -1, 1792, 128),
)
NN = (((1,), (0,)), ((), ()))
f32 = jnp.float32
bf16 = jnp.bfloat16


def finish(fin_ref, ev_ref, out_ref, evidence_ref):
    for k in range(NX):
        end = min(F, W * (k + 1))
        out_ref[:, W * k : end] = fin_ref[k, :, : end - W * k]
    evidence_ref[...] = ev_ref[...]


def kernel(
    img_hbm, proj_hbm, noise_hbm, prior_ref, group_ref, offset_ref, out_ref, ev_ref,
    img_v, noise_v, img_ref, xin, white, inv3, pbuf, qbuf, sc_send, sc_recv, post_send, post_recv,
    wt, parts, in1, mid1, in2, mid2, in3, own, got,
    load, img_s, img_r, cross_s, cross_r, pair_s, pair_r, side_s, side_r, sc_s, sc_r, post_s, post_r,
    st_s, st_r, own_s, own_r,
):
    cls = lax.axis_index("cls")
    img = lax.axis_index("img")
    h, c = cls // 2, cls % 2
    lo, z, x = img // (NZ * NX), (img // NX) % NZ, img % NX
    y = 2 * h + lo
    turn = (0, 3 - 2 * lo, 1 + 2 * lo, 2)
    half = z % 2

    def device(y_, z_, x_, c_):
        return {"cls": (y_ // 2) * 2 + c_, "img": ((y_ % 2) * NZ + z_) * NX + x_}

    def group(dx, dc):
        return device(y, z, (x + dx) % NX, (c + dc) % 2)

    def along_y(d):
        return device((y + d) % NY, z, x, c)

    def along_z(d):
        return device(y, (z + d) % NZ, x, c)

    across = device((y + NY - 1 + 2 * lo) % NY, z, x, c)
    beside = device(y + 1 - 2 * lo, z, x, c)

    def copy(src, dst, send, recv, to):
        return pltpu.make_async_remote_copy(
            src_ref=src, dst_ref=dst, send_sem=send, recv_sem=recv,
            device_id=to, device_id_type=pl.DeviceIdType.MESH,
        )

    load_img = pltpu.make_async_copy(img_hbm, img_v, load.at[0])
    load_noise = pltpu.make_async_copy(noise_hbm, noise_v, load.at[1])

    load_proj = pltpu.make_async_copy(
        proj_hbm.at[pl.ds(x * PARTS, WHOLE)], pbuf.at[0, pl.ds(0, WHOLE)], load.at[2]
    )
    load_rest = pltpu.make_async_copy(
        proj_hbm.at[pl.ds((x % (NX - 1)) * PARTS + WHOLE, PARTS - WHOLE)],
        pbuf.at[0, pl.ds(WHOLE, PARTS - WHOLE)], load.at[3],
    )
    load_img.start()
    load_proj.start()

    @pl.when(x < NX - 1)
    def _():
        load_rest.start()

    load_noise.start()

    barrier = pltpu.get_barrier_semaphore()
    partners = [group(s // 2, s % 2) for s in range(1, 2 * NX)]
    partners += [along_y(1), along_y(NY - 1), along_z(1), along_z(NZ - 1)]
    for d in (2, 4, 6):
        for e in range(NX):
            partners += [device((y + d) % NY, z, (x + e) % NX, c)]
            partners += [device(y, (z + d) % NZ, (x + e) % NX, c)]
    for to in partners:
        pl.semaphore_signal(barrier, inc=1, device_id=to, device_id_type=pl.DeviceIdType.MESH)

    tag = lax.broadcasted_iota(jnp.int32, (TAG, ROWS), 0)
    is_group = (tag < 96) & (tag % 32 == group_ref[...])
    is_offset = (tag >= 96) & (tag < 108) & (tag % 4 == offset_ref[...])
    tags = jnp.transpose(jnp.where(is_group | is_offset, 1.0, 0.0).astype(f32)).astype(bf16)
    load_img.wait()
    for k in range(NX):
        end = min(F, W * (k + 1))
        img_ref[k, :, : end - W * k] = img_v[:, W * k : end]
        if end - W * k < W:
            img_ref[k, :, end - W * k : W] = jnp.zeros((ROWS, W * (k + 1) - end), bf16)
        img_ref[k, :, W:] = tags
    load_proj.wait()

    @pl.when(x < NX - 1)
    def _():
        load_rest.wait()

    @pl.when(x == NX - 1)
    def _():
        pbuf[0, WHOLE:] = jnp.zeros((PARTS - WHOLE, CHUNK, BLOCK), bf16)

    pl.semaphore_wait(barrier, len(partners))

    def turned(m, low):
        return (m + 2 * low) % CHUNKS

    def to_across(m):
        mine = half * CHUNKS + turned(m, 1 - lo)
        src, dst = (pbuf.at[0, mine], pbuf.at[1, mine])
        if m >= CHUNKS:
            src, dst = (pbuf.at[2, mine], pbuf.at[3, mine])
        return copy(src, dst, cross_s.at[m], cross_r.at[m], across)

    def from_across(m):
        return pbuf.at[1 if m < CHUNKS else 3, half * CHUNKS + turned(m, lo)]

    def to_beside(m):
        dst = pbuf.at[2 if m < CHUNKS else 3, half * CHUNKS + turned(m, lo)]
        return copy(from_across(m), dst, pair_s.at[m], pair_r.at[m], beside)

    def from_beside(m):
        return pbuf.at[2 if m < CHUNKS else 3, half * CHUNKS + turned(m, 1 - lo)]

    def to_side(way, m):
        ref = from_across(m) if way == 0 else from_beside(m)
        up = 1 - 2 * (turned(m, lo if way == 0 else 1 - lo) // 2)
        to = device(y, (z + NZ + up) % NZ, x, c)
        return copy(ref, ref, side_s.at[way, m], side_r.at[way, m], to)

    def sided(way, m):
        chunk = (1 - half) * CHUNKS + turned(m, lo if way == 0 else 1 - lo)
        ref = pbuf.at[(1 + way) if m < CHUNKS else 3, chunk]
        copy(ref, ref, side_s.at[way, m], side_r.at[way, m], along_z(1)).wait_recv()

    def crossed(m):
        ref = from_across(m)
        copy(ref, ref, cross_s.at[m], cross_r.at[m], across).wait_recv()
        to_beside(m).start()
        to_side(0, m).start()

    def paired(m):
        ref = from_beside(m)
        copy(ref, ref, pair_s.at[m], pair_r.at[m], beside).wait_recv()
        if m < 2:
            to_across(CHUNKS + m).start()
        to_side(1, m).start()

    def image(p):
        return copy(
            img_ref.at[(x + STEPS[p]) % NX], xin.at[2 * p], img_s.at[2 * p], img_r.at[2 * p],
            group(STEPS[p], 0),
        )

    def to_sibling(p):
        src = img_ref.at[x] if p == 0 else xin.at[2 * p]
        s = 2 * p + 1
        return copy(src, xin.at[s], img_s.at[s], img_r.at[s], group(0, 1))

    for m in range(CHUNKS):
        to_across(m).start()
    for p in (1, 2, 3):
        image(p).start()
    to_sibling(0).start()

    xin[0] = img_ref[x]
    load_noise.wait()

    def pieces(inv, width):
        hi = inv.astype(bf16)
        rest = inv - hi.astype(f32)
        mid = rest.astype(bf16)
        low = (rest - mid.astype(f32)).astype(bf16)
        inv3[0:GROUPS, :width] = hi
        inv3[GROUPS : 2 * GROUPS, :width] = mid
        inv3[2 * GROUPS : 3 * GROUPS, :width] = low

    inv3[3 * GROUPS :] = jnp.zeros((TAG - 3 * GROUPS, W), bf16)

    @pl.when(x < NX - 1)
    def _():
        pieces(1.0 / noise_v[:, pl.ds(pl.multiple_of(x * W, 128), W)], W)

    @pl.when(x == NX - 1)
    def _():
        pieces(1.0 / noise_v[:, F - LAST :], LAST)
        inv3[: 3 * GROUPS, LAST:] = jnp.zeros((3 * GROUPS, W - LAST), bf16)

    row = lax.broadcasted_iota(jnp.int32, (TAG, BLOCK), 0)
    piece = jnp.where(row < 96, row // 32, jnp.minimum((row - 96) // 4, 3))

    def block_of(slot):
        return pbuf[slot].reshape(W, BLOCK)

    def columns(slot):
        p = block_of(slot).astype(f32)
        square = p * p
        s_hi = square.astype(bf16)
        s_lo = (square - s_hi.astype(f32)).astype(bf16)
        q = lax.dot_general(inv3[...], s_hi, NN, preferred_element_type=f32)
        q += lax.dot_general(inv3[...], s_lo, NN, preferred_element_type=f32)
        q = q[0:32] + q[32:64] + q[64:96]
        prior = jnp.zeros((TAG, BLOCK), f32)
        for o in range(CLASSES):
            log_prior = prior_ref[0, (h + turn[slot] + CLASSES - o) % CLASSES]
            prior = jnp.where(row % CLASSES == o, log_prior * (1.0 / NX), prior)
        value = jnp.where(row < 96, -0.5 * jnp.concatenate([q] * 4, axis=0), prior)
        v_hi = value.astype(bf16).astype(f32)
        v_mid = (value - v_hi).astype(bf16).astype(f32)
        v_lo = value - v_hi - v_mid
        both = jnp.where(piece == 2, v_lo, 0.0)
        both = jnp.where(piece == 1, v_mid, both)
        qbuf[slot] = jnp.where(piece == 0, v_hi, both).astype(bf16)

    def image_arrived(p):
        image(p).wait_recv()
        to_sibling(p).start()

    def score_copy(slot, s):
        return copy(
            sc_send.at[slot, s], sc_recv.at[slot, s], sc_s.at[slot, s], sc_r.at[slot, s],
            group((NX - STEPS[s // 2]) % NX, s % 2),
        )

    def scores(slot, first, last):
        rows = (last - first) * ROWS
        part = lax.dot_general(
            white[first:last].reshape(rows, W), block_of(slot), NN, preferred_element_type=f32
        )
        part += lax.dot_general(
            xin[first:last, :, W:].reshape(rows, TAG), qbuf[slot], NN, preferred_element_type=f32
        )
        sc_send[slot, first:last] = part.reshape(last - first, ROWS, BLOCK)
        for s in (6, 7, 2, 4, 3, 5, 1):
            if first <= s < last:
                score_copy(slot, s).start()

    def whiten(s):
        inverse = jnp.dot(xin[s, :, W:], inv3[...], preferred_element_type=f32)
        white[s] = (xin[s, :, :W].astype(f32) * inverse).astype(bf16)

    whiten(0)
    columns(0)
    crossed(0)
    crossed(1)
    crossed(2)
    paired(0)
    crossed(3)
    paired(1)
    image_arrived(1)
    image_arrived(2)
    whiten(2)
    whiten(4)
    paired(2)
    crossed(4)
    for s in (1, 3, 5):
        to_sibling(s // 2).wait_recv()
        whiten(s)
    paired(3)
    scores(0, 0, EARLY)
    crossed(5)
    for m in range(CHUNKS):
        sided(0, m)
    columns(1)
    scores(1, 0, EARLY)
    paired(4)
    image_arrived(3)
    whiten(6)
    for m in range(CHUNKS):
        sided(1, m)
    columns(2)
    paired(5)
    to_sibling(3).wait_recv()
    whiten(7)
    scores(0, EARLY, 2 * NX)
    scores(1, EARLY, 2 * NX)
    scores(2, 0, 2 * NX)
    for m in (CHUNKS, CHUNKS + 1):
        sided(0, m)
        sided(1, m)
    columns(3)
    scores(3, 0, 2 * NX)

    total = {}
    for slot in range(4):
        for s in range(1, 2 * NX):
            score_copy(slot, s).wait_recv()
        for dc in (0, 1):
            terms = [sc_send[slot, 0]] if dc == 0 else [sc_recv[slot, 1]]
            terms += [sc_recv[slot, 2 * dx + dc] for dx in range(1, NX)]
            total[slot, dc] = (terms[0] + terms[1]) + (terms[2] + terms[3])
    peak = None
    for value in total.values():
        peak = value if peak is None else jnp.maximum(peak, value)
    peak = jnp.max(peak, axis=1, keepdims=True)
    mass = None
    for value in total.values():
        term = jnp.exp(value - peak)
        mass = term if mass is None else mass + term
    evidence = peak + jnp.log(jnp.sum(mass, axis=1, keepdims=True))
    ev_ref[...] = jnp.transpose(jnp.broadcast_to(evidence, (ROWS, TAG)))[0:1, :]
    for (slot, dc), value in total.items():
        post_send[dc, slot] = jnp.exp(value - evidence).astype(bf16)

    def post_copy(s):
        return copy(
            post_send.at[s % 2], post_recv.at[s], post_s.at[s], post_r.at[s],
            group(STEPS[s // 2], s % 2),
        )

    for s in (6, 7, 2, 4, 3, 5, 1):
        post_copy(s).start()
    post_recv[0] = post_send[0]
    for s in (1, 2, 4, 3, 5, 6, 7):
        post_copy(s).wait_recv()

    for slot in range(4):
        wt[BLOCK * slot : BLOCK * (slot + 1)] = jnp.transpose(post_recv[:, slot].reshape(ALL, BLOCK))

    place = {"z": z, "y": y}
    other = {"z": "y", "y": "z"}

    def along(axis, d):
        at = (place[axis] + d + 8) % 8
        return device(y, at, x, c) if axis == "z" else device(at, z, x, c)

    def near(axis, side):
        return along(axis, side * (1 - 2 * (place[axis] % 2)))

    def stage1(i):
        axis, side = STREAMS[i][:2]
        return copy(
            parts[i].at[1 - place[axis] % 2], in1[i], st_s.at[0, i], st_r.at[0, i], near(axis, side)
        )

    def stage2(i):
        axis, side = STREAMS[i][:2]
        return copy(
            mid1[i].at[1 - place[other[axis]] % 2], in2[i], st_s.at[1, i], st_r.at[1, i],
            near(other[axis], side),
        )

    def stage3(i, d):
        axis = STREAMS[i][0]
        return copy(
            mid2[i].at[(place[axis] // 2 + d) % 4], in3[i].at[d - 1], st_s.at[1 + d, i],
            st_r.at[1 + d, i], along(axis, 2 * d),
        )

    def last(axis, d, e):
        n = "zy".index(axis)
        at = (place[other[axis]] + 2 * d) % 8
        to = device(at, z, (x + e) % NX, c) if axis == "z" else device(y, at, (x + e) % NX, c)
        return copy(
            own[n].at[(place[other[axis]] // 2 + d) % 4, (x + e) % NX], got[n].at[d, x],
            own_s.at[n, 4 * d + e], own_r.at[n, 4 * d + e], to,
        )

    def last_in(axis, d, e):
        n = "zy".index(axis)
        ref = got[n].at[d, (x + NX - e) % NX]
        return copy(ref, ref, own_s.at[n, 4 * d + e], own_r.at[n, 4 * d + e], group(1, 0))

    order = range(len(STREAMS))
    for i in order:
        axis, _, col, width = STREAMS[i]
        part = jnp.dot(
            wt[...], white[:, :, col : col + width].reshape(ALL, width), preferred_element_type=f32
        ).astype(bf16)
        for slot in range(4):
            y_half = (h + turn[slot]) % 4
            for r in range(2 * NZ):
                low, z_ = r // NZ, r % NZ
                at = BLOCK * slot + OWN * r
                if axis == "z":
                    parts[i][z_ % 2, low, z_ // 2, y_half] = part[at : at + OWN]
                else:
                    parts[i][low, z_ % 2, y_half, z_ // 2] = part[at : at + OWN]
        stage1(i).start()
    for i in order:
        axis = STREAMS[i][0]
        stage1(i).wait_recv()
        total = parts[i][place[axis] % 2].astype(f32) + in1[i][...].astype(f32)
        mid1[i][...] = total.astype(bf16)
        stage2(i).start()
    for i in order:
        axis = STREAMS[i][0]
        stage2(i).wait_recv()
        total = mid1[i][place[other[axis]] % 2].astype(f32) + in2[i][...].astype(f32)
        mid2[i][...] = total.astype(bf16)
        for d in (2, 1, 3):
            stage3(i, d).start()
    far_first = [(d, e) for d in (2, 1, 3, 0) for e in (2, 1, 3, 0) if d or e]
    for axis in "zy":
        n = "zy".index(axis)
        for i in order:
            if STREAMS[i][0] != axis:
                continue
            _, _, col, width = STREAMS[i]
            col -= WA * n
            acc = mid2[i][place[axis] // 2].astype(f32)
            for d in (1, 3, 2):
                stage3(i, d).wait_recv()
                acc += in3[i][d - 1].astype(f32)
            for k in range(NX):
                own[n][:, k, :, col : col + width] = acc[:, 2 * k : 2 * k + 2].astype(bf16)
        for d, e in far_first:
            last(axis, d, e).start()
        got[n][0, x] = own[n][place[other[axis]] // 2, x]
    for axis in "zy":
        n = "zy".index(axis)
        for d, e in reversed(far_first):
            last_in(axis, d, e).wait_recv()
        acc = got[n][0].astype(f32)
        for d in range(1, 4):
            acc += got[n][d].astype(f32)
        out_ref[:, :, WA * n : WA * n + (WA, WB)[n]] = acc

    for m in range(6):
        to_across(m).wait_send()
        to_beside(m).wait_send()
        to_side(0, m).wait_send()
        to_side(1, m).wait_send()
    for p in range(NX):
        if p:
            image(p).wait_send()
        to_sibling(p).wait_send()
    for s in range(1, 2 * NX):
        for slot in range(4):
            score_copy(slot, s).wait_send()
        post_copy(s).wait_send()
    for i in order:
        stage1(i).wait_send()
        stage2(i).wait_send()
        for d in (1, 2, 3):
            stage3(i, d).wait_send()
    for d, e in far_first:
        last("z", d, e).wait_send()
        last("y", d, e).wait_send()


def body(images, projections, noise_power, class_logprior, groups, offsets):
    dma = pltpu.SemaphoreType.DMA
    anywhere = pl.BlockSpec(memory_space=pl.ANY)
    vmem = pl.BlockSpec(memory_space=pltpu.VMEM)
    out, evidence = pl.pallas_call(
        kernel,
        out_shape=(
            jax.ShapeDtypeStruct((NX, 2, W), f32),
            jax.ShapeDtypeStruct((1, ROWS), f32),
        ),
        in_specs=[anywhere] * 3 + [pl.BlockSpec(memory_space=pltpu.SMEM), vmem, vmem],
        out_specs=(vmem, vmem),
        scratch_shapes=[
            pltpu.VMEM((ROWS, F), bf16),
            pltpu.VMEM((GROUPS, F), f32),
            pltpu.VMEM((NX, ROWS, W + TAG), bf16),
            pltpu.VMEM((2 * NX, ROWS, W + TAG), bf16),
            pltpu.VMEM((2 * NX, ROWS, W), bf16),
            pltpu.VMEM((TAG, W), bf16),
            pltpu.VMEM((4, PARTS, CHUNK, BLOCK), bf16),
            pltpu.VMEM((4, TAG, BLOCK), bf16),
            pltpu.VMEM((4, 2 * NX, ROWS, BLOCK), f32),
            pltpu.VMEM((4, 2 * NX, ROWS, BLOCK), f32),
            pltpu.VMEM((2, 4, ROWS, BLOCK), bf16),
            pltpu.VMEM((2 * NX, 4, ROWS, BLOCK), bf16),
            pltpu.VMEM((4 * BLOCK, ALL), bf16),
            [pltpu.VMEM((2, 2, 4, 4, OWN, t[3]), bf16) for t in STREAMS],
            [pltpu.VMEM((2, 4, 4, OWN, t[3]), bf16) for t in STREAMS],
            [pltpu.VMEM((2, 4, 4, OWN, t[3]), bf16) for t in STREAMS],
            [pltpu.VMEM((4, 4, OWN, t[3]), bf16) for t in STREAMS],
            [pltpu.VMEM((4, 4, OWN, t[3]), bf16) for t in STREAMS],
            [pltpu.VMEM((3, 4, OWN, t[3]), bf16) for t in STREAMS],
            [pltpu.VMEM((4, NX, 2, t), bf16) for t in (WA, WB)],
            [pltpu.VMEM((4, NX, 2, t), bf16) for t in (WA, WB)],
            dma((4,)),
            dma((2 * NX,)), dma((2 * NX,)),
            dma((6,)), dma((6,)),
            dma((6,)), dma((6,)),
            dma((2, 6)), dma((2, 6)),
            dma((4, 2 * NX)), dma((4, 2 * NX)),
            dma((2 * NX,)), dma((2 * NX,)),
            dma((5, len(STREAMS))), dma((5, len(STREAMS))),
            dma((2, 16)), dma((2, 16)),
        ],
        compiler_params=pltpu.CompilerParams(
            collective_id=0, has_side_effects=True, vmem_limit_bytes=58 * 1024 * 1024
        ),
        name="estep",
    )(
        images, projections.T.reshape(F // CHUNK, CHUNK, BLOCK), noise_power, class_logprior.reshape(1, CLASSES),
        groups.reshape(1, ROWS), offsets.reshape(1, ROWS),
    )
    out, evidence = pl.pallas_call(
        finish,
        out_shape=(
            jax.ShapeDtypeStruct((2, F), f32),
            jax.ShapeDtypeStruct((1, ROWS), f32),
        ),
        in_specs=[vmem, vmem],
        out_specs=(vmem, vmem),
        name="finish",
    )(out, evidence)
    return (out, evidence.reshape(ROWS))


def solution(mesh):
    in_specs = (
        P(("cls", "img"), None),
        P("cls", None),
        P(),
        P(),
        P(("cls", "img")),
        P(("cls", "img")),
    )
    out_specs = (P(("cls", "img"), None), P(("cls", "img")))
    return jax.shard_map(body, mesh=mesh, in_specs=in_specs, out_specs=out_specs, check_vma=False)
```

```python
import jax
import jax.numpy as jnp
from jax import lax
from jax.experimental import pallas as pl
from jax.experimental.pallas import tpu as pltpu
from jax.sharding import PartitionSpec as P

NX, NY, NZ = 4, 8, 8
F = 7200
W = 1920
TAG = 128
ROWS = 56
ALL = 2 * NX * ROWS
BLOCK = 128
CHUNKS = 4
PARTS = 2 * CHUNKS
CHUNK = W // PARTS
WHOLE = F // CHUNK - (NX - 1) * PARTS
STEPS = (0, 1, 3, 2)
EARLY = 6
LAST = F - (NX - 1) * W
WA = 1024
WB = W - WA
GROUPS = 32
CLASSES = 4
OWN = 8
STREAMS = (
    ("z", 1, 0, 256), ("z", -1, 256, 256), ("y", 1, 1024, 256), ("y", -1, 1280, 256),
    ("z", 1, 512, 256), ("z", -1, 768, 256), ("y", 1, 1536, 256), ("y", -1, 1792, 128),
)
NN = (((1,), (0,)), ((), ()))
f32 = jnp.float32
bf16 = jnp.bfloat16


def finish(fin_ref, ev_ref, out_ref, evidence_ref):
    for k in range(NX):
        end = min(F, W * (k + 1))
        out_ref[:, W * k : end] = fin_ref[k, :, : end - W * k]
    evidence_ref[...] = ev_ref[...]


def kernel(
    img_hbm, proj_hbm, noise_hbm, prior_ref, group_ref, offset_ref, out_ref, ev_ref,
    img_v, noise_v, img_ref, xin, white, inv3, pbuf, qbuf, sc_send, sc_recv, post_send, post_recv,
    wt, parts, in1, mid1, in2, mid2, in3, own, got,
    near_up, near_down, load, img_s, img_r, cross_s, cross_r, pair_s, pair_r, side_s, side_r, sc_s, sc_r, post_s, post_r,
    st_s, st_r, own_s, own_r,
):
    cls = lax.axis_index("cls")
    img = lax.axis_index("img")
    h, c = cls // 2, cls % 2
    lo, z, x = img // (NZ * NX), (img // NX) % NZ, img % NX
    y = 2 * h + lo
    turn = (0, 3 - 2 * lo, 1 + 2 * lo, 2)
    half = z % 2

    def device(y_, z_, x_, c_):
        return {"cls": (y_ // 2) * 2 + c_, "img": ((y_ % 2) * NZ + z_) * NX + x_}

    def group(dx, dc):
        return device(y, z, (x + dx) % NX, (c + dc) % 2)

    def along_y(d):
        return device((y + d) % NY, z, x, c)

    def along_z(d):
        return device(y, (z + d) % NZ, x, c)

    across = device((y + NY - 1 + 2 * lo) % NY, z, x, c)
    beside = device(y + 1 - 2 * lo, z, x, c)

    def copy(src, dst, send, recv, to):
        return pltpu.make_async_remote_copy(
            src_ref=src, dst_ref=dst, send_sem=send, recv_sem=recv,
            device_id=to, device_id_type=pl.DeviceIdType.MESH,
        )

    load_img = pltpu.make_async_copy(img_hbm, img_v, load.at[0])
    load_noise = pltpu.make_async_copy(noise_hbm, noise_v, load.at[1])

    load_proj = pltpu.make_async_copy(
        proj_hbm.at[pl.ds(x * PARTS, WHOLE)], pbuf.at[0, pl.ds(0, WHOLE)], load.at[2]
    )
    load_rest = pltpu.make_async_copy(
        proj_hbm.at[pl.ds((x % (NX - 1)) * PARTS + WHOLE, PARTS - WHOLE)],
        pbuf.at[0, pl.ds(WHOLE, PARTS - WHOLE)], load.at[3],
    )
    load_img.start()
    load_proj.start()

    @pl.when(x < NX - 1)
    def _():
        load_rest.start()

    load_noise.start()

    barrier = pltpu.get_barrier_semaphore()
    partners = [group(s // 2, s % 2) for s in range(1, 2 * NX)]
    partners += [along_y(1), along_y(NY - 1), along_z(1), along_z(NZ - 1)]
    for to in partners:
        pl.semaphore_signal(barrier, inc=1, device_id=to, device_id_type=pl.DeviceIdType.MESH)

    tag = lax.broadcasted_iota(jnp.int32, (TAG, ROWS), 0)
    is_group = (tag < 96) & (tag % 32 == group_ref[...])
    is_offset = (tag >= 96) & (tag < 108) & (tag % 4 == offset_ref[...])
    tags = jnp.transpose(jnp.where(is_group | is_offset, 1.0, 0.0).astype(f32)).astype(bf16)
    load_img.wait()
    for k in range(NX):
        end = min(F, W * (k + 1))
        img_ref[k, :, : end - W * k] = img_v[:, W * k : end]
        if end - W * k < W:
            img_ref[k, :, end - W * k : W] = jnp.zeros((ROWS, W * (k + 1) - end), bf16)
        img_ref[k, :, W:] = tags
    load_proj.wait()

    @pl.when(x < NX - 1)
    def _():
        load_rest.wait()

    @pl.when(x == NX - 1)
    def _():
        pbuf[0, WHOLE:] = jnp.zeros((PARTS - WHOLE, CHUNK, BLOCK), bf16)

    pl.semaphore_wait(barrier, len(partners))

    def turned(m, low):
        return (m + 2 * low) % CHUNKS

    def to_across(m):
        mine = half * CHUNKS + turned(m, 1 - lo)
        src, dst = (pbuf.at[0, mine], pbuf.at[1, mine])
        if m >= CHUNKS:
            src, dst = (pbuf.at[2, mine], pbuf.at[3, mine])
        return copy(src, dst, cross_s.at[m], cross_r.at[m], across)

    def from_across(m):
        return pbuf.at[1 if m < CHUNKS else 3, half * CHUNKS + turned(m, lo)]

    def to_beside(m):
        dst = pbuf.at[2 if m < CHUNKS else 3, half * CHUNKS + turned(m, lo)]
        return copy(from_across(m), dst, pair_s.at[m], pair_r.at[m], beside)

    def from_beside(m):
        return pbuf.at[2 if m < CHUNKS else 3, half * CHUNKS + turned(m, 1 - lo)]

    def to_side(way, m):
        ref = from_across(m) if way == 0 else from_beside(m)
        up = 1 - 2 * (turned(m, lo if way == 0 else 1 - lo) // 2)
        to = device(y, (z + NZ + up) % NZ, x, c)
        return copy(ref, ref, side_s.at[way, m], side_r.at[way, m], to)

    def sided(way, m):
        chunk = (1 - half) * CHUNKS + turned(m, lo if way == 0 else 1 - lo)
        ref = pbuf.at[(1 + way) if m < CHUNKS else 3, chunk]
        copy(ref, ref, side_s.at[way, m], side_r.at[way, m], along_z(1)).wait_recv()

    def crossed(m):
        ref = from_across(m)
        copy(ref, ref, cross_s.at[m], cross_r.at[m], across).wait_recv()
        to_beside(m).start()
        to_side(0, m).start()

    def paired(m):
        ref = from_beside(m)
        copy(ref, ref, pair_s.at[m], pair_r.at[m], beside).wait_recv()
        if m < 2:
            to_across(CHUNKS + m).start()
        to_side(1, m).start()

    def image(p):
        return copy(
            img_ref.at[(x + STEPS[p]) % NX], xin.at[2 * p], img_s.at[2 * p], img_r.at[2 * p],
            group(STEPS[p], 0),
        )

    def to_sibling(p):
        src = img_ref.at[x] if p == 0 else xin.at[2 * p]
        s = 2 * p + 1
        return copy(src, xin.at[s], img_s.at[s], img_r.at[s], group(0, 1))

    def tell(r):
        for n, at in ((0, along_y), (1, along_z)):
            pl.semaphore_signal(
                near_up.at[n, r - 1], inc=1, device_id=at(1), device_id_type=pl.DeviceIdType.MESH
            )
            if r <= 2:
                pl.semaphore_signal(
                    near_down.at[n, r - 1], inc=1, device_id=at(7),
                    device_id_type=pl.DeviceIdType.MESH,
                )

    def told(r):
        for n in (0, 1):
            pl.semaphore_wait(near_up.at[n, r - 1], 1)
            if r <= 2:
                pl.semaphore_wait(near_down.at[n, r - 1], 1)
        if r < 4:
            tell(r + 1)

    for m in range(CHUNKS):
        to_across(m).start()
    tell(1)
    for p in (1, 2, 3):
        image(p).start()
    to_sibling(0).start()

    xin[0] = img_ref[x]
    load_noise.wait()

    def pieces(inv, width):
        hi = inv.astype(bf16)
        rest = inv - hi.astype(f32)
        mid = rest.astype(bf16)
        low = (rest - mid.astype(f32)).astype(bf16)
        inv3[0:GROUPS, :width] = hi
        inv3[GROUPS : 2 * GROUPS, :width] = mid
        inv3[2 * GROUPS : 3 * GROUPS, :width] = low

    inv3[3 * GROUPS :] = jnp.zeros((TAG - 3 * GROUPS, W), bf16)

    @pl.when(x < NX - 1)
    def _():
        pieces(1.0 / noise_v[:, pl.ds(pl.multiple_of(x * W, 128), W)], W)

    @pl.when(x == NX - 1)
    def _():
        pieces(1.0 / noise_v[:, F - LAST :], LAST)
        inv3[: 3 * GROUPS, LAST:] = jnp.zeros((3 * GROUPS, W - LAST), bf16)

    row = lax.broadcasted_iota(jnp.int32, (TAG, BLOCK), 0)
    piece = jnp.where(row < 96, row // 32, jnp.minimum((row - 96) // 4, 3))

    def block_of(slot):
        return pbuf[slot].reshape(W, BLOCK)

    def columns(slot):
        p = block_of(slot).astype(f32)
        square = p * p
        s_hi = square.astype(bf16)
        s_lo = (square - s_hi.astype(f32)).astype(bf16)
        q = lax.dot_general(inv3[...], s_hi, NN, preferred_element_type=f32)
        q += lax.dot_general(inv3[...], s_lo, NN, preferred_element_type=f32)
        q = q[0:32] + q[32:64] + q[64:96]
        prior = jnp.zeros((TAG, BLOCK), f32)
        for o in range(CLASSES):
            log_prior = prior_ref[0, (h + turn[slot] + CLASSES - o) % CLASSES]
            prior = jnp.where(row % CLASSES == o, log_prior * (1.0 / NX), prior)
        value = jnp.where(row < 96, -0.5 * jnp.concatenate([q] * 4, axis=0), prior)
        v_hi = value.astype(bf16).astype(f32)
        v_mid = (value - v_hi).astype(bf16).astype(f32)
        v_lo = value - v_hi - v_mid
        both = jnp.where(piece == 2, v_lo, 0.0)
        both = jnp.where(piece == 1, v_mid, both)
        qbuf[slot] = jnp.where(piece == 0, v_hi, both).astype(bf16)

    def image_arrived(p):
        image(p).wait_recv()
        to_sibling(p).start()

    def score_copy(slot, s):
        return copy(
            sc_send.at[slot, s], sc_recv.at[slot, s], sc_s.at[slot, s], sc_r.at[slot, s],
            group((NX - STEPS[s // 2]) % NX, s % 2),
        )

    def scores(slot, first, last):
        rows = (last - first) * ROWS
        part = lax.dot_general(
            white[first:last].reshape(rows, W), block_of(slot), NN, preferred_element_type=f32
        )
        part += lax.dot_general(
            xin[first:last, :, W:].reshape(rows, TAG), qbuf[slot], NN, preferred_element_type=f32
        )
        sc_send[slot, first:last] = part.reshape(last - first, ROWS, BLOCK)
        for s in (6, 7, 2, 4, 3, 5, 1):
            if first <= s < last:
                score_copy(slot, s).start()

    def whiten(s):
        inverse = jnp.dot(xin[s, :, W:], inv3[...], preferred_element_type=f32)
        white[s] = (xin[s, :, :W].astype(f32) * inverse).astype(bf16)

    whiten(0)
    columns(0)
    crossed(0)
    crossed(1)
    told(1)
    crossed(2)
    paired(0)
    crossed(3)
    told(2)
    image_arrived(1)
    image_arrived(2)
    paired(1)
    whiten(2)
    whiten(4)
    for s in (1, 3, 5):
        to_sibling(s // 2).wait_recv()
        whiten(s)
    paired(2)
    scores(0, 0, EARLY)
    crossed(4)
    paired(3)
    for m in range(CHUNKS):
        sided(0, m)
    crossed(5)
    columns(1)
    scores(1, 0, EARLY)
    paired(4)
    image_arrived(3)
    whiten(6)
    for m in range(CHUNKS):
        sided(1, m)
    columns(2)
    paired(5)
    told(3)
    to_sibling(3).wait_recv()
    whiten(7)
    scores(0, EARLY, 2 * NX)
    scores(1, EARLY, 2 * NX)
    scores(2, 0, 2 * NX)
    for m in (CHUNKS, CHUNKS + 1):
        sided(0, m)
        sided(1, m)
    told(4)
    columns(3)
    scores(3, 0, 2 * NX)

    total = {}
    for slot in range(4):
        for s in range(1, 2 * NX):
            score_copy(slot, s).wait_recv()
        for dc in (0, 1):
            terms = [sc_send[slot, 0]] if dc == 0 else [sc_recv[slot, 1]]
            terms += [sc_recv[slot, 2 * dx + dc] for dx in range(1, NX)]
            total[slot, dc] = (terms[0] + terms[1]) + (terms[2] + terms[3])
    peak = None
    for value in total.values():
        peak = value if peak is None else jnp.maximum(peak, value)
    peak = jnp.max(peak, axis=1, keepdims=True)
    mass = None
    for value in total.values():
        term = jnp.exp(value - peak)
        mass = term if mass is None else mass + term
    evidence = peak + jnp.log(jnp.sum(mass, axis=1, keepdims=True))
    ev_ref[...] = jnp.transpose(jnp.broadcast_to(evidence, (ROWS, TAG)))[0:1, :]
    for (slot, dc), value in total.items():
        post_send[dc, slot] = jnp.exp(value - evidence).astype(bf16)

    def post_copy(s):
        return copy(
            post_send.at[s % 2], post_recv.at[s], post_s.at[s], post_r.at[s],
            group(STEPS[s // 2], s % 2),
        )

    for s in (6, 7, 2, 4, 3, 5, 1):
        post_copy(s).start()
    post_recv[0] = post_send[0]
    for s in (1, 2, 4, 3, 5, 6, 7):
        post_copy(s).wait_recv()

    for slot in range(4):
        wt[BLOCK * slot : BLOCK * (slot + 1)] = jnp.transpose(post_recv[:, slot].reshape(ALL, BLOCK))

    place = {"z": z, "y": y}
    other = {"z": "y", "y": "z"}

    def along(axis, d):
        at = (place[axis] + d + 8) % 8
        return device(y, at, x, c) if axis == "z" else device(at, z, x, c)

    def near(axis, side):
        return along(axis, side * (1 - 2 * (place[axis] % 2)))

    def stage1(i):
        axis, side = STREAMS[i][:2]
        return copy(
            parts[i].at[1 - place[axis] % 2], in1[i], st_s.at[0, i], st_r.at[0, i], near(axis, side)
        )

    def stage2(i):
        axis, side = STREAMS[i][:2]
        return copy(
            mid1[i].at[1 - place[other[axis]] % 2], in2[i], st_s.at[1, i], st_r.at[1, i],
            near(other[axis], side),
        )

    def stage3(i, d):
        axis = STREAMS[i][0]
        return copy(
            mid2[i].at[(place[axis] // 2 + d) % 4], in3[i].at[d - 1], st_s.at[1 + d, i],
            st_r.at[1 + d, i], along(axis, 2 * d),
        )

    def last(axis, d, e):
        n = "zy".index(axis)
        at = (place[other[axis]] + 2 * d) % 8
        to = device(at, z, (x + e) % NX, c) if axis == "z" else device(y, at, (x + e) % NX, c)
        return copy(
            own[n].at[(place[other[axis]] // 2 + d) % 4, (x + e) % NX], got[n].at[d, x],
            own_s.at[n, 4 * d + e], own_r.at[n, 4 * d + e], to,
        )

    def last_in(axis, d, e):
        n = "zy".index(axis)
        ref = got[n].at[d, (x + NX - e) % NX]
        return copy(ref, ref, own_s.at[n, 4 * d + e], own_r.at[n, 4 * d + e], group(1, 0))

    order = range(len(STREAMS))
    for i in order:
        axis, _, col, width = STREAMS[i]
        part = jnp.dot(
            wt[...], white[:, :, col : col + width].reshape(ALL, width), preferred_element_type=f32
        ).astype(bf16)
        for slot in range(4):
            y_half = (h + turn[slot]) % 4
            for r in range(2 * NZ):
                low, z_ = r // NZ, r % NZ
                at = BLOCK * slot + OWN * r
                if axis == "z":
                    parts[i][z_ % 2, low, z_ // 2, y_half] = part[at : at + OWN]
                else:
                    parts[i][low, z_ % 2, y_half, z_ // 2] = part[at : at + OWN]
        stage1(i).start()
    for i in order:
        axis = STREAMS[i][0]
        stage1(i).wait_recv()
        total = parts[i][place[axis] % 2].astype(f32) + in1[i][...].astype(f32)
        mid1[i][...] = total.astype(bf16)
        stage2(i).start()
    for i in order:
        axis = STREAMS[i][0]
        stage2(i).wait_recv()
        total = mid1[i][place[other[axis]] % 2].astype(f32) + in2[i][...].astype(f32)
        mid2[i][...] = total.astype(bf16)
        for d in (2, 1, 3):
            stage3(i, d).start()
    far_first = [(d, e) for d in (2, 1, 3, 0) for e in (2, 1, 3, 0) if d or e]
    for axis in "zy":
        n = "zy".index(axis)
        for i in order:
            if STREAMS[i][0] != axis:
                continue
            _, _, col, width = STREAMS[i]
            col -= WA * n
            acc = mid2[i][place[axis] // 2].astype(f32)
            for d in (1, 3, 2):
                stage3(i, d).wait_recv()
                acc += in3[i][d - 1].astype(f32)
            for k in range(NX):
                own[n][:, k, :, col : col + width] = acc[:, 2 * k : 2 * k + 2].astype(bf16)
        for d, e in far_first:
            last(axis, d, e).start()
        got[n][0, x] = own[n][place[other[axis]] // 2, x]
    for axis in "zy":
        n = "zy".index(axis)
        for d, e in reversed(far_first):
            last_in(axis, d, e).wait_recv()
        acc = got[n][0].astype(f32)
        for d in range(1, 4):
            acc += got[n][d].astype(f32)
        out_ref[:, :, WA * n : WA * n + (WA, WB)[n]] = acc

    for m in range(6):
        to_across(m).wait_send()
        to_beside(m).wait_send()
        to_side(0, m).wait_send()
        to_side(1, m).wait_send()
    for p in range(NX):
        if p:
            image(p).wait_send()
        to_sibling(p).wait_send()
    for s in range(1, 2 * NX):
        for slot in range(4):
            score_copy(slot, s).wait_send()
        post_copy(s).wait_send()
    for i in order:
        stage1(i).wait_send()
        stage2(i).wait_send()
        for d in (1, 2, 3):
            stage3(i, d).wait_send()
    for d, e in far_first:
        last("z", d, e).wait_send()
        last("y", d, e).wait_send()


def body(images, projections, noise_power, class_logprior, groups, offsets):
    dma = pltpu.SemaphoreType.DMA
    anywhere = pl.BlockSpec(memory_space=pl.ANY)
    vmem = pl.BlockSpec(memory_space=pltpu.VMEM)
    out, evidence = pl.pallas_call(
        kernel,
        out_shape=(
            jax.ShapeDtypeStruct((NX, 2, W), f32),
            jax.ShapeDtypeStruct((1, ROWS), f32),
        ),
        in_specs=[anywhere] * 3 + [pl.BlockSpec(memory_space=pltpu.SMEM), vmem, vmem],
        out_specs=(vmem, vmem),
        scratch_shapes=[
            pltpu.VMEM((ROWS, F), bf16),
            pltpu.VMEM((GROUPS, F), f32),
            pltpu.VMEM((NX, ROWS, W + TAG), bf16),
            pltpu.VMEM((2 * NX, ROWS, W + TAG), bf16),
            pltpu.VMEM((2 * NX, ROWS, W), bf16),
            pltpu.VMEM((TAG, W), bf16),
            pltpu.VMEM((4, PARTS, CHUNK, BLOCK), bf16),
            pltpu.VMEM((4, TAG, BLOCK), bf16),
            pltpu.VMEM((4, 2 * NX, ROWS, BLOCK), f32),
            pltpu.VMEM((4, 2 * NX, ROWS, BLOCK), f32),
            pltpu.VMEM((2, 4, ROWS, BLOCK), bf16),
            pltpu.VMEM((2 * NX, 4, ROWS, BLOCK), bf16),
            pltpu.VMEM((4 * BLOCK, ALL), bf16),
            [pltpu.VMEM((2, 2, 4, 4, OWN, t[3]), bf16) for t in STREAMS],
            [pltpu.VMEM((2, 4, 4, OWN, t[3]), bf16) for t in STREAMS],
            [pltpu.VMEM((2, 4, 4, OWN, t[3]), bf16) for t in STREAMS],
            [pltpu.VMEM((4, 4, OWN, t[3]), bf16) for t in STREAMS],
            [pltpu.VMEM((4, 4, OWN, t[3]), bf16) for t in STREAMS],
            [pltpu.VMEM((3, 4, OWN, t[3]), bf16) for t in STREAMS],
            [pltpu.VMEM((4, NX, 2, t), bf16) for t in (WA, WB)],
            [pltpu.VMEM((4, NX, 2, t), bf16) for t in (WA, WB)],
            pltpu.SemaphoreType.REGULAR((2, 4)),
            pltpu.SemaphoreType.REGULAR((2, 2)),
            dma((4,)),
            dma((2 * NX,)), dma((2 * NX,)),
            dma((6,)), dma((6,)),
            dma((6,)), dma((6,)),
            dma((2, 6)), dma((2, 6)),
            dma((4, 2 * NX)), dma((4, 2 * NX)),
            dma((2 * NX,)), dma((2 * NX,)),
            dma((5, len(STREAMS))), dma((5, len(STREAMS))),
            dma((2, 16)), dma((2, 16)),
        ],
        compiler_params=pltpu.CompilerParams(
            collective_id=0, has_side_effects=True, vmem_limit_bytes=58 * 1024 * 1024
        ),
        name="estep",
    )(
        images, projections.T.reshape(F // CHUNK, CHUNK, BLOCK), noise_power, class_logprior.reshape(1, CLASSES),
        groups.reshape(1, ROWS), offsets.reshape(1, ROWS),
    )
    out, evidence = pl.pallas_call(
        finish,
        out_shape=(
            jax.ShapeDtypeStruct((2, F), f32),
            jax.ShapeDtypeStruct((1, ROWS), f32),
        ),
        in_specs=[vmem, vmem],
        out_specs=(vmem, vmem),
        name="finish",
    )(out, evidence)
    return (out, evidence.reshape(ROWS))


def solution(mesh):
    in_specs = (
        P(("cls", "img"), None),
        P("cls", None),
        P(),
        P(),
        P(("cls", "img")),
        P(("cls", "img")),
    )
    out_specs = (P(("cls", "img"), None), P(("cls", "img")))
    return jax.shard_map(body, mesh=mesh, in_specs=in_specs, out_specs=out_specs, check_vma=False)
```

```python
import jax
import jax.numpy as jnp
from jax import lax
from jax.experimental import pallas as pl
from jax.experimental.pallas import tpu as pltpu
from jax.sharding import PartitionSpec as P

NX, NY, NZ = 4, 8, 8
F = 7200
W = 1920
TAG = 128
ROWS = 56
ALL = 2 * NX * ROWS
BLOCK = 128
CHUNKS = 4
PARTS = 2 * CHUNKS
CHUNK = W // PARTS
WHOLE = F // CHUNK - (NX - 1) * PARTS
STEPS = (0, 1, 3, 2)
EARLY = 6
LAST = F - (NX - 1) * W
WA = 1024
WB = W - WA
GROUPS = 32
CLASSES = 4
OWN = 8
STREAMS = (
    ("z", 1, 0, 256), ("z", -1, 256, 256), ("y", 1, 1024, 256), ("y", -1, 1280, 256),
    ("z", 1, 512, 256), ("z", -1, 768, 256), ("y", 1, 1536, 256), ("y", -1, 1792, 128),
)
NN = (((1,), (0,)), ((), ()))
f32 = jnp.float32
bf16 = jnp.bfloat16


def finish(fin_ref, ev_ref, out_ref, evidence_ref):
    for k in range(NX):
        end = min(F, W * (k + 1))
        out_ref[:, W * k : end] = fin_ref[k, :, : end - W * k]
    evidence_ref[...] = ev_ref[...]


def kernel(
    img_hbm, proj_hbm, noise_hbm, prior_ref, group_ref, offset_ref, out_hbm, ev_hbm,
    out_ref, ev_ref,
    img_v, noise_v, img_ref, xin, white, inv3, pbuf, qbuf, sc_send, sc_recv, post_send, post_recv,
    wt, parts, in1, mid1, in2, mid2, in3, own, got,
    near_up, near_down, load, img_s, img_r, ring_s, cross_r, pair_r, side_r, sc_s, sc_r,
    post_s, post_r,
    st_s, st_r, own_s, own_r,
):
    cls = lax.axis_index("cls")
    img = lax.axis_index("img")
    h, c = cls // 2, cls % 2
    lo, z, x = img // (NZ * NX), (img // NX) % NZ, img % NX
    y = 2 * h + lo
    turn = (0, 3 - 2 * lo, 1 + 2 * lo, 2)
    half = z % 2

    def device(y_, z_, x_, c_):
        return {"cls": (y_ // 2) * 2 + c_, "img": ((y_ % 2) * NZ + z_) * NX + x_}

    def group(dx, dc):
        return device(y, z, (x + dx) % NX, (c + dc) % 2)

    def along_y(d):
        return device((y + d) % NY, z, x, c)

    def along_z(d):
        return device(y, (z + d) % NZ, x, c)

    across = device((y + NY - 1 + 2 * lo) % NY, z, x, c)
    beside = device(y + 1 - 2 * lo, z, x, c)

    def copy(src, dst, send, recv, to):
        return pltpu.make_async_remote_copy(
            src_ref=src, dst_ref=dst, send_sem=send, recv_sem=recv,
            device_id=to, device_id_type=pl.DeviceIdType.MESH,
        )

    load_img = pltpu.make_async_copy(img_hbm, img_v, load.at[0])
    load_noise = pltpu.make_async_copy(noise_hbm, noise_v, load.at[1])

    load_proj = pltpu.make_async_copy(
        proj_hbm.at[pl.ds(x * PARTS, WHOLE)], pbuf.at[0, pl.ds(0, WHOLE)], load.at[2]
    )
    load_rest = pltpu.make_async_copy(
        proj_hbm.at[pl.ds((x % (NX - 1)) * PARTS + WHOLE, PARTS - WHOLE)],
        pbuf.at[0, pl.ds(WHOLE, PARTS - WHOLE)], load.at[3],
    )
    load_img.start()
    load_proj.start()

    @pl.when(x < NX - 1)
    def _():
        load_rest.start()

    load_noise.start()

    barrier = pltpu.get_barrier_semaphore()
    partners = [group(s // 2, s % 2) for s in range(1, 2 * NX)]
    partners += [along_y(1), along_y(NY - 1), along_z(1), along_z(NZ - 1)]
    for to in partners:
        pl.semaphore_signal(barrier, inc=1, device_id=to, device_id_type=pl.DeviceIdType.MESH)

    tag = lax.broadcasted_iota(jnp.int32, (TAG, ROWS), 0)
    is_group = (tag < 96) & (tag % 32 == group_ref[...])
    is_offset = (tag >= 96) & (tag < 108) & (tag % 4 == offset_ref[...])
    tags = jnp.transpose(jnp.where(is_group | is_offset, 1.0, 0.0).astype(f32)).astype(bf16)
    load_img.wait()
    for k in range(NX):
        end = min(F, W * (k + 1))
        img_ref[k, :, : end - W * k] = img_v[:, W * k : end]
        if end - W * k < W:
            img_ref[k, :, end - W * k : W] = jnp.zeros((ROWS, W * (k + 1) - end), bf16)
        img_ref[k, :, W:] = tags
    load_proj.wait()

    @pl.when(x < NX - 1)
    def _():
        load_rest.wait()

    @pl.when(x == NX - 1)
    def _():
        pbuf[0, WHOLE:] = jnp.zeros((PARTS - WHOLE, CHUNK, BLOCK), bf16)

    pl.semaphore_wait(barrier, len(partners))

    def turned(m, low):
        return (m + 2 * low) % CHUNKS

    def to_across(m):
        mine = half * CHUNKS + turned(m, 1 - lo)
        src, dst = (pbuf.at[0, mine], pbuf.at[1, mine])
        if m >= CHUNKS:
            src, dst = (pbuf.at[2, mine], pbuf.at[3, mine])
        return copy(src, dst, ring_s.at[0], cross_r.at[m], across)

    def from_across(m):
        return pbuf.at[1 if m < CHUNKS else 3, half * CHUNKS + turned(m, lo)]

    def to_beside(m):
        dst = pbuf.at[2 if m < CHUNKS else 3, half * CHUNKS + turned(m, lo)]
        return copy(from_across(m), dst, ring_s.at[1], pair_r.at[m], beside)

    def from_beside(m):
        return pbuf.at[2 if m < CHUNKS else 3, half * CHUNKS + turned(m, 1 - lo)]

    def to_side(way, m):
        ref = from_across(m) if way == 0 else from_beside(m)
        up = 1 - 2 * (turned(m, lo if way == 0 else 1 - lo) // 2)
        to = device(y, (z + NZ + up) % NZ, x, c)
        return copy(ref, ref, ring_s.at[2 + way], side_r.at[way if m < CHUNKS else 2], to)

    def sided(slot):
        ref = pbuf.at[slot, pl.ds((1 - half) * CHUNKS, CHUNKS)]
        copy(ref, ref, ring_s.at[2], side_r.at[slot - 1], along_z(1)).wait_recv()

    def crossed(m):
        ref = from_across(m)
        copy(ref, ref, ring_s.at[0], cross_r.at[m], across).wait_recv()
        to_beside(m).start()
        to_side(0, m).start()

    def paired(m):
        ref = from_beside(m)
        copy(ref, ref, ring_s.at[1], pair_r.at[m], beside).wait_recv()
        if m < 2:
            to_across(CHUNKS + m).start()
        to_side(1, m).start()

    def image(p):
        return copy(
            img_ref.at[(x + STEPS[p]) % NX], xin.at[2 * p], img_s.at[0], img_r.at[2 * p],
            group(STEPS[p], 0),
        )

    def to_sibling(p):
        src = img_ref.at[x] if p == 0 else xin.at[2 * p]
        s = 2 * p + 1
        return copy(src, xin.at[s], img_s.at[1], img_r.at[s], group(0, 1))

    def tell(r):
        for n, at in ((0, along_y), (1, along_z)):
            pl.semaphore_signal(
                near_up.at[n, r - 1], inc=1, device_id=at(1), device_id_type=pl.DeviceIdType.MESH
            )
            if r <= 2:
                pl.semaphore_signal(
                    near_down.at[n, r - 1], inc=1, device_id=at(7),
                    device_id_type=pl.DeviceIdType.MESH,
                )

    def told(r):
        for n in (0, 1):
            pl.semaphore_wait(near_up.at[n, r - 1], 1)
            if r <= 2:
                pl.semaphore_wait(near_down.at[n, r - 1], 1)
        if r < 4:
            tell(r + 1)

    for m in range(CHUNKS):
        to_across(m).start()
    tell(1)
    for p in (1, 2, 3):
        image(p).start()
    to_sibling(0).start()

    xin[0] = img_ref[x]
    load_noise.wait()

    def pieces(inv, width):
        hi = inv.astype(bf16)
        rest = inv - hi.astype(f32)
        mid = rest.astype(bf16)
        low = (rest - mid.astype(f32)).astype(bf16)
        inv3[0:GROUPS, :width] = hi
        inv3[GROUPS : 2 * GROUPS, :width] = mid
        inv3[2 * GROUPS : 3 * GROUPS, :width] = low

    inv3[3 * GROUPS :] = jnp.zeros((TAG - 3 * GROUPS, W), bf16)

    @pl.when(x < NX - 1)
    def _():
        pieces(1.0 / noise_v[:, pl.ds(pl.multiple_of(x * W, 128), W)], W)

    @pl.when(x == NX - 1)
    def _():
        pieces(1.0 / noise_v[:, F - LAST :], LAST)
        inv3[: 3 * GROUPS, LAST:] = jnp.zeros((3 * GROUPS, W - LAST), bf16)

    row = lax.broadcasted_iota(jnp.int32, (TAG, BLOCK), 0)
    piece = jnp.where(row < 96, row // 32, jnp.minimum((row - 96) // 4, 3))

    def block_of(slot):
        return pbuf[slot].reshape(W, BLOCK)

    def columns(slot):
        p = block_of(slot).astype(f32)
        square = p * p
        s_hi = square.astype(bf16)
        s_lo = (square - s_hi.astype(f32)).astype(bf16)
        q = lax.dot_general(inv3[...], s_hi, NN, preferred_element_type=f32)
        q += lax.dot_general(inv3[...], s_lo, NN, preferred_element_type=f32)
        q = q[0:32] + q[32:64] + q[64:96]
        prior = jnp.zeros((TAG, BLOCK), f32)
        for o in range(CLASSES):
            log_prior = prior_ref[0, (h + turn[slot] + CLASSES - o) % CLASSES]
            prior = jnp.where(row % CLASSES == o, log_prior * (1.0 / NX), prior)
        value = jnp.where(row < 96, -0.5 * jnp.concatenate([q] * 4, axis=0), prior)
        v_hi = value.astype(bf16).astype(f32)
        v_mid = (value - v_hi).astype(bf16).astype(f32)
        v_lo = value - v_hi - v_mid
        both = jnp.where(piece == 2, v_lo, 0.0)
        both = jnp.where(piece == 1, v_mid, both)
        qbuf[slot] = jnp.where(piece == 0, v_hi, both).astype(bf16)

    def image_arrived(p):
        image(p).wait_recv()
        to_sibling(p).start()

    def score_copy(slot, s):
        return copy(
            sc_send.at[slot, s], sc_recv.at[slot, s], sc_s.at[slot], sc_r.at[slot],
            group((NX - STEPS[s // 2]) % NX, s % 2),
        )

    def scores(slot, first, last):
        rows = (last - first) * ROWS
        part = lax.dot_general(
            white[first:last].reshape(rows, W), block_of(slot), NN, preferred_element_type=f32
        )
        part += lax.dot_general(
            xin[first:last, :, W:].reshape(rows, TAG), qbuf[slot], NN, preferred_element_type=f32
        )
        sc_send[slot, first:last] = part.reshape(last - first, ROWS, BLOCK)
        for s in (6, 7, 2, 4, 3, 5, 1):
            if first <= s < last:
                score_copy(slot, s).start()

    def whiten(s):
        inverse = jnp.dot(xin[s, :, W:], inv3[...], preferred_element_type=f32)
        white[s] = (xin[s, :, :W].astype(f32) * inverse).astype(bf16)

    whiten(0)
    columns(0)
    crossed(0)
    crossed(1)
    told(1)
    crossed(2)
    paired(0)
    crossed(3)
    told(2)
    image_arrived(1)
    image_arrived(2)
    paired(1)
    whiten(2)
    whiten(4)
    for s in (1, 3, 5):
        to_sibling(s // 2).wait_recv()
        whiten(s)
    paired(2)
    scores(0, 0, EARLY)
    crossed(4)
    paired(3)
    sided(1)
    crossed(5)
    columns(1)
    scores(1, 0, EARLY)
    paired(4)
    image_arrived(3)
    whiten(6)
    sided(2)
    columns(2)
    paired(5)
    told(3)
    to_sibling(3).wait_recv()
    whiten(7)
    scores(0, EARLY, 2 * NX)
    scores(1, EARLY, 2 * NX)
    scores(2, 0, 2 * NX)
    sided(3)
    told(4)
    columns(3)
    scores(3, 0, 2 * NX)

    total = {}
    for slot in range(4):
        ref = sc_recv.at[slot, pl.ds(1, 2 * NX - 1)]
        copy(ref, ref, sc_s.at[slot], sc_r.at[slot], group(1, 0)).wait_recv()
        for dc in (0, 1):
            terms = [sc_send[slot, 0]] if dc == 0 else [sc_recv[slot, 1]]
            terms += [sc_recv[slot, 2 * dx + dc] for dx in range(1, NX)]
            total[slot, dc] = (terms[0] + terms[1]) + (terms[2] + terms[3])
    peak = None
    for value in total.values():
        peak = value if peak is None else jnp.maximum(peak, value)
    peak = jnp.max(peak, axis=1, keepdims=True)
    mass = None
    for value in total.values():
        term = jnp.exp(value - peak)
        mass = term if mass is None else mass + term
    evidence = peak + jnp.log(jnp.sum(mass, axis=1, keepdims=True))
    ev_ref[...] = jnp.transpose(jnp.broadcast_to(evidence, (ROWS, TAG)))[0:1, :]
    store_ev = pltpu.make_async_copy(ev_ref, ev_hbm, load.at[4])
    store_ev.start()
    for (slot, dc), value in total.items():
        post_send[dc, slot] = jnp.exp(value - evidence).astype(bf16)

    def post_copy(s):
        return copy(
            post_send.at[s % 2], post_recv.at[s], post_s.at[0], post_r.at[0],
            group(STEPS[s // 2], s % 2),
        )

    for s in (6, 7, 2, 4, 3, 5, 1):
        post_copy(s).start()
    post_recv[0] = post_send[0]
    posts = post_recv.at[pl.ds(1, 2 * NX - 1)]
    all_posts = copy(posts, posts, post_s.at[0], post_r.at[0], group(1, 0))
    all_posts.wait_recv()

    for slot in range(4):
        wt[BLOCK * slot : BLOCK * (slot + 1)] = jnp.transpose(post_recv[:, slot].reshape(ALL, BLOCK))

    place = {"z": z, "y": y}
    other = {"z": "y", "y": "z"}

    def along(axis, d):
        at = (place[axis] + d + 8) % 8
        return device(y, at, x, c) if axis == "z" else device(at, z, x, c)

    def near(axis, side):
        return along(axis, side * (1 - 2 * (place[axis] % 2)))

    def stage1(i):
        axis, side = STREAMS[i][:2]
        return copy(
            parts[i].at[1 - place[axis] % 2], in1[i], st_s.at[0, i], st_r.at[0, i], near(axis, side)
        )

    def stage2(i):
        axis, side = STREAMS[i][:2]
        return copy(
            mid1[i].at[1 - place[other[axis]] % 2], in2[i], st_s.at[1, i], st_r.at[1, i],
            near(other[axis], side),
        )

    def stage3(i, d):
        axis = STREAMS[i][0]
        return copy(
            mid2[i].at[(place[axis] // 2 + d) % 4], in3[i].at[d - 1], st_s.at[2, i],
            st_r.at[2, i], along(axis, 2 * d),
        )

    def all3(i):
        return copy(in3[i], in3[i], st_s.at[2, i], st_r.at[2, i], along("z", 2))

    def last(axis, d, e):
        n = "zy".index(axis)
        at = (place[other[axis]] + 2 * d) % 8
        to = device(at, z, (x + e) % NX, c) if axis == "z" else device(y, at, (x + e) % NX, c)
        return copy(
            own[n].at[(place[other[axis]] // 2 + d) % 4, (x + e) % NX], got[n].at[d, x],
            own_s.at[n, d], own_r.at[n, d], to,
        )

    def self_copy(n, axis):
        return pltpu.make_async_copy(
            own[n].at[place[other[axis]] // 2, x], got[n].at[0, x], own_r.at[n, 0]
        )

    def last_in(n, d):
        return copy(got[n].at[d], got[n].at[d], own_s.at[n, d], own_r.at[n, d], group(1, 0))

    order = range(len(STREAMS))
    for i in order:
        axis, _, col, width = STREAMS[i]
        part = jnp.dot(
            wt[...], white[:, :, col : col + width].reshape(ALL, width), preferred_element_type=f32
        ).astype(bf16)
        for slot in range(4):
            y_half = (h + turn[slot]) % 4
            for r in range(2 * NZ):
                low, z_ = r // NZ, r % NZ
                at = BLOCK * slot + OWN * r
                if axis == "z":
                    parts[i][z_ % 2, low, z_ // 2, y_half] = part[at : at + OWN]
                else:
                    parts[i][low, z_ % 2, y_half, z_ // 2] = part[at : at + OWN]
        stage1(i).start()
    for i in order:
        axis = STREAMS[i][0]
        stage1(i).wait_recv()
        total = parts[i][place[axis] % 2].astype(f32) + in1[i][...].astype(f32)
        mid1[i][...] = total.astype(bf16)
        stage2(i).start()
    for i in order:
        axis = STREAMS[i][0]
        stage2(i).wait_recv()
        total = mid1[i][place[other[axis]] % 2].astype(f32) + in2[i][...].astype(f32)
        mid2[i][...] = total.astype(bf16)
        for d in (2, 1, 3):
            stage3(i, d).start()
    far_first = [(d, e) for d in (2, 1, 3, 0) for e in (2, 1, 3, 0) if d or e]
    for axis in "zy":
        n = "zy".index(axis)
        for i in order:
            if STREAMS[i][0] != axis:
                continue
            _, _, col, width = STREAMS[i]
            col -= WA * n
            acc = mid2[i][place[axis] // 2].astype(f32)
            all3(i).wait_recv()
            for d in (1, 3, 2):
                acc += in3[i][d - 1].astype(f32)
            for k in range(NX):
                own[n][:, k, :, col : col + width] = acc[:, 2 * k : 2 * k + 2].astype(bf16)
        for d, e in far_first:
            last(axis, d, e).start()
        self_copy(n, axis).start()
    for axis in "zy":
        n = "zy".index(axis)
        for d in (0, 1, 3, 2):
            last_in(n, d).wait_recv()
        acc = got[n][0].astype(f32)
        for d in range(1, 4):
            acc += got[n][d].astype(f32)
        out_ref[:, :, WA * n : WA * n + (WA, WB)[n]] = acc
    store_out = pltpu.make_async_copy(out_ref, out_hbm, load.at[5])
    store_out.start()

    def sent(ref, sem):
        copy(ref, ref, sem, cross_r.at[0], across).wait_send()

    for n in range(4):
        sent(pbuf.at[n, pl.ds(0, 6)], ring_s.at[n])
    sent(xin.at[pl.ds(0, NX - 1)], img_s.at[0])
    sent(xin.at[pl.ds(0, NX)], img_s.at[1])
    for slot in range(4):
        sent(sc_send.at[slot, pl.ds(1, 2 * NX - 1)], sc_s.at[slot])
    all_posts.wait_send()
    for i in order:
        stage1(i).wait_send()
        stage2(i).wait_send()
        all3(i).wait_send()
    for n in range(2):
        sent(own[n].at[0, pl.ds(0, NX - 1)], own_s.at[n, 0])
        for d in (1, 2, 3):
            sent(own[n].at[d], own_s.at[n, d])
    store_ev.wait()
    store_out.wait()


def body(images, projections, noise_power, class_logprior, groups, offsets):
    dma = pltpu.SemaphoreType.DMA
    anywhere = pl.BlockSpec(memory_space=pl.ANY)
    vmem = pl.BlockSpec(memory_space=pltpu.VMEM)
    out, evidence = pl.pallas_call(
        kernel,
        out_shape=(
            jax.ShapeDtypeStruct((NX, 2, W), f32),
            jax.ShapeDtypeStruct((1, ROWS), f32),
        ),
        in_specs=[anywhere] * 3 + [pl.BlockSpec(memory_space=pltpu.SMEM), vmem, vmem],
        out_specs=(anywhere, anywhere),
        scratch_shapes=[
            pltpu.VMEM((NX, 2, W), f32),
            pltpu.VMEM((1, ROWS), f32),
            pltpu.VMEM((ROWS, F), bf16),
            pltpu.VMEM((GROUPS, F), f32),
            pltpu.VMEM((NX, ROWS, W + TAG), bf16),
            pltpu.VMEM((2 * NX, ROWS, W + TAG), bf16),
            pltpu.VMEM((2 * NX, ROWS, W), bf16),
            pltpu.VMEM((TAG, W), bf16),
            pltpu.VMEM((4, PARTS, CHUNK, BLOCK), bf16),
            pltpu.VMEM((4, TAG, BLOCK), bf16),
            pltpu.VMEM((4, 2 * NX, ROWS, BLOCK), f32),
            pltpu.VMEM((4, 2 * NX, ROWS, BLOCK), f32),
            pltpu.VMEM((2, 4, ROWS, BLOCK), bf16),
            pltpu.VMEM((2 * NX, 4, ROWS, BLOCK), bf16),
            pltpu.VMEM((4 * BLOCK, ALL), bf16),
            [pltpu.VMEM((2, 2, 4, 4, OWN, t[3]), bf16) for t in STREAMS],
            [pltpu.VMEM((2, 4, 4, OWN, t[3]), bf16) for t in STREAMS],
            [pltpu.VMEM((2, 4, 4, OWN, t[3]), bf16) for t in STREAMS],
            [pltpu.VMEM((4, 4, OWN, t[3]), bf16) for t in STREAMS],
            [pltpu.VMEM((4, 4, OWN, t[3]), bf16) for t in STREAMS],
            [pltpu.VMEM((3, 4, OWN, t[3]), bf16) for t in STREAMS],
            [pltpu.VMEM((4, NX, 2, t), bf16) for t in (WA, WB)],
            [pltpu.VMEM((4, NX, 2, t), bf16) for t in (WA, WB)],
            pltpu.SemaphoreType.REGULAR((2, 4)),
            pltpu.SemaphoreType.REGULAR((2, 2)),
            dma((6,)),
            dma((2,)), dma((2 * NX,)),
            dma((4,)), dma((6,)), dma((6,)), dma((3,)),
            dma((4,)), dma((4,)),
            dma((1,)), dma((1,)),
            dma((3, len(STREAMS))), dma((3, len(STREAMS))),
            dma((2, 4)), dma((2, 4)),
        ],
        compiler_params=pltpu.CompilerParams(
            collective_id=0, has_side_effects=True, vmem_limit_bytes=58 * 1024 * 1024
        ),
        name="estep",
    )(
        images, projections.T.reshape(F // CHUNK, CHUNK, BLOCK), noise_power, class_logprior.reshape(1, CLASSES),
        groups.reshape(1, ROWS), offsets.reshape(1, ROWS),
    )
    out, evidence = pl.pallas_call(
        finish,
        out_shape=(
            jax.ShapeDtypeStruct((2, F), f32),
            jax.ShapeDtypeStruct((1, ROWS), f32),
        ),
        in_specs=[vmem, vmem],
        out_specs=(vmem, vmem),
        name="finish",
    )(out, evidence)
    return (out, evidence.reshape(ROWS))


def solution(mesh):
    in_specs = (
        P(("cls", "img"), None),
        P("cls", None),
        P(),
        P(),
        P(("cls", "img")),
        P(("cls", "img")),
    )
    out_specs = (P(("cls", "img"), None), P(("cls", "img")))
    return jax.shard_map(body, mesh=mesh, in_specs=in_specs, out_specs=out_specs, check_vma=False)
```

```python
import jax
import jax.numpy as jnp
from jax import lax
from jax.experimental import pallas as pl
from jax.experimental.pallas import tpu as pltpu
from jax.sharding import PartitionSpec as P

NX, NY, NZ = 4, 8, 8
F = 7200
W = 1920
TAG = 128
ROWS = 56
ALL = 2 * NX * ROWS
BLOCK = 128
CHUNKS = 4
PARTS = 2 * CHUNKS
CHUNK = W // PARTS
WHOLE = F // CHUNK - (NX - 1) * PARTS
STEPS = (0, 1, 3, 2)
EARLY = 6
LAST = F - (NX - 1) * W
WA = 1024
WB = W - WA
GROUPS = 32
CLASSES = 4
OWN = 8
STREAMS = (
    ("z", 1, 0, 256), ("z", -1, 256, 256), ("y", 1, 1024, 256), ("y", -1, 1280, 256),
    ("z", 1, 512, 256), ("z", -1, 768, 256), ("y", 1, 1536, 256), ("y", -1, 1792, 128),
)
NN = (((1,), (0,)), ((), ()))
f32 = jnp.float32
bf16 = jnp.bfloat16


def finish(fin_hbm, ev_hbm, out_hbm, evidence_hbm, fin_ref, ev_ref, out_ref, sem):
    load_fin = pltpu.make_async_copy(fin_hbm, fin_ref, sem.at[0])
    load_ev = pltpu.make_async_copy(ev_hbm, ev_ref, sem.at[1])
    store_ev = pltpu.make_async_copy(ev_ref, evidence_hbm, sem.at[2])
    store_out = pltpu.make_async_copy(out_ref, out_hbm, sem.at[3])
    load_fin.start()
    load_ev.start()
    load_ev.wait()
    store_ev.start()
    load_fin.wait()
    for k in range(NX):
        end = min(F, W * (k + 1))
        out_ref[:, W * k : end] = fin_ref[k, :, : end - W * k]
    store_out.start()
    store_ev.wait()
    store_out.wait()


def kernel(
    img_hbm, proj_hbm, noise_hbm, prior_ref, group_ref, offset_ref, out_hbm, ev_hbm,
    out_ref, ev_ref,
    img_v, noise_v, img_ref, xin, white, inv3, pbuf, qbuf, sc_send, sc_recv, post_send, post_recv,
    wt, parts, in1, mid1, in2, mid2, in3, own, got,
    near_up, near_down, load, img_s, img_r, ring_s, cross_r, pair_r, side_r, sc_s, sc_r,
    post_s, post_r,
    st_s, st_r, own_s, own_r,
):
    cls = lax.axis_index("cls")
    img = lax.axis_index("img")
    h, c = cls // 2, cls % 2
    lo, z, x = img // (NZ * NX), (img // NX) % NZ, img % NX
    y = 2 * h + lo
    turn = (0, 3 - 2 * lo, 1 + 2 * lo, 2)
    half = z % 2

    def device(y_, z_, x_, c_):
        return {"cls": (y_ // 2) * 2 + c_, "img": ((y_ % 2) * NZ + z_) * NX + x_}

    def group(dx, dc):
        return device(y, z, (x + dx) % NX, (c + dc) % 2)

    def along_y(d):
        return device((y + d) % NY, z, x, c)

    def along_z(d):
        return device(y, (z + d) % NZ, x, c)

    across = device((y + NY - 1 + 2 * lo) % NY, z, x, c)
    beside = device(y + 1 - 2 * lo, z, x, c)

    def copy(src, dst, send, recv, to):
        return pltpu.make_async_remote_copy(
            src_ref=src, dst_ref=dst, send_sem=send, recv_sem=recv,
            device_id=to, device_id_type=pl.DeviceIdType.MESH,
        )

    load_img = pltpu.make_async_copy(img_hbm, img_v, load.at[0])
    load_noise = pltpu.make_async_copy(noise_hbm, noise_v, load.at[1])

    load_proj = pltpu.make_async_copy(
        proj_hbm.at[pl.ds(x * PARTS, WHOLE)], pbuf.at[0, pl.ds(0, WHOLE)], load.at[2]
    )
    load_rest = pltpu.make_async_copy(
        proj_hbm.at[pl.ds((x % (NX - 1)) * PARTS + WHOLE, PARTS - WHOLE)],
        pbuf.at[0, pl.ds(WHOLE, PARTS - WHOLE)], load.at[3],
    )
    load_img.start()
    load_proj.start()

    @pl.when(x < NX - 1)
    def _():
        load_rest.start()

    load_noise.start()

    barrier = pltpu.get_barrier_semaphore()
    partners = [group(s // 2, s % 2) for s in range(1, 2 * NX)]
    partners += [along_y(1), along_y(NY - 1), along_z(1), along_z(NZ - 1)]
    for to in partners:
        pl.semaphore_signal(barrier, inc=1, device_id=to, device_id_type=pl.DeviceIdType.MESH)

    tag = lax.broadcasted_iota(jnp.int32, (TAG, ROWS), 0)
    is_group = (tag < 96) & (tag % 32 == group_ref[...])
    is_offset = (tag >= 96) & (tag < 108) & (tag % 4 == offset_ref[...])
    tags = jnp.transpose(jnp.where(is_group | is_offset, 1.0, 0.0).astype(f32)).astype(bf16)
    load_img.wait()
    for k in range(NX):
        end = min(F, W * (k + 1))
        img_ref[k, :, : end - W * k] = img_v[:, W * k : end]
        if end - W * k < W:
            img_ref[k, :, end - W * k : W] = jnp.zeros((ROWS, W * (k + 1) - end), bf16)
        img_ref[k, :, W:] = tags
    load_proj.wait()

    @pl.when(x < NX - 1)
    def _():
        load_rest.wait()

    @pl.when(x == NX - 1)
    def _():
        pbuf[0, WHOLE:] = jnp.zeros((PARTS - WHOLE, CHUNK, BLOCK), bf16)

    pl.semaphore_wait(barrier, len(partners))

    def turned(m, low):
        return (m + 2 * low) % CHUNKS

    def to_across(m):
        mine = half * CHUNKS + turned(m, 1 - lo)
        src, dst = (pbuf.at[0, mine], pbuf.at[1, mine])
        if m >= CHUNKS:
            src, dst = (pbuf.at[2, mine], pbuf.at[3, mine])
        return copy(src, dst, ring_s.at[0], cross_r.at[m], across)

    def from_across(m):
        return pbuf.at[1 if m < CHUNKS else 3, half * CHUNKS + turned(m, lo)]

    def to_beside(m):
        dst = pbuf.at[2 if m < CHUNKS else 3, half * CHUNKS + turned(m, lo)]
        return copy(from_across(m), dst, ring_s.at[1], pair_r.at[m], beside)

    def from_beside(m):
        return pbuf.at[2 if m < CHUNKS else 3, half * CHUNKS + turned(m, 1 - lo)]

    def to_side(way, m):
        ref = from_across(m) if way == 0 else from_beside(m)
        up = 1 - 2 * (turned(m, lo if way == 0 else 1 - lo) // 2)
        to = device(y, (z + NZ + up) % NZ, x, c)
        return copy(ref, ref, ring_s.at[2 + way], side_r.at[way if m < CHUNKS else 2], to)

    def sided(slot):
        ref = pbuf.at[slot, pl.ds((1 - half) * CHUNKS, CHUNKS)]
        copy(ref, ref, ring_s.at[2], side_r.at[slot - 1], along_z(1)).wait_recv()

    def crossed(m):
        ref = from_across(m)
        copy(ref, ref, ring_s.at[0], cross_r.at[m], across).wait_recv()
        to_beside(m).start()
        to_side(0, m).start()

    def paired(m):
        ref = from_beside(m)
        copy(ref, ref, ring_s.at[1], pair_r.at[m], beside).wait_recv()
        if m < 2:
            to_across(CHUNKS + m).start()
        to_side(1, m).start()

    def image(p):
        return copy(
            img_ref.at[(x + STEPS[p]) % NX], xin.at[2 * p], img_s.at[0], img_r.at[2 * p],
            group(STEPS[p], 0),
        )

    def to_sibling(p):
        src = img_ref.at[x] if p == 0 else xin.at[2 * p]
        s = 2 * p + 1
        return copy(src, xin.at[s], img_s.at[1], img_r.at[s], group(0, 1))

    def tell(r):
        for n, at in ((0, along_y), (1, along_z)):
            pl.semaphore_signal(
                near_up.at[n, r - 1], inc=1, device_id=at(1), device_id_type=pl.DeviceIdType.MESH
            )
            if r <= 2:
                pl.semaphore_signal(
                    near_down.at[n, r - 1], inc=1, device_id=at(7),
                    device_id_type=pl.DeviceIdType.MESH,
                )

    def told(r):
        for n in (0, 1):
            pl.semaphore_wait(near_up.at[n, r - 1], 1)
            if r <= 2:
                pl.semaphore_wait(near_down.at[n, r - 1], 1)
        if r < 4:
            tell(r + 1)

    for m in range(CHUNKS):
        to_across(m).start()
    tell(1)
    for p in (1, 2, 3):
        image(p).start()
    to_sibling(0).start()

    xin[0] = img_ref[x]
    load_noise.wait()

    def pieces(inv, width):
        hi = inv.astype(bf16)
        rest = inv - hi.astype(f32)
        mid = rest.astype(bf16)
        low = (rest - mid.astype(f32)).astype(bf16)
        inv3[0:GROUPS, :width] = hi
        inv3[GROUPS : 2 * GROUPS, :width] = mid
        inv3[2 * GROUPS : 3 * GROUPS, :width] = low

    inv3[3 * GROUPS :] = jnp.zeros((TAG - 3 * GROUPS, W), bf16)

    @pl.when(x < NX - 1)
    def _():
        pieces(1.0 / noise_v[:, pl.ds(pl.multiple_of(x * W, 128), W)], W)

    @pl.when(x == NX - 1)
    def _():
        pieces(1.0 / noise_v[:, F - LAST :], LAST)
        inv3[: 3 * GROUPS, LAST:] = jnp.zeros((3 * GROUPS, W - LAST), bf16)

    row = lax.broadcasted_iota(jnp.int32, (TAG, BLOCK), 0)
    piece = jnp.where(row < 96, row // 32, jnp.minimum((row - 96) // 4, 3))

    def block_of(slot):
        return pbuf[slot].reshape(W, BLOCK)

    def columns(slot):
        p = block_of(slot).astype(f32)
        square = p * p
        s_hi = square.astype(bf16)
        s_lo = (square - s_hi.astype(f32)).astype(bf16)
        q = lax.dot_general(inv3[...], s_hi, NN, preferred_element_type=f32)
        q += lax.dot_general(inv3[...], s_lo, NN, preferred_element_type=f32)
        q = q[0:32] + q[32:64] + q[64:96]
        prior = jnp.zeros((TAG, BLOCK), f32)
        for o in range(CLASSES):
            log_prior = prior_ref[0, (h + turn[slot] + CLASSES - o) % CLASSES]
            prior = jnp.where(row % CLASSES == o, log_prior * (1.0 / NX), prior)
        value = jnp.where(row < 96, -0.5 * jnp.concatenate([q] * 4, axis=0), prior)
        v_hi = value.astype(bf16).astype(f32)
        v_mid = (value - v_hi).astype(bf16).astype(f32)
        v_lo = value - v_hi - v_mid
        both = jnp.where(piece == 2, v_lo, 0.0)
        both = jnp.where(piece == 1, v_mid, both)
        qbuf[slot] = jnp.where(piece == 0, v_hi, both).astype(bf16)

    def image_arrived(p):
        image(p).wait_recv()
        to_sibling(p).start()

    def score_copy(slot, s):
        return copy(
            sc_send.at[slot, s], sc_recv.at[slot, s], sc_s.at[slot], sc_r.at[slot],
            group((NX - STEPS[s // 2]) % NX, s % 2),
        )

    def scores(slot, first, last):
        rows = (last - first) * ROWS
        part = lax.dot_general(
            white[first:last].reshape(rows, W), block_of(slot), NN, preferred_element_type=f32
        )
        part += lax.dot_general(
            xin[first:last, :, W:].reshape(rows, TAG), qbuf[slot], NN, preferred_element_type=f32
        )
        sc_send[slot, first:last] = part.reshape(last - first, ROWS, BLOCK)
        for s in (6, 7, 2, 4, 3, 5, 1):
            if first <= s < last:
                score_copy(slot, s).start()

    def whiten(s):
        inverse = jnp.dot(xin[s, :, W:], inv3[...], preferred_element_type=f32)
        white[s] = (xin[s, :, :W].astype(f32) * inverse).astype(bf16)

    whiten(0)
    columns(0)
    crossed(0)
    crossed(1)
    told(1)
    crossed(2)
    paired(0)
    crossed(3)
    told(2)
    image_arrived(1)
    image_arrived(2)
    paired(1)
    whiten(2)
    whiten(4)
    for s in (1, 3, 5):
        to_sibling(s // 2).wait_recv()
        whiten(s)
    paired(2)
    scores(0, 0, EARLY)
    crossed(4)
    paired(3)
    sided(1)
    crossed(5)
    columns(1)
    image_arrived(3)
    scores(1, 0, EARLY)
    whiten(6)
    paired(4)
    to_sibling(3).wait_recv()
    whiten(7)
    paired(5)
    scores(0, EARLY, 2 * NX)
    scores(1, EARLY, 2 * NX)
    told(3)
    sided(2)
    columns(2)
    scores(2, 0, 2 * NX)
    sided(3)
    told(4)
    columns(3)
    scores(3, 0, 2 * NX)

    total = {}
    for slot in range(4):
        ref = sc_recv.at[slot, pl.ds(1, 2 * NX - 1)]
        copy(ref, ref, sc_s.at[slot], sc_r.at[slot], group(1, 0)).wait_recv()
        for dc in (0, 1):
            terms = [sc_send[slot, 0]] if dc == 0 else [sc_recv[slot, 1]]
            terms += [sc_recv[slot, 2 * dx + dc] for dx in range(1, NX)]
            total[slot, dc] = (terms[0] + terms[1]) + (terms[2] + terms[3])
    peak = None
    for value in total.values():
        peak = value if peak is None else jnp.maximum(peak, value)
    peak = jnp.max(peak, axis=1, keepdims=True)
    mass = None
    for value in total.values():
        term = jnp.exp(value - peak)
        mass = term if mass is None else mass + term
    evidence = peak + jnp.log(jnp.sum(mass, axis=1, keepdims=True))
    ev_ref[...] = jnp.transpose(jnp.broadcast_to(evidence, (ROWS, TAG)))[0:1, :]
    store_ev = pltpu.make_async_copy(ev_ref, ev_hbm, load.at[4])
    store_ev.start()
    for (slot, dc), value in total.items():
        post_send[dc, slot] = jnp.exp(value - evidence).astype(bf16)

    def post_copy(s):
        return copy(
            post_send.at[s % 2], post_recv.at[s], post_s.at[0], post_r.at[0],
            group(STEPS[s // 2], s % 2),
        )

    for s in (6, 7, 2, 4, 3, 5, 1):
        post_copy(s).start()
    post_recv[0] = post_send[0]
    posts = post_recv.at[pl.ds(1, 2 * NX - 1)]
    all_posts = copy(posts, posts, post_s.at[0], post_r.at[0], group(1, 0))
    all_posts.wait_recv()

    for slot in range(4):
        wt[BLOCK * slot : BLOCK * (slot + 1)] = jnp.transpose(post_recv[:, slot].reshape(ALL, BLOCK))

    place = {"z": z, "y": y}
    other = {"z": "y", "y": "z"}

    def along(axis, d):
        at = (place[axis] + d + 8) % 8
        return device(y, at, x, c) if axis == "z" else device(at, z, x, c)

    def near(axis, side):
        return along(axis, side * (1 - 2 * (place[axis] % 2)))

    def stage1(i):
        axis, side = STREAMS[i][:2]
        return copy(
            parts[i].at[1 - place[axis] % 2], in1[i], st_s.at[0, i], st_r.at[0, i], near(axis, side)
        )

    def stage2(i):
        axis, side = STREAMS[i][:2]
        return copy(
            mid1[i].at[1 - place[other[axis]] % 2], in2[i], st_s.at[1, i], st_r.at[1, i],
            near(other[axis], side),
        )

    def stage3(i, d):
        axis = STREAMS[i][0]
        return copy(
            mid2[i].at[(place[axis] // 2 + d) % 4], in3[i].at[d - 1], st_s.at[2, i],
            st_r.at[2, i], along(axis, 2 * d),
        )

    def all3(i):
        return copy(in3[i], in3[i], st_s.at[2, i], st_r.at[2, i], along("z", 2))

    def last(axis, d, e):
        n = "zy".index(axis)
        at = (place[other[axis]] + 2 * d) % 8
        to = device(at, z, (x + e) % NX, c) if axis == "z" else device(y, at, (x + e) % NX, c)
        return copy(
            own[n].at[(place[other[axis]] // 2 + d) % 4, (x + e) % NX], got[n].at[d, x],
            own_s.at[n, d], own_r.at[n, d], to,
        )

    def self_copy(n, axis):
        return pltpu.make_async_copy(
            own[n].at[place[other[axis]] // 2, x], got[n].at[0, x], own_r.at[n, 0]
        )

    def last_in(n, d):
        return copy(got[n].at[d], got[n].at[d], own_s.at[n, d], own_r.at[n, d], group(1, 0))

    order = range(len(STREAMS))
    for i in order:
        axis, _, col, width = STREAMS[i]
        part = jnp.dot(
            wt[...], white[:, :, col : col + width].reshape(ALL, width), preferred_element_type=f32
        ).astype(bf16)
        for slot in range(4):
            y_half = (h + turn[slot]) % 4
            for r in range(2 * NZ):
                low, z_ = r // NZ, r % NZ
                at = BLOCK * slot + OWN * r
                if axis == "z":
                    parts[i][z_ % 2, low, z_ // 2, y_half] = part[at : at + OWN]
                else:
                    parts[i][low, z_ % 2, y_half, z_ // 2] = part[at : at + OWN]
        stage1(i).start()
    for i in order:
        axis = STREAMS[i][0]
        stage1(i).wait_recv()
        total = parts[i][place[axis] % 2].astype(f32) + in1[i][...].astype(f32)
        mid1[i][...] = total.astype(bf16)
        stage2(i).start()
    for i in order:
        axis = STREAMS[i][0]
        stage2(i).wait_recv()
        total = mid1[i][place[other[axis]] % 2].astype(f32) + in2[i][...].astype(f32)
        mid2[i][...] = total.astype(bf16)
        for d in (2, 1, 3):
            stage3(i, d).start()
    far_first = [(d, e) for d in (2, 1, 3, 0) for e in (2, 1, 3, 0) if d or e]
    for axis in "zy":
        n = "zy".index(axis)
        for i in order:
            if STREAMS[i][0] != axis:
                continue
            _, _, col, width = STREAMS[i]
            col -= WA * n
            acc = mid2[i][place[axis] // 2].astype(f32)
            all3(i).wait_recv()
            for d in (1, 3, 2):
                acc += in3[i][d - 1].astype(f32)
            for k in range(NX):
                own[n][:, k, :, col : col + width] = acc[:, 2 * k : 2 * k + 2].astype(bf16)
        for d, e in far_first:
            last(axis, d, e).start()
        self_copy(n, axis).start()
    for axis in "zy":
        n = "zy".index(axis)
        for d in (0, 1, 3, 2):
            last_in(n, d).wait_recv()
        acc = got[n][0].astype(f32)
        for d in range(1, 4):
            acc += got[n][d].astype(f32)
        out_ref[:, :, WA * n : WA * n + (WA, WB)[n]] = acc
    store_out = pltpu.make_async_copy(out_ref, out_hbm, load.at[5])
    store_out.start()

    def sent(ref, sem):
        copy(ref, ref, sem, cross_r.at[0], across).wait_send()

    for n in range(4):
        sent(pbuf.at[n, pl.ds(0, 6)], ring_s.at[n])
    sent(xin.at[pl.ds(0, NX - 1)], img_s.at[0])
    sent(xin.at[pl.ds(0, NX)], img_s.at[1])
    for slot in range(4):
        sent(sc_send.at[slot, pl.ds(1, 2 * NX - 1)], sc_s.at[slot])
    all_posts.wait_send()
    for i in order:
        stage1(i).wait_send()
        stage2(i).wait_send()
        all3(i).wait_send()
    for n in range(2):
        sent(own[n].at[0, pl.ds(0, NX - 1)], own_s.at[n, 0])
        for d in (1, 2, 3):
            sent(own[n].at[d], own_s.at[n, d])
    store_ev.wait()
    store_out.wait()


def body(images, projections, noise_power, class_logprior, groups, offsets):
    dma = pltpu.SemaphoreType.DMA
    anywhere = pl.BlockSpec(memory_space=pl.ANY)
    vmem = pl.BlockSpec(memory_space=pltpu.VMEM)
    out, evidence = pl.pallas_call(
        kernel,
        out_shape=(
            jax.ShapeDtypeStruct((NX, 2, W), f32),
            jax.ShapeDtypeStruct((1, ROWS), f32),
        ),
        in_specs=[anywhere] * 3 + [pl.BlockSpec(memory_space=pltpu.SMEM), vmem, vmem],
        out_specs=(anywhere, anywhere),
        scratch_shapes=[
            pltpu.VMEM((NX, 2, W), f32),
            pltpu.VMEM((1, ROWS), f32),
            pltpu.VMEM((ROWS, F), bf16),
            pltpu.VMEM((GROUPS, F), f32),
            pltpu.VMEM((NX, ROWS, W + TAG), bf16),
            pltpu.VMEM((2 * NX, ROWS, W + TAG), bf16),
            pltpu.VMEM((2 * NX, ROWS, W), bf16),
            pltpu.VMEM((TAG, W), bf16),
            pltpu.VMEM((4, PARTS, CHUNK, BLOCK), bf16),
            pltpu.VMEM((4, TAG, BLOCK), bf16),
            pltpu.VMEM((4, 2 * NX, ROWS, BLOCK), f32),
            pltpu.VMEM((4, 2 * NX, ROWS, BLOCK), f32),
            pltpu.VMEM((2, 4, ROWS, BLOCK), bf16),
            pltpu.VMEM((2 * NX, 4, ROWS, BLOCK), bf16),
            pltpu.VMEM((4 * BLOCK, ALL), bf16),
            [pltpu.VMEM((2, 2, 4, 4, OWN, t[3]), bf16) for t in STREAMS],
            [pltpu.VMEM((2, 4, 4, OWN, t[3]), bf16) for t in STREAMS],
            [pltpu.VMEM((2, 4, 4, OWN, t[3]), bf16) for t in STREAMS],
            [pltpu.VMEM((4, 4, OWN, t[3]), bf16) for t in STREAMS],
            [pltpu.VMEM((4, 4, OWN, t[3]), bf16) for t in STREAMS],
            [pltpu.VMEM((3, 4, OWN, t[3]), bf16) for t in STREAMS],
            [pltpu.VMEM((4, NX, 2, t), bf16) for t in (WA, WB)],
            [pltpu.VMEM((4, NX, 2, t), bf16) for t in (WA, WB)],
            pltpu.SemaphoreType.REGULAR((2, 4)),
            pltpu.SemaphoreType.REGULAR((2, 2)),
            dma((6,)),
            dma((2,)), dma((2 * NX,)),
            dma((4,)), dma((6,)), dma((6,)), dma((3,)),
            dma((4,)), dma((4,)),
            dma((1,)), dma((1,)),
            dma((3, len(STREAMS))), dma((3, len(STREAMS))),
            dma((2, 4)), dma((2, 4)),
        ],
        compiler_params=pltpu.CompilerParams(
            collective_id=0, has_side_effects=True, vmem_limit_bytes=58 * 1024 * 1024
        ),
        name="estep",
    )(
        images, projections.T.reshape(F // CHUNK, CHUNK, BLOCK), noise_power, class_logprior.reshape(1, CLASSES),
        groups.reshape(1, ROWS), offsets.reshape(1, ROWS),
    )
    out, evidence = pl.pallas_call(
        finish,
        out_shape=(
            jax.ShapeDtypeStruct((2, F), f32),
            jax.ShapeDtypeStruct((1, ROWS), f32),
        ),
        in_specs=[anywhere, anywhere],
        out_specs=(anywhere, anywhere),
        scratch_shapes=[
            pltpu.VMEM((NX, 2, W), f32),
            pltpu.VMEM((1, ROWS), f32),
            pltpu.VMEM((2, F), f32),
            dma((4,)),
        ],
        name="finish",
    )(out, evidence)
    return (out, evidence.reshape(ROWS))


def solution(mesh):
    in_specs = (
        P(("cls", "img"), None),
        P("cls", None),
        P(),
        P(),
        P(("cls", "img")),
        P(("cls", "img")),
    )
    out_specs = (P(("cls", "img"), None), P(("cls", "img")))
    return jax.shard_map(body, mesh=mesh, in_specs=in_specs, out_specs=out_specs, check_vma=False)
```

```python
import jax
import jax.numpy as jnp
from jax import lax
from jax.experimental import pallas as pl
from jax.experimental.pallas import tpu as pltpu
from jax.sharding import PartitionSpec as P

NX, NY, NZ = 4, 8, 8
F = 7200
W = 1920
TAG = 128
ROWS = 56
ALL = 2 * NX * ROWS
BLOCK = 128
CHUNKS = 4
PARTS = 2 * CHUNKS
CHUNK = W // PARTS
WHOLE = F // CHUNK - (NX - 1) * PARTS
STEPS = (0, 1, 3, 2)
EARLY = 6
LAST = F - (NX - 1) * W
WA = 1024
WB = W - WA
GROUPS = 32
CLASSES = 4
OWN = 8
STREAMS = (
    ("z", 1, 0, 256), ("z", -1, 256, 256), ("y", 1, 1024, 256), ("y", -1, 1280, 256),
    ("z", 1, 512, 256), ("z", -1, 768, 256), ("y", 1, 1536, 256), ("y", -1, 1792, 128),
)
NN = (((1,), (0,)), ((), ()))
f32 = jnp.float32
bf16 = jnp.bfloat16


def finish(fin_hbm, ev_hbm, out_hbm, evidence_hbm, fin_ref, ev_ref, out_ref, sem):
    load_fin = pltpu.make_async_copy(fin_hbm, fin_ref, sem.at[0])
    load_ev = pltpu.make_async_copy(ev_hbm, ev_ref, sem.at[1])
    store_ev = pltpu.make_async_copy(ev_ref, evidence_hbm, sem.at[2])
    store_out = pltpu.make_async_copy(out_ref, out_hbm, sem.at[3])
    load_fin.start()
    load_ev.start()
    load_ev.wait()
    store_ev.start()
    load_fin.wait()
    for k in range(NX):
        end = min(F, W * (k + 1))
        out_ref[:, W * k : end] = fin_ref[k, :, : end - W * k]
    store_out.start()
    store_ev.wait()
    store_out.wait()


def kernel(
    img_hbm, proj_hbm, noise_hbm, prior_hbm, group_hbm, offset_hbm, out_hbm, ev_hbm,
    prior_ref, group_ref, offset_ref, out_ref, ev_ref,
    img_v, noise_v, img_ref, xin, white, inv3, pbuf, qbuf, sc_send, sc_recv, post_send, post_recv,
    wt, parts, in1, mid1, in2, mid2, in3, own, got,
    near_up, near_down, load, img_s, img_r, ring_s, cross_r, pair_r, side_r, sc_s, sc_r,
    post_s, post_r,
    st_s, st_r, own_s, own_r,
):
    cls = lax.axis_index("cls")
    img = lax.axis_index("img")
    h, c = cls // 2, cls % 2
    lo, z, x = img // (NZ * NX), (img // NX) % NZ, img % NX
    y = 2 * h + lo
    turn = (0, 3 - 2 * lo, 1 + 2 * lo, 2)
    half = z % 2

    def device(y_, z_, x_, c_):
        return {"cls": (y_ // 2) * 2 + c_, "img": ((y_ % 2) * NZ + z_) * NX + x_}

    def group(dx, dc):
        return device(y, z, (x + dx) % NX, (c + dc) % 2)

    def along_y(d):
        return device((y + d) % NY, z, x, c)

    def along_z(d):
        return device(y, (z + d) % NZ, x, c)

    across = device((y + NY - 1 + 2 * lo) % NY, z, x, c)
    beside = device(y + 1 - 2 * lo, z, x, c)

    def copy(src, dst, send, recv, to):
        return pltpu.make_async_remote_copy(
            src_ref=src, dst_ref=dst, send_sem=send, recv_sem=recv,
            device_id=to, device_id_type=pl.DeviceIdType.MESH,
        )

    load_tags = [
        pltpu.make_async_copy(group_hbm, group_ref, load.at[6]),
        pltpu.make_async_copy(offset_hbm, offset_ref, load.at[7]),
    ]
    load_prior = pltpu.make_async_copy(prior_hbm, prior_ref, load.at[8])

    def load_img(k):
        lanes = pl.ds(W * k, min(F, W * (k + 1)) - W * k)
        dst = img_ref.at[k, :, pl.ds(0, W)] if k < NX - 1 else img_v
        return pltpu.make_async_copy(img_hbm.at[:, lanes], dst, load.at[9 + k])

    load_noise = pltpu.make_async_copy(noise_hbm, noise_v, load.at[1])

    load_proj = pltpu.make_async_copy(
        proj_hbm.at[pl.ds(x * PARTS, WHOLE)], pbuf.at[0, pl.ds(0, WHOLE)], load.at[2]
    )
    load_rest = pltpu.make_async_copy(
        proj_hbm.at[pl.ds((x % (NX - 1)) * PARTS + WHOLE, PARTS - WHOLE)],
        pbuf.at[0, pl.ds(WHOLE, PARTS - WHOLE)], load.at[3],
    )
    for one in load_tags:
        one.start()
    load_proj.start()

    @pl.when(x < NX - 1)
    def _():
        load_rest.start()

    for k in range(NX):
        load_img(k).start()
    load_prior.start()

    barrier = pltpu.get_barrier_semaphore()
    partners = [group(s // 2, s % 2) for s in range(1, 2 * NX)]
    partners += [along_y(1), along_y(NY - 1), along_z(1), along_z(NZ - 1)]
    for to in partners:
        pl.semaphore_signal(barrier, inc=1, device_id=to, device_id_type=pl.DeviceIdType.MESH)

    img_ref[NX - 1, :, LAST:W] = jnp.zeros((ROWS, W - LAST), bf16)
    tag = lax.broadcasted_iota(jnp.int32, (TAG, ROWS), 0)
    for one in load_tags:
        one.wait()
    is_group = (tag < 96) & (tag % 32 == group_ref[...])
    is_offset = (tag >= 96) & (tag < 108) & (tag % 4 == offset_ref[...])
    tags = jnp.transpose(jnp.where(is_group | is_offset, 1.0, 0.0).astype(f32)).astype(bf16)
    for k in range(NX):
        img_ref[k, :, W:] = tags
    load_proj.wait()

    @pl.when(x < NX - 1)
    def _():
        load_rest.wait()

    @pl.when(x == NX - 1)
    def _():
        pbuf[0, WHOLE:] = jnp.zeros((PARTS - WHOLE, CHUNK, BLOCK), bf16)

    for k in range(NX):
        load_img(k).wait()
    img_ref[NX - 1, :, :LAST] = img_v[...]
    load_noise.start()
    load_prior.wait()

    pl.semaphore_wait(barrier, len(partners))

    def turned(m, low):
        return (m + 2 * low) % CHUNKS

    def to_across(m):
        mine = half * CHUNKS + turned(m, 1 - lo)
        src, dst = (pbuf.at[0, mine], pbuf.at[1, mine])
        if m >= CHUNKS:
            src, dst = (pbuf.at[2, mine], pbuf.at[3, mine])
        return copy(src, dst, ring_s.at[0], cross_r.at[m], across)

    def from_across(m):
        return pbuf.at[1 if m < CHUNKS else 3, half * CHUNKS + turned(m, lo)]

    def to_beside(m):
        dst = pbuf.at[2 if m < CHUNKS else 3, half * CHUNKS + turned(m, lo)]
        return copy(from_across(m), dst, ring_s.at[1], pair_r.at[m], beside)

    def from_beside(m):
        return pbuf.at[2 if m < CHUNKS else 3, half * CHUNKS + turned(m, 1 - lo)]

    def to_side(way, m):
        ref = from_across(m) if way == 0 else from_beside(m)
        up = 1 - 2 * (turned(m, lo if way == 0 else 1 - lo) // 2)
        to = device(y, (z + NZ + up) % NZ, x, c)
        return copy(ref, ref, ring_s.at[2 + way], side_r.at[way if m < CHUNKS else 2], to)

    def sided(slot):
        ref = pbuf.at[slot, pl.ds((1 - half) * CHUNKS, CHUNKS)]
        copy(ref, ref, ring_s.at[2], side_r.at[slot - 1], along_z(1)).wait_recv()

    def crossed(m):
        ref = from_across(m)
        copy(ref, ref, ring_s.at[0], cross_r.at[m], across).wait_recv()
        to_beside(m).start()
        to_side(0, m).start()

    def paired(m):
        ref = from_beside(m)
        copy(ref, ref, ring_s.at[1], pair_r.at[m], beside).wait_recv()
        if m < 2:
            to_across(CHUNKS + m).start()
        to_side(1, m).start()

    def image(p):
        return copy(
            img_ref.at[(x + STEPS[p]) % NX], xin.at[2 * p], img_s.at[0], img_r.at[2 * p],
            group(STEPS[p], 0),
        )

    def to_sibling(p):
        src = img_ref.at[x] if p == 0 else xin.at[2 * p]
        s = 2 * p + 1
        return copy(src, xin.at[s], img_s.at[1], img_r.at[s], group(0, 1))

    def tell(r):
        for n, at in ((0, along_y), (1, along_z)):
            pl.semaphore_signal(
                near_up.at[n, r - 1], inc=1, device_id=at(1), device_id_type=pl.DeviceIdType.MESH
            )
            if r <= 2:
                pl.semaphore_signal(
                    near_down.at[n, r - 1], inc=1, device_id=at(7),
                    device_id_type=pl.DeviceIdType.MESH,
                )

    def told(r):
        for n in (0, 1):
            pl.semaphore_wait(near_up.at[n, r - 1], 1)
            if r <= 2:
                pl.semaphore_wait(near_down.at[n, r - 1], 1)
        if r < 4:
            tell(r + 1)

    for m in range(CHUNKS):
        to_across(m).start()
    tell(1)
    for p in (1, 2, 3):
        image(p).start()
    to_sibling(0).start()

    xin[0] = img_ref[x]
    load_noise.wait()

    def pieces(inv, width):
        hi = inv.astype(bf16)
        rest = inv - hi.astype(f32)
        mid = rest.astype(bf16)
        low = (rest - mid.astype(f32)).astype(bf16)
        inv3[0:GROUPS, :width] = hi
        inv3[GROUPS : 2 * GROUPS, :width] = mid
        inv3[2 * GROUPS : 3 * GROUPS, :width] = low

    inv3[3 * GROUPS :] = jnp.zeros((TAG - 3 * GROUPS, W), bf16)

    @pl.when(x < NX - 1)
    def _():
        pieces(1.0 / noise_v[:, pl.ds(pl.multiple_of(x * W, 128), W)], W)

    @pl.when(x == NX - 1)
    def _():
        pieces(1.0 / noise_v[:, F - LAST :], LAST)
        inv3[: 3 * GROUPS, LAST:] = jnp.zeros((3 * GROUPS, W - LAST), bf16)

    row = lax.broadcasted_iota(jnp.int32, (TAG, BLOCK), 0)
    piece = jnp.where(row < 96, row // 32, jnp.minimum((row - 96) // 4, 3))

    def block_of(slot):
        return pbuf[slot].reshape(W, BLOCK)

    def columns(slot):
        p = block_of(slot).astype(f32)
        square = p * p
        s_hi = square.astype(bf16)
        s_lo = (square - s_hi.astype(f32)).astype(bf16)
        q = lax.dot_general(inv3[...], s_hi, NN, preferred_element_type=f32)
        q += lax.dot_general(inv3[...], s_lo, NN, preferred_element_type=f32)
        q = q[0:32] + q[32:64] + q[64:96]
        prior = jnp.zeros((TAG, BLOCK), f32)
        for o in range(CLASSES):
            log_prior = prior_ref[0, (h + turn[slot] + CLASSES - o) % CLASSES]
            prior = jnp.where(row % CLASSES == o, log_prior * (1.0 / NX), prior)
        value = jnp.where(row < 96, -0.5 * jnp.concatenate([q] * 4, axis=0), prior)
        v_hi = value.astype(bf16).astype(f32)
        v_mid = (value - v_hi).astype(bf16).astype(f32)
        v_lo = value - v_hi - v_mid
        both = jnp.where(piece == 2, v_lo, 0.0)
        both = jnp.where(piece == 1, v_mid, both)
        qbuf[slot] = jnp.where(piece == 0, v_hi, both).astype(bf16)

    def image_arrived(p):
        image(p).wait_recv()
        to_sibling(p).start()

    def score_copy(slot, s):
        return copy(
            sc_send.at[slot, s], sc_recv.at[slot, s], sc_s.at[slot], sc_r.at[slot],
            group((NX - STEPS[s // 2]) % NX, s % 2),
        )

    def scores(slot, first, last):
        rows = (last - first) * ROWS
        part = lax.dot_general(
            white[first:last].reshape(rows, W), block_of(slot), NN, preferred_element_type=f32
        )
        part += lax.dot_general(
            xin[first:last, :, W:].reshape(rows, TAG), qbuf[slot], NN, preferred_element_type=f32
        )
        sc_send[slot, first:last] = part.reshape(last - first, ROWS, BLOCK)
        for s in (6, 7, 2, 4, 3, 5, 1):
            if first <= s < last:
                score_copy(slot, s).start()

    def whiten(s):
        inverse = jnp.dot(xin[s, :, W:], inv3[...], preferred_element_type=f32)
        white[s] = (xin[s, :, :W].astype(f32) * inverse).astype(bf16)

    whiten(0)
    columns(0)
    crossed(0)
    crossed(1)
    told(1)
    crossed(2)
    paired(0)
    crossed(3)
    told(2)
    image_arrived(1)
    image_arrived(2)
    paired(1)
    whiten(2)
    whiten(4)
    for s in (1, 3, 5):
        to_sibling(s // 2).wait_recv()
        whiten(s)
    paired(2)
    scores(0, 0, EARLY)
    crossed(4)
    paired(3)
    sided(1)
    crossed(5)
    columns(1)
    image_arrived(3)
    scores(1, 0, EARLY)
    whiten(6)
    paired(4)
    to_sibling(3).wait_recv()
    whiten(7)
    paired(5)
    scores(0, EARLY, 2 * NX)
    scores(1, EARLY, 2 * NX)
    told(3)
    sided(2)
    columns(2)
    scores(2, 0, 2 * NX)
    sided(3)
    told(4)
    columns(3)
    scores(3, 0, 2 * NX)

    total = {}
    for slot in range(4):
        ref = sc_recv.at[slot, pl.ds(1, 2 * NX - 1)]
        copy(ref, ref, sc_s.at[slot], sc_r.at[slot], group(1, 0)).wait_recv()
        for dc in (0, 1):
            terms = [sc_send[slot, 0]] if dc == 0 else [sc_recv[slot, 1]]
            terms += [sc_recv[slot, 2 * dx + dc] for dx in range(1, NX)]
            total[slot, dc] = (terms[0] + terms[1]) + (terms[2] + terms[3])
    peak = None
    for value in total.values():
        peak = value if peak is None else jnp.maximum(peak, value)
    peak = jnp.max(peak, axis=1, keepdims=True)
    mass = None
    for value in total.values():
        term = jnp.exp(value - peak)
        mass = term if mass is None else mass + term
    evidence = peak + jnp.log(jnp.sum(mass, axis=1, keepdims=True))
    ev_ref[...] = jnp.transpose(jnp.broadcast_to(evidence, (ROWS, TAG)))[0:1, :]
    store_ev = pltpu.make_async_copy(ev_ref, ev_hbm, load.at[4])
    store_ev.start()
    for (slot, dc), value in total.items():
        post_send[dc, slot] = jnp.exp(value - evidence).astype(bf16)

    def post_copy(s):
        return copy(
            post_send.at[s % 2], post_recv.at[s], post_s.at[0], post_r.at[0],
            group(STEPS[s // 2], s % 2),
        )

    for s in (6, 7, 2, 4, 3, 5, 1):
        post_copy(s).start()
    post_recv[0] = post_send[0]
    posts = post_recv.at[pl.ds(1, 2 * NX - 1)]
    all_posts = copy(posts, posts, post_s.at[0], post_r.at[0], group(1, 0))
    all_posts.wait_recv()

    for slot in range(4):
        wt[BLOCK * slot : BLOCK * (slot + 1)] = jnp.transpose(post_recv[:, slot].reshape(ALL, BLOCK))

    place = {"z": z, "y": y}
    other = {"z": "y", "y": "z"}

    def along(axis, d):
        at = (place[axis] + d + 8) % 8
        return device(y, at, x, c) if axis == "z" else device(at, z, x, c)

    def near(axis, side):
        return along(axis, side * (1 - 2 * (place[axis] % 2)))

    def stage1(i):
        axis, side = STREAMS[i][:2]
        return copy(
            parts[i].at[1 - place[axis] % 2], in1[i], st_s.at[0, i], st_r.at[0, i], near(axis, side)
        )

    def stage2(i):
        axis, side = STREAMS[i][:2]
        return copy(
            mid1[i].at[1 - place[other[axis]] % 2], in2[i], st_s.at[1, i], st_r.at[1, i],
            near(other[axis], side),
        )

    def stage3(i, d):
        axis = STREAMS[i][0]
        return copy(
            mid2[i].at[(place[axis] // 2 + d) % 4], in3[i].at[d - 1], st_s.at[2, i],
            st_r.at[2, i], along(axis, 2 * d),
        )

    def all3(i):
        return copy(in3[i], in3[i], st_s.at[2, i], st_r.at[2, i], along("z", 2))

    def last(axis, d, e):
        n = "zy".index(axis)
        at = (place[other[axis]] + 2 * d) % 8
        to = device(at, z, (x + e) % NX, c) if axis == "z" else device(y, at, (x + e) % NX, c)
        return copy(
            own[n].at[(place[other[axis]] // 2 + d) % 4, (x + e) % NX], got[n].at[d, x],
            own_s.at[n, d], own_r.at[n, d], to,
        )

    def self_copy(n, axis):
        return pltpu.make_async_copy(
            own[n].at[place[other[axis]] // 2, x], got[n].at[0, x], own_r.at[n, 0]
        )

    def last_in(n, d):
        return copy(got[n].at[d], got[n].at[d], own_s.at[n, d], own_r.at[n, d], group(1, 0))

    order = range(len(STREAMS))
    for i in order:
        axis, _, col, width = STREAMS[i]
        part = jnp.dot(
            wt[...], white[:, :, col : col + width].reshape(ALL, width), preferred_element_type=f32
        ).astype(bf16)
        for slot in range(4):
            y_half = (h + turn[slot]) % 4
            for r in range(2 * NZ):
                low, z_ = r // NZ, r % NZ
                at = BLOCK * slot + OWN * r
                if axis == "z":
                    parts[i][z_ % 2, low, z_ // 2, y_half] = part[at : at + OWN]
                else:
                    parts[i][low, z_ % 2, y_half, z_ // 2] = part[at : at + OWN]
        stage1(i).start()
    for i in order:
        axis = STREAMS[i][0]
        stage1(i).wait_recv()
        total = parts[i][place[axis] % 2].astype(f32) + in1[i][...].astype(f32)
        mid1[i][...] = total.astype(bf16)
        stage2(i).start()
    for i in order:
        axis = STREAMS[i][0]
        stage2(i).wait_recv()
        total = mid1[i][place[other[axis]] % 2].astype(f32) + in2[i][...].astype(f32)
        mid2[i][...] = total.astype(bf16)
        for d in (2, 1, 3):
            stage3(i, d).start()
    far_first = [(d, e) for d in (2, 1, 3, 0) for e in (2, 1, 3, 0) if d or e]
    for axis in "zy":
        n = "zy".index(axis)
        for i in order:
            if STREAMS[i][0] != axis:
                continue
            _, _, col, width = STREAMS[i]
            col -= WA * n
            acc = mid2[i][place[axis] // 2].astype(f32)
            all3(i).wait_recv()
            for d in (1, 3, 2):
                acc += in3[i][d - 1].astype(f32)
            for k in range(NX):
                own[n][:, k, :, col : col + width] = acc[:, 2 * k : 2 * k + 2].astype(bf16)
        for d, e in far_first:
            last(axis, d, e).start()
        self_copy(n, axis).start()
    for axis in "zy":
        n = "zy".index(axis)
        for d in (0, 1, 3, 2):
            last_in(n, d).wait_recv()
        acc = got[n][0].astype(f32)
        for d in range(1, 4):
            acc += got[n][d].astype(f32)
        out_ref[:, :, WA * n : WA * n + (WA, WB)[n]] = acc
    store_out = pltpu.make_async_copy(out_ref, out_hbm, load.at[5])
    store_out.start()

    def sent(ref, sem):
        copy(ref, ref, sem, cross_r.at[0], across).wait_send()

    for n in range(4):
        sent(pbuf.at[n, pl.ds(0, 6)], ring_s.at[n])
    sent(xin.at[pl.ds(0, NX - 1)], img_s.at[0])
    sent(xin.at[pl.ds(0, NX)], img_s.at[1])
    for slot in range(4):
        sent(sc_send.at[slot, pl.ds(1, 2 * NX - 1)], sc_s.at[slot])
    all_posts.wait_send()
    for i in order:
        stage1(i).wait_send()
        stage2(i).wait_send()
        all3(i).wait_send()
    for n in range(2):
        sent(own[n].at[0, pl.ds(0, NX - 1)], own_s.at[n, 0])
        for d in (1, 2, 3):
            sent(own[n].at[d], own_s.at[n, d])
    store_ev.wait()
    store_out.wait()


def body(images, projections, noise_power, class_logprior, groups, offsets):
    dma = pltpu.SemaphoreType.DMA
    anywhere = pl.BlockSpec(memory_space=pl.ANY)
    out, evidence = pl.pallas_call(
        kernel,
        out_shape=(
            jax.ShapeDtypeStruct((NX, 2, W), f32),
            jax.ShapeDtypeStruct((1, ROWS), f32),
        ),
        in_specs=[anywhere] * 6,
        out_specs=(anywhere, anywhere),
        scratch_shapes=[
            pltpu.SMEM((1, CLASSES), f32),
            pltpu.VMEM((1, ROWS), jnp.int32),
            pltpu.VMEM((1, ROWS), jnp.int32),
            pltpu.VMEM((NX, 2, W), f32),
            pltpu.VMEM((1, ROWS), f32),
            pltpu.VMEM((ROWS, LAST), bf16),
            pltpu.VMEM((GROUPS, F), f32),
            pltpu.VMEM((NX, ROWS, W + TAG), bf16),
            pltpu.VMEM((2 * NX, ROWS, W + TAG), bf16),
            pltpu.VMEM((2 * NX, ROWS, W), bf16),
            pltpu.VMEM((TAG, W), bf16),
            pltpu.VMEM((4, PARTS, CHUNK, BLOCK), bf16),
            pltpu.VMEM((4, TAG, BLOCK), bf16),
            pltpu.VMEM((4, 2 * NX, ROWS, BLOCK), f32),
            pltpu.VMEM((4, 2 * NX, ROWS, BLOCK), f32),
            pltpu.VMEM((2, 4, ROWS, BLOCK), bf16),
            pltpu.VMEM((2 * NX, 4, ROWS, BLOCK), bf16),
            pltpu.VMEM((4 * BLOCK, ALL), bf16),
            [pltpu.VMEM((2, 2, 4, 4, OWN, t[3]), bf16) for t in STREAMS],
            [pltpu.VMEM((2, 4, 4, OWN, t[3]), bf16) for t in STREAMS],
            [pltpu.VMEM((2, 4, 4, OWN, t[3]), bf16) for t in STREAMS],
            [pltpu.VMEM((4, 4, OWN, t[3]), bf16) for t in STREAMS],
            [pltpu.VMEM((4, 4, OWN, t[3]), bf16) for t in STREAMS],
            [pltpu.VMEM((3, 4, OWN, t[3]), bf16) for t in STREAMS],
            [pltpu.VMEM((4, NX, 2, t), bf16) for t in (WA, WB)],
            [pltpu.VMEM((4, NX, 2, t), bf16) for t in (WA, WB)],
            pltpu.SemaphoreType.REGULAR((2, 4)),
            pltpu.SemaphoreType.REGULAR((2, 2)),
            dma((9 + NX,)),
            dma((2,)), dma((2 * NX,)),
            dma((4,)), dma((6,)), dma((6,)), dma((3,)),
            dma((4,)), dma((4,)),
            dma((1,)), dma((1,)),
            dma((3, len(STREAMS))), dma((3, len(STREAMS))),
            dma((2, 4)), dma((2, 4)),
        ],
        compiler_params=pltpu.CompilerParams(
            collective_id=0, has_side_effects=True, vmem_limit_bytes=58 * 1024 * 1024
        ),
        name="estep",
    )(
        images, projections.T.reshape(F // CHUNK, CHUNK, BLOCK), noise_power, class_logprior.reshape(1, CLASSES),
        groups.reshape(1, ROWS), offsets.reshape(1, ROWS),
    )
    out, evidence = pl.pallas_call(
        finish,
        out_shape=(
            jax.ShapeDtypeStruct((2, F), f32),
            jax.ShapeDtypeStruct((1, ROWS), f32),
        ),
        in_specs=[anywhere, anywhere],
        out_specs=(anywhere, anywhere),
        scratch_shapes=[
            pltpu.VMEM((NX, 2, W), f32),
            pltpu.VMEM((1, ROWS), f32),
            pltpu.VMEM((2, F), f32),
            dma((4,)),
        ],
        name="finish",
    )(out, evidence)
    return (out, evidence.reshape(ROWS))


def solution(mesh):
    in_specs = (
        P(("cls", "img"), None),
        P("cls", None),
        P(),
        P(),
        P(("cls", "img")),
        P(("cls", "img")),
    )
    out_specs = (P(("cls", "img"), None), P(("cls", "img")))
    return jax.shard_map(body, mesh=mesh, in_specs=in_specs, out_specs=out_specs, check_vma=False)
```

```python
import jax
import jax.numpy as jnp
from jax import lax
from jax.experimental import pallas as pl
from jax.experimental.pallas import tpu as pltpu
from jax.sharding import PartitionSpec as P

NX, NY, NZ = 4, 8, 8
F = 7200
W = 1920
TAG = 128
ROWS = 56
ALL = 2 * NX * ROWS
BLOCK = 128
CHUNKS = 4
PARTS = 2 * CHUNKS
CHUNK = W // PARTS
WHOLE = F // CHUNK - (NX - 1) * PARTS
STEPS = (0, 1, 3, 2)
EARLY = 6
PARTED = ((0, 32), (32, 24))
LAST = F - (NX - 1) * W
WA = 1024
WB = W - WA
GROUPS = 32
CLASSES = 4
OWN = 8
STREAMS = (
    ("z", 1, 0, 256), ("z", -1, 256, 256), ("y", 1, 1024, 256), ("y", -1, 1280, 256),
    ("z", 1, 512, 256), ("z", -1, 768, 256), ("y", 1, 1536, 256), ("y", -1, 1792, 128),
)
NN = (((1,), (0,)), ((), ()))
f32 = jnp.float32
bf16 = jnp.bfloat16


def finish(fin_hbm, ev_hbm, out_hbm, evidence_hbm, fin_ref, ev_ref, out_ref, sem):
    load_fin = pltpu.make_async_copy(fin_hbm, fin_ref, sem.at[0])
    load_ev = pltpu.make_async_copy(ev_hbm, ev_ref, sem.at[1])
    store_ev = pltpu.make_async_copy(ev_ref, evidence_hbm, sem.at[2])
    store_out = pltpu.make_async_copy(out_ref, out_hbm, sem.at[3])
    load_fin.start()
    load_ev.start()
    load_ev.wait()
    store_ev.start()
    load_fin.wait()
    for k in range(NX):
        end = min(F, W * (k + 1))
        out_ref[:, W * k : end] = fin_ref[k, :, : end - W * k]
    store_out.start()
    store_ev.wait()
    store_out.wait()


def kernel(
    img_hbm, proj_hbm, noise_hbm, prior_hbm, group_hbm, offset_hbm, out_hbm, ev_hbm,
    prior_ref, group_ref, offset_ref, out_ref, ev_ref,
    img_v, noise_v, img_ref, xin, white, inv3, pbuf, qbuf, sc_send, sc_recv, post_send, post_recv,
    wt, parts, in1, mid1, in2, mid2, in3, own, got,
    near_up, near_down, load, img_s, img_r, ring_s, cross_r, pair_r, side_r, sc_s, sc_r,
    post_s, post_r,
    st_s, st_r, own_s, own_r,
):
    cls = lax.axis_index("cls")
    img = lax.axis_index("img")
    h, c = cls // 2, cls % 2
    lo, z, x = img // (NZ * NX), (img // NX) % NZ, img % NX
    y = 2 * h + lo
    turn = (0, 3 - 2 * lo, 1 + 2 * lo, 2)
    half = z % 2

    def device(y_, z_, x_, c_):
        return {"cls": (y_ // 2) * 2 + c_, "img": ((y_ % 2) * NZ + z_) * NX + x_}

    def group(dx, dc):
        return device(y, z, (x + dx) % NX, (c + dc) % 2)

    def along_y(d):
        return device((y + d) % NY, z, x, c)

    def along_z(d):
        return device(y, (z + d) % NZ, x, c)

    across = device((y + NY - 1 + 2 * lo) % NY, z, x, c)
    beside = device(y + 1 - 2 * lo, z, x, c)

    def copy(src, dst, send, recv, to):
        return pltpu.make_async_remote_copy(
            src_ref=src, dst_ref=dst, send_sem=send, recv_sem=recv,
            device_id=to, device_id_type=pl.DeviceIdType.MESH,
        )

    load_tags = [
        pltpu.make_async_copy(group_hbm, group_ref, load.at[6]),
        pltpu.make_async_copy(offset_hbm, offset_ref, load.at[7]),
    ]
    load_prior = pltpu.make_async_copy(prior_hbm, prior_ref, load.at[8])

    def load_img(k):
        lanes = pl.ds(W * k, min(F, W * (k + 1)) - W * k)
        dst = img_ref.at[k, :, pl.ds(0, W)] if k < NX - 1 else img_v
        return pltpu.make_async_copy(img_hbm.at[:, lanes], dst, load.at[9 + k])

    load_noise = pltpu.make_async_copy(noise_hbm, noise_v, load.at[1])

    load_proj = pltpu.make_async_copy(
        proj_hbm.at[pl.ds(x * PARTS, WHOLE)], pbuf.at[0, pl.ds(0, WHOLE)], load.at[2]
    )
    load_rest = pltpu.make_async_copy(
        proj_hbm.at[pl.ds((x % (NX - 1)) * PARTS + WHOLE, PARTS - WHOLE)],
        pbuf.at[0, pl.ds(WHOLE, PARTS - WHOLE)], load.at[3],
    )
    for one in load_tags:
        one.start()
    load_proj.start()

    @pl.when(x < NX - 1)
    def _():
        load_rest.start()

    for k in range(NX):
        load_img(k).start()
    load_prior.start()

    barrier = pltpu.get_barrier_semaphore()
    partners = [group(s // 2, s % 2) for s in range(1, 2 * NX)]
    partners += [along_y(1), along_y(NY - 1), along_z(1), along_z(NZ - 1)]
    for to in partners:
        pl.semaphore_signal(barrier, inc=1, device_id=to, device_id_type=pl.DeviceIdType.MESH)

    img_ref[NX - 1, :, LAST:W] = jnp.zeros((ROWS, W - LAST), bf16)
    tag = lax.broadcasted_iota(jnp.int32, (TAG, ROWS), 0)
    for one in load_tags:
        one.wait()
    is_group = (tag < 96) & (tag % 32 == group_ref[...])
    is_offset = (tag >= 96) & (tag < 108) & (tag % 4 == offset_ref[...])
    tags = jnp.transpose(jnp.where(is_group | is_offset, 1.0, 0.0).astype(f32)).astype(bf16)
    for k in range(NX):
        img_ref[k, :, W:] = tags
    load_proj.wait()

    @pl.when(x < NX - 1)
    def _():
        load_rest.wait()

    @pl.when(x == NX - 1)
    def _():
        pbuf[0, WHOLE:] = jnp.zeros((PARTS - WHOLE, CHUNK, BLOCK), bf16)

    for k in range(NX):
        load_img(k).wait()
    img_ref[NX - 1, :, :LAST] = img_v[...]
    load_noise.start()
    load_prior.wait()

    pl.semaphore_wait(barrier, len(partners))

    def turned(m, low):
        return (m + 2 * low) % CHUNKS

    def to_across(m):
        mine = half * CHUNKS + turned(m, 1 - lo)
        src, dst = (pbuf.at[0, mine], pbuf.at[1, mine])
        if m >= CHUNKS:
            src, dst = (pbuf.at[2, mine], pbuf.at[3, mine])
        return copy(src, dst, ring_s.at[0], cross_r.at[m], across)

    def from_across(m):
        return pbuf.at[1 if m < CHUNKS else 3, half * CHUNKS + turned(m, lo)]

    def to_beside(m):
        dst = pbuf.at[2 if m < CHUNKS else 3, half * CHUNKS + turned(m, lo)]
        return copy(from_across(m), dst, ring_s.at[1], pair_r.at[m], beside)

    def from_beside(m):
        return pbuf.at[2 if m < CHUNKS else 3, half * CHUNKS + turned(m, 1 - lo)]

    def to_side(way, m):
        ref = from_across(m) if way == 0 else from_beside(m)
        up = 1 - 2 * (turned(m, lo if way == 0 else 1 - lo) // 2)
        to = device(y, (z + NZ + up) % NZ, x, c)
        return copy(ref, ref, ring_s.at[2 + way], side_r.at[way if m < CHUNKS else 2], to)

    def sided(slot):
        ref = pbuf.at[slot, pl.ds((1 - half) * CHUNKS, CHUNKS)]
        copy(ref, ref, ring_s.at[2], side_r.at[slot - 1], along_z(1)).wait_recv()

    def crossed(m):
        ref = from_across(m)
        copy(ref, ref, ring_s.at[0], cross_r.at[m], across).wait_recv()
        to_beside(m).start()
        to_side(0, m).start()

    def paired(m):
        ref = from_beside(m)
        copy(ref, ref, ring_s.at[1], pair_r.at[m], beside).wait_recv()
        if m < 2:
            to_across(CHUNKS + m).start()
        to_side(1, m).start()

    def image(p):
        return copy(
            img_ref.at[(x + STEPS[p]) % NX], xin.at[2 * p], img_s.at[0], img_r.at[2 * p],
            group(STEPS[p], 0),
        )

    def to_sibling(p):
        src = img_ref.at[x] if p == 0 else xin.at[2 * p]
        s = 2 * p + 1
        return copy(src, xin.at[s], img_s.at[1], img_r.at[s], group(0, 1))

    def tell(r):
        for n, at in ((0, along_y), (1, along_z)):
            pl.semaphore_signal(
                near_up.at[n, r - 1], inc=1, device_id=at(1), device_id_type=pl.DeviceIdType.MESH
            )
            if r <= 2:
                pl.semaphore_signal(
                    near_down.at[n, r - 1], inc=1, device_id=at(7),
                    device_id_type=pl.DeviceIdType.MESH,
                )

    def told(r):
        for n in (0, 1):
            pl.semaphore_wait(near_up.at[n, r - 1], 1)
            if r <= 2:
                pl.semaphore_wait(near_down.at[n, r - 1], 1)
        if r < 4:
            tell(r + 1)

    for m in range(CHUNKS):
        to_across(m).start()
    tell(1)
    for p in (1, 2, 3):
        image(p).start()
    to_sibling(0).start()

    xin[0] = img_ref[x]
    load_noise.wait()

    def pieces(inv, width):
        hi = inv.astype(bf16)
        rest = inv - hi.astype(f32)
        mid = rest.astype(bf16)
        low = (rest - mid.astype(f32)).astype(bf16)
        inv3[0:GROUPS, :width] = hi
        inv3[GROUPS : 2 * GROUPS, :width] = mid
        inv3[2 * GROUPS : 3 * GROUPS, :width] = low

    inv3[3 * GROUPS :] = jnp.zeros((TAG - 3 * GROUPS, W), bf16)

    @pl.when(x < NX - 1)
    def _():
        pieces(1.0 / noise_v[:, pl.ds(pl.multiple_of(x * W, 128), W)], W)

    @pl.when(x == NX - 1)
    def _():
        pieces(1.0 / noise_v[:, F - LAST :], LAST)
        inv3[: 3 * GROUPS, LAST:] = jnp.zeros((3 * GROUPS, W - LAST), bf16)

    row = lax.broadcasted_iota(jnp.int32, (TAG, BLOCK), 0)
    piece = jnp.where(row < 96, row // 32, jnp.minimum((row - 96) // 4, 3))

    def block_of(slot):
        return pbuf[slot].reshape(W, BLOCK)

    def columns(slot):
        p = block_of(slot).astype(f32)
        square = p * p
        s_hi = square.astype(bf16)
        s_lo = (square - s_hi.astype(f32)).astype(bf16)
        q = lax.dot_general(inv3[...], s_hi, NN, preferred_element_type=f32)
        q += lax.dot_general(inv3[...], s_lo, NN, preferred_element_type=f32)
        q = q[0:32] + q[32:64] + q[64:96]
        prior = jnp.zeros((TAG, BLOCK), f32)
        for o in range(CLASSES):
            log_prior = prior_ref[0, (h + turn[slot] + CLASSES - o) % CLASSES]
            prior = jnp.where(row % CLASSES == o, log_prior * (1.0 / NX), prior)
        value = jnp.where(row < 96, -0.5 * jnp.concatenate([q] * 4, axis=0), prior)
        v_hi = value.astype(bf16).astype(f32)
        v_mid = (value - v_hi).astype(bf16).astype(f32)
        v_lo = value - v_hi - v_mid
        both = jnp.where(piece == 2, v_lo, 0.0)
        both = jnp.where(piece == 1, v_mid, both)
        qbuf[slot] = jnp.where(piece == 0, v_hi, both).astype(bf16)

    def image_arrived(p):
        image(p).wait_recv()
        to_sibling(p).start()

    def score_copy(slot, s):
        return copy(
            sc_send.at[slot, s], sc_recv.at[slot, s], sc_s.at[slot], sc_r.at[slot],
            group((NX - STEPS[s // 2]) % NX, s % 2),
        )

    def score_part(n, s):
        rows = pl.ds(*PARTED[n])
        return copy(
            sc_send.at[3, s, rows], sc_recv.at[3, s, rows], sc_s.at[3 + n], sc_r.at[3 + n],
            group((NX - STEPS[s // 2]) % NX, s % 2),
        )

    def scores(slot, first, last):
        rows = (last - first) * ROWS
        part = lax.dot_general(
            white[first:last].reshape(rows, W), block_of(slot), NN, preferred_element_type=f32
        )
        part += lax.dot_general(
            xin[first:last, :, W:].reshape(rows, TAG), qbuf[slot], NN, preferred_element_type=f32
        )
        sc_send[slot, first:last] = part.reshape(last - first, ROWS, BLOCK)
        if slot == 3:
            for n in range(2):
                for s in (6, 7, 2, 4, 3, 5, 1):
                    score_part(n, s).start()
            return
        for s in (6, 7, 2, 4, 3, 5, 1):
            if first <= s < last:
                score_copy(slot, s).start()

    def whiten(s):
        inverse = jnp.dot(xin[s, :, W:], inv3[...], preferred_element_type=f32)
        white[s] = (xin[s, :, :W].astype(f32) * inverse).astype(bf16)

    whiten(0)
    columns(0)
    crossed(0)
    crossed(1)
    told(1)
    crossed(2)
    paired(0)
    crossed(3)
    told(2)
    image_arrived(1)
    image_arrived(2)
    paired(1)
    whiten(2)
    whiten(4)
    for s in (1, 3, 5):
        to_sibling(s // 2).wait_recv()
        whiten(s)
    paired(2)
    scores(0, 0, EARLY)
    crossed(4)
    paired(3)
    sided(1)
    crossed(5)
    columns(1)
    image_arrived(3)
    scores(1, 0, EARLY)
    whiten(6)
    paired(4)
    to_sibling(3).wait_recv()
    whiten(7)
    paired(5)
    scores(0, EARLY, 2 * NX)
    scores(1, EARLY, 2 * NX)
    told(3)
    sided(2)
    columns(2)
    scores(2, 0, 2 * NX)
    sided(3)
    told(4)
    columns(3)
    scores(3, 0, 2 * NX)

    def all_scores(slot, n=0):
        ref = sc_recv.at[slot, pl.ds(1, 2 * NX - 1)]
        if slot == 3:
            ref = sc_recv.at[slot, pl.ds(1, 2 * NX - 1), pl.ds(*PARTED[n])]
        return copy(ref, ref, sc_s.at[slot + n], sc_r.at[slot + n], group(1, 0))

    def post_copy(n, s):
        rows = pl.ds(*PARTED[n])
        return copy(
            post_send.at[s % 2, :, rows], post_recv.at[s, :, rows], post_s.at[n], post_r.at[n],
            group(STEPS[s // 2], s % 2),
        )

    def all_posts(n):
        ref = post_recv.at[pl.ds(1, 2 * NX - 1), :, pl.ds(*PARTED[n])]
        return copy(ref, ref, post_s.at[n], post_r.at[n], group(1, 0))

    for slot in range(3):
        all_scores(slot).wait_recv()
    evidences = []
    for n in range(2):
        first, rows = PARTED[n]
        here = slice(first, first + rows)
        all_scores(3, n).wait_recv()
        total = {}
        for slot in range(4):
            for dc in (0, 1):
                terms = [sc_send[slot, 0, here]] if dc == 0 else [sc_recv[slot, 1, here]]
                terms += [sc_recv[slot, 2 * dx + dc, here] for dx in range(1, NX)]
                total[slot, dc] = (terms[0] + terms[1]) + (terms[2] + terms[3])
        peak = None
        for value in total.values():
            peak = value if peak is None else jnp.maximum(peak, value)
        peak = jnp.max(peak, axis=1, keepdims=True)
        mass = None
        for value in total.values():
            term = jnp.exp(value - peak)
            mass = term if mass is None else mass + term
        evidence = peak + jnp.log(jnp.sum(mass, axis=1, keepdims=True))
        evidences.append(evidence)
        for (slot, dc), value in total.items():
            post_send[dc, slot, here] = jnp.exp(value - evidence).astype(bf16)
        for s in (6, 7, 2, 4, 3, 5, 1):
            post_copy(n, s).start()

    evidence = jnp.broadcast_to(jnp.concatenate(evidences, axis=0), (ROWS, TAG))
    ev_ref[...] = jnp.transpose(evidence)[0:1, :]
    store_ev = pltpu.make_async_copy(ev_ref, ev_hbm, load.at[4])
    store_ev.start()
    post_recv[0] = post_send[0]
    for n in range(2):
        all_posts(n).wait_recv()

    for slot in range(4):
        wt[BLOCK * slot : BLOCK * (slot + 1)] = jnp.transpose(post_recv[:, slot].reshape(ALL, BLOCK))

    place = {"z": z, "y": y}
    other = {"z": "y", "y": "z"}

    def along(axis, d):
        at = (place[axis] + d + 8) % 8
        return device(y, at, x, c) if axis == "z" else device(at, z, x, c)

    def near(axis, side):
        return along(axis, side * (1 - 2 * (place[axis] % 2)))

    def stage1(i):
        axis, side = STREAMS[i][:2]
        return copy(
            parts[i].at[1 - place[axis] % 2], in1[i], st_s.at[0, i], st_r.at[0, i], near(axis, side)
        )

    def stage2(i):
        axis, side = STREAMS[i][:2]
        return copy(
            mid1[i].at[1 - place[other[axis]] % 2], in2[i], st_s.at[1, i], st_r.at[1, i],
            near(other[axis], side),
        )

    def stage3(i, d):
        axis = STREAMS[i][0]
        return copy(
            mid2[i].at[(place[axis] // 2 + d) % 4], in3[i].at[d - 1], st_s.at[2, i],
            st_r.at[2, i], along(axis, 2 * d),
        )

    def all3(i):
        return copy(in3[i], in3[i], st_s.at[2, i], st_r.at[2, i], along("z", 2))

    def last(axis, d, e):
        n = "zy".index(axis)
        at = (place[other[axis]] + 2 * d) % 8
        to = device(at, z, (x + e) % NX, c) if axis == "z" else device(y, at, (x + e) % NX, c)
        return copy(
            own[n].at[(place[other[axis]] // 2 + d) % 4, (x + e) % NX], got[n].at[d, x],
            own_s.at[n, d], own_r.at[n, d], to,
        )

    def self_copy(n, axis):
        return pltpu.make_async_copy(
            own[n].at[place[other[axis]] // 2, x], got[n].at[0, x], own_r.at[n, 0]
        )

    def last_in(n, d):
        return copy(got[n].at[d], got[n].at[d], own_s.at[n, d], own_r.at[n, d], group(1, 0))

    order = range(len(STREAMS))
    for i in order:
        axis, _, col, width = STREAMS[i]
        part = jnp.dot(
            wt[...], white[:, :, col : col + width].reshape(ALL, width), preferred_element_type=f32
        ).astype(bf16)
        for slot in range(4):
            y_half = (h + turn[slot]) % 4
            for r in range(2 * NZ):
                low, z_ = r // NZ, r % NZ
                at = BLOCK * slot + OWN * r
                if axis == "z":
                    parts[i][z_ % 2, low, z_ // 2, y_half] = part[at : at + OWN]
                else:
                    parts[i][low, z_ % 2, y_half, z_ // 2] = part[at : at + OWN]
        stage1(i).start()
    for i in order:
        axis = STREAMS[i][0]
        stage1(i).wait_recv()
        total = parts[i][place[axis] % 2].astype(f32) + in1[i][...].astype(f32)
        mid1[i][...] = total.astype(bf16)
        stage2(i).start()
    for i in order:
        axis = STREAMS[i][0]
        stage2(i).wait_recv()
        total = mid1[i][place[other[axis]] % 2].astype(f32) + in2[i][...].astype(f32)
        mid2[i][...] = total.astype(bf16)
        for d in (2, 1, 3):
            stage3(i, d).start()
    far_first = [(d, e) for d in (2, 1, 3, 0) for e in (2, 1, 3, 0) if d or e]
    for axis in "zy":
        n = "zy".index(axis)
        for i in order:
            if STREAMS[i][0] != axis:
                continue
            _, _, col, width = STREAMS[i]
            col -= WA * n
            acc = mid2[i][place[axis] // 2].astype(f32)
            all3(i).wait_recv()
            for d in (1, 3, 2):
                acc += in3[i][d - 1].astype(f32)
            for k in range(NX):
                own[n][:, k, :, col : col + width] = acc[:, 2 * k : 2 * k + 2].astype(bf16)
        for d, e in far_first:
            last(axis, d, e).start()
        self_copy(n, axis).start()
    for axis in "zy":
        n = "zy".index(axis)
        for d in (0, 1, 3, 2):
            last_in(n, d).wait_recv()
        acc = got[n][0].astype(f32)
        for d in range(1, 4):
            acc += got[n][d].astype(f32)
        out_ref[:, :, WA * n : WA * n + (WA, WB)[n]] = acc
    store_out = pltpu.make_async_copy(out_ref, out_hbm, load.at[5])
    store_out.start()

    def sent(ref, sem):
        copy(ref, ref, sem, cross_r.at[0], across).wait_send()

    for n in range(4):
        sent(pbuf.at[n, pl.ds(0, 6)], ring_s.at[n])
    sent(xin.at[pl.ds(0, NX - 1)], img_s.at[0])
    sent(xin.at[pl.ds(0, NX)], img_s.at[1])
    for slot in range(3):
        all_scores(slot).wait_send()
    for n in range(2):
        all_scores(3, n).wait_send()
        all_posts(n).wait_send()
    for i in order:
        stage1(i).wait_send()
        stage2(i).wait_send()
        all3(i).wait_send()
    for n in range(2):
        sent(own[n].at[0, pl.ds(0, NX - 1)], own_s.at[n, 0])
        for d in (1, 2, 3):
            sent(own[n].at[d], own_s.at[n, d])
    store_ev.wait()
    store_out.wait()


def body(images, projections, noise_power, class_logprior, groups, offsets):
    dma = pltpu.SemaphoreType.DMA
    anywhere = pl.BlockSpec(memory_space=pl.ANY)
    out, evidence = pl.pallas_call(
        kernel,
        out_shape=(
            jax.ShapeDtypeStruct((NX, 2, W), f32),
            jax.ShapeDtypeStruct((1, ROWS), f32),
        ),
        in_specs=[anywhere] * 6,
        out_specs=(anywhere, anywhere),
        scratch_shapes=[
            pltpu.SMEM((1, CLASSES), f32),
            pltpu.VMEM((1, ROWS), jnp.int32),
            pltpu.VMEM((1, ROWS), jnp.int32),
            pltpu.VMEM((NX, 2, W), f32),
            pltpu.VMEM((1, ROWS), f32),
            pltpu.VMEM((ROWS, LAST), bf16),
            pltpu.VMEM((GROUPS, F), f32),
            pltpu.VMEM((NX, ROWS, W + TAG), bf16),
            pltpu.VMEM((2 * NX, ROWS, W + TAG), bf16),
            pltpu.VMEM((2 * NX, ROWS, W), bf16),
            pltpu.VMEM((TAG, W), bf16),
            pltpu.VMEM((4, PARTS, CHUNK, BLOCK), bf16),
            pltpu.VMEM((4, TAG, BLOCK), bf16),
            pltpu.VMEM((4, 2 * NX, ROWS, BLOCK), f32),
            pltpu.VMEM((4, 2 * NX, ROWS, BLOCK), f32),
            pltpu.VMEM((2, 4, ROWS, BLOCK), bf16),
            pltpu.VMEM((2 * NX, 4, ROWS, BLOCK), bf16),
            pltpu.VMEM((4 * BLOCK, ALL), bf16),
            [pltpu.VMEM((2, 2, 4, 4, OWN, t[3]), bf16) for t in STREAMS],
            [pltpu.VMEM((2, 4, 4, OWN, t[3]), bf16) for t in STREAMS],
            [pltpu.VMEM((2, 4, 4, OWN, t[3]), bf16) for t in STREAMS],
            [pltpu.VMEM((4, 4, OWN, t[3]), bf16) for t in STREAMS],
            [pltpu.VMEM((4, 4, OWN, t[3]), bf16) for t in STREAMS],
            [pltpu.VMEM((3, 4, OWN, t[3]), bf16) for t in STREAMS],
            [pltpu.VMEM((4, NX, 2, t), bf16) for t in (WA, WB)],
            [pltpu.VMEM((4, NX, 2, t), bf16) for t in (WA, WB)],
            pltpu.SemaphoreType.REGULAR((2, 4)),
            pltpu.SemaphoreType.REGULAR((2, 2)),
            dma((9 + NX,)),
            dma((2,)), dma((2 * NX,)),
            dma((4,)), dma((6,)), dma((6,)), dma((3,)),
            dma((5,)), dma((5,)),
            dma((2,)), dma((2,)),
            dma((3, len(STREAMS))), dma((3, len(STREAMS))),
            dma((2, 4)), dma((2, 4)),
        ],
        compiler_params=pltpu.CompilerParams(
            collective_id=0, has_side_effects=True, vmem_limit_bytes=58 * 1024 * 1024
        ),
        name="estep",
    )(
        images, projections.T.reshape(F // CHUNK, CHUNK, BLOCK), noise_power, class_logprior.reshape(1, CLASSES),
        groups.reshape(1, ROWS), offsets.reshape(1, ROWS),
    )
    out, evidence = pl.pallas_call(
        finish,
        out_shape=(
            jax.ShapeDtypeStruct((2, F), f32),
            jax.ShapeDtypeStruct((1, ROWS), f32),
        ),
        in_specs=[anywhere, anywhere],
        out_specs=(anywhere, anywhere),
        scratch_shapes=[
            pltpu.VMEM((NX, 2, W), f32),
            pltpu.VMEM((1, ROWS), f32),
            pltpu.VMEM((2, F), f32),
            dma((4,)),
        ],
        name="finish",
    )(out, evidence)
    return (out, evidence.reshape(ROWS))


def solution(mesh):
    in_specs = (
        P(("cls", "img"), None),
        P("cls", None),
        P(),
        P(),
        P(("cls", "img")),
        P(("cls", "img")),
    )
    out_specs = (P(("cls", "img"), None), P(("cls", "img")))
    return jax.shard_map(body, mesh=mesh, in_specs=in_specs, out_specs=out_specs, check_vma=False)
```

```python
import jax
import jax.numpy as jnp
from jax import lax
from jax.experimental import pallas as pl
from jax.experimental.pallas import tpu as pltpu
from jax.sharding import PartitionSpec as P

NX, NY, NZ = 4, 8, 8
F = 7200
W = 1920
TAG = 128
ROWS = 56
ALL = 2 * NX * ROWS
BLOCK = 128
CHUNKS = 4
PARTS = 2 * CHUNKS
CHUNK = W // PARTS
WHOLE = F // CHUNK - (NX - 1) * PARTS
STEPS = (0, 1, 3, 2)
EARLY = 6
PARTED = ((0, 32), (32, 24))
LAST = F - (NX - 1) * W
WA = 1024
WB = W - WA
GROUPS = 32
CLASSES = 4
OWN = 8
STREAMS = (
    ("z", 1, 0, 256), ("z", -1, 256, 256), ("y", 1, 1024, 256), ("y", -1, 1280, 256),
    ("z", 1, 512, 256), ("z", -1, 768, 256), ("y", 1, 1536, 256), ("y", -1, 1792, 128),
)
NN = (((1,), (0,)), ((), ()))
f32 = jnp.float32
bf16 = jnp.bfloat16


def finish(fin_hbm, ev_hbm, out_hbm, evidence_hbm, fin_ref, ev_ref, out_ref, sem):
    load_fin = pltpu.make_async_copy(fin_hbm, fin_ref, sem.at[0])
    load_ev = pltpu.make_async_copy(ev_hbm, ev_ref, sem.at[1])
    store_ev = pltpu.make_async_copy(ev_ref, evidence_hbm, sem.at[2])
    store_out = pltpu.make_async_copy(out_ref, out_hbm, sem.at[3])
    load_fin.start()
    load_ev.start()
    load_ev.wait()
    store_ev.start()
    load_fin.wait()
    for k in range(NX):
        end = min(F, W * (k + 1))
        out_ref[:, W * k : end] = fin_ref[k, :, : end - W * k]
    store_out.start()
    store_ev.wait()
    store_out.wait()


def kernel(
    img_hbm, proj_hbm, noise_hbm, prior_hbm, group_hbm, offset_hbm, out_hbm, ev_hbm,
    prior_ref, group_ref, offset_ref, out_ref, ev_ref,
    img_v, noise_v, img_ref, xin, white, inv3, pbuf, qbuf, sc_send, sc_recv, post_send, post_recv,
    wt, parts, in1, mid1, in2, mid2, in3, own, got,
    near_up, near_down, load, img_s, img_r, ring_s, cross_r, pair_r, side_r, sc_s, sc_r,
    post_s, post_r,
    st_s, st_r, own_s, own_r,
):
    cls = lax.axis_index("cls")
    img = lax.axis_index("img")
    h, c = cls // 2, cls % 2
    lo, z, x = img // (NZ * NX), (img // NX) % NZ, img % NX
    y = 2 * h + lo
    turn = (0, 3 - 2 * lo, 1 + 2 * lo, 2)
    half = z % 2

    def device(y_, z_, x_, c_):
        return {"cls": (y_ // 2) * 2 + c_, "img": ((y_ % 2) * NZ + z_) * NX + x_}

    def group(dx, dc):
        return device(y, z, (x + dx) % NX, (c + dc) % 2)

    def along_y(d):
        return device((y + d) % NY, z, x, c)

    def along_z(d):
        return device(y, (z + d) % NZ, x, c)

    across = device((y + NY - 1 + 2 * lo) % NY, z, x, c)
    beside = device(y + 1 - 2 * lo, z, x, c)

    def copy(src, dst, send, recv, to):
        return pltpu.make_async_remote_copy(
            src_ref=src, dst_ref=dst, send_sem=send, recv_sem=recv,
            device_id=to, device_id_type=pl.DeviceIdType.MESH,
        )

    load_tags = [
        pltpu.make_async_copy(group_hbm, group_ref, load.at[7]),
        pltpu.make_async_copy(offset_hbm, offset_ref, load.at[8]),
    ]
    load_prior = pltpu.make_async_copy(prior_hbm, prior_ref, load.at[9])

    def load_img(k):
        lanes = pl.ds(W * k, min(F, W * (k + 1)) - W * k)
        dst = img_ref.at[k, :, pl.ds(0, W)] if k < NX - 1 else img_v
        return pltpu.make_async_copy(img_hbm.at[:, lanes], dst, load.at[10 + k])

    load_noise = pltpu.make_async_copy(noise_hbm, noise_v, load.at[1])

    load_proj = pltpu.make_async_copy(
        proj_hbm.at[pl.ds(x * PARTS, WHOLE)], pbuf.at[0, pl.ds(0, WHOLE)], load.at[2]
    )
    load_rest = pltpu.make_async_copy(
        proj_hbm.at[pl.ds((x % (NX - 1)) * PARTS + WHOLE, PARTS - WHOLE)],
        pbuf.at[0, pl.ds(WHOLE, PARTS - WHOLE)], load.at[3],
    )
    for one in load_tags:
        one.start()
    load_proj.start()

    @pl.when(x < NX - 1)
    def _():
        load_rest.start()

    for k in range(NX):
        load_img(k).start()
    load_prior.start()

    barrier = pltpu.get_barrier_semaphore()
    partners = [group(s // 2, s % 2) for s in range(1, 2 * NX)]
    partners += [along_y(1), along_y(NY - 1), along_z(1), along_z(NZ - 1)]
    for to in partners:
        pl.semaphore_signal(barrier, inc=1, device_id=to, device_id_type=pl.DeviceIdType.MESH)

    img_ref[NX - 1, :, LAST:W] = jnp.zeros((ROWS, W - LAST), bf16)
    tag = lax.broadcasted_iota(jnp.int32, (TAG, ROWS), 0)
    for one in load_tags:
        one.wait()
    is_group = (tag < 96) & (tag % 32 == group_ref[...])
    is_offset = (tag >= 96) & (tag < 108) & (tag % 4 == offset_ref[...])
    tags = jnp.transpose(jnp.where(is_group | is_offset, 1.0, 0.0).astype(f32)).astype(bf16)
    for k in range(NX):
        img_ref[k, :, W:] = tags
    load_proj.wait()

    @pl.when(x < NX - 1)
    def _():
        load_rest.wait()

    @pl.when(x == NX - 1)
    def _():
        pbuf[0, WHOLE:] = jnp.zeros((PARTS - WHOLE, CHUNK, BLOCK), bf16)

    for k in range(NX):
        load_img(k).wait()
    img_ref[NX - 1, :, :LAST] = img_v[...]
    load_noise.start()
    load_prior.wait()

    pl.semaphore_wait(barrier, len(partners))

    def turned(m, low):
        return (m + 2 * low) % CHUNKS

    def to_across(m):
        mine = half * CHUNKS + turned(m, 1 - lo)
        src, dst = (pbuf.at[0, mine], pbuf.at[1, mine])
        if m >= CHUNKS:
            src, dst = (pbuf.at[2, mine], pbuf.at[3, mine])
        return copy(src, dst, ring_s.at[0], cross_r.at[m], across)

    def from_across(m):
        return pbuf.at[1 if m < CHUNKS else 3, half * CHUNKS + turned(m, lo)]

    def to_beside(m):
        dst = pbuf.at[2 if m < CHUNKS else 3, half * CHUNKS + turned(m, lo)]
        return copy(from_across(m), dst, ring_s.at[1], pair_r.at[m], beside)

    def from_beside(m):
        return pbuf.at[2 if m < CHUNKS else 3, half * CHUNKS + turned(m, 1 - lo)]

    def to_side(way, m):
        ref = from_across(m) if way == 0 else from_beside(m)
        up = 1 - 2 * (turned(m, lo if way == 0 else 1 - lo) // 2)
        to = device(y, (z + NZ + up) % NZ, x, c)
        return copy(ref, ref, ring_s.at[2 + way], side_r.at[way if m < CHUNKS else 2], to)

    def sided(slot):
        ref = pbuf.at[slot, pl.ds((1 - half) * CHUNKS, CHUNKS)]
        copy(ref, ref, ring_s.at[2], side_r.at[slot - 1], along_z(1)).wait_recv()

    def crossed(m):
        ref = from_across(m)
        copy(ref, ref, ring_s.at[0], cross_r.at[m], across).wait_recv()
        to_beside(m).start()
        to_side(0, m).start()

    def paired(m):
        ref = from_beside(m)
        copy(ref, ref, ring_s.at[1], pair_r.at[m], beside).wait_recv()
        if m < 2:
            to_across(CHUNKS + m).start()
        to_side(1, m).start()

    def image(p):
        return copy(
            img_ref.at[(x + STEPS[p]) % NX], xin.at[2 * p], img_s.at[0], img_r.at[2 * p],
            group(STEPS[p], 0),
        )

    def to_sibling(p):
        src = img_ref.at[x] if p == 0 else xin.at[2 * p]
        s = 2 * p + 1
        return copy(src, xin.at[s], img_s.at[1], img_r.at[s], group(0, 1))

    def tell(r):
        for n, at in ((0, along_y), (1, along_z)):
            pl.semaphore_signal(
                near_up.at[n, r - 1], inc=1, device_id=at(1), device_id_type=pl.DeviceIdType.MESH
            )
            if r <= 2:
                pl.semaphore_signal(
                    near_down.at[n, r - 1], inc=1, device_id=at(7),
                    device_id_type=pl.DeviceIdType.MESH,
                )

    def told(r):
        for n in (0, 1):
            pl.semaphore_wait(near_up.at[n, r - 1], 1)
            if r <= 2:
                pl.semaphore_wait(near_down.at[n, r - 1], 1)
        if r < 4:
            tell(r + 1)

    for m in range(CHUNKS):
        to_across(m).start()
    tell(1)
    for p in (1, 2, 3):
        image(p).start()
    to_sibling(0).start()

    xin[0] = img_ref[x]
    load_noise.wait()

    def pieces(inv, width):
        hi = inv.astype(bf16)
        rest = inv - hi.astype(f32)
        mid = rest.astype(bf16)
        low = (rest - mid.astype(f32)).astype(bf16)
        inv3[0:GROUPS, :width] = hi
        inv3[GROUPS : 2 * GROUPS, :width] = mid
        inv3[2 * GROUPS : 3 * GROUPS, :width] = low

    inv3[3 * GROUPS :] = jnp.zeros((TAG - 3 * GROUPS, W), bf16)

    @pl.when(x < NX - 1)
    def _():
        pieces(1.0 / noise_v[:, pl.ds(pl.multiple_of(x * W, 128), W)], W)

    @pl.when(x == NX - 1)
    def _():
        pieces(1.0 / noise_v[:, F - LAST :], LAST)
        inv3[: 3 * GROUPS, LAST:] = jnp.zeros((3 * GROUPS, W - LAST), bf16)

    row = lax.broadcasted_iota(jnp.int32, (TAG, BLOCK), 0)
    piece = jnp.where(row < 96, row // 32, jnp.minimum((row - 96) // 4, 3))

    def block_of(slot):
        return pbuf[slot].reshape(W, BLOCK)

    def columns(slot):
        p = block_of(slot).astype(f32)
        square = p * p
        s_hi = square.astype(bf16)
        s_lo = (square - s_hi.astype(f32)).astype(bf16)
        both = jnp.concatenate([s_hi, s_lo], axis=1)
        q = lax.dot_general(inv3[: 3 * GROUPS], both, NN, preferred_element_type=f32)
        q = q[0:32] + q[32:64] + q[64:96]
        q = q[:, :BLOCK] + q[:, BLOCK:]
        prior = jnp.zeros((TAG, BLOCK), f32)
        for o in range(CLASSES):
            log_prior = prior_ref[0, (h + turn[slot] + CLASSES - o) % CLASSES]
            prior = jnp.where(row % CLASSES == o, log_prior * (1.0 / NX), prior)
        value = jnp.where(row < 96, -0.5 * jnp.concatenate([q] * 4, axis=0), prior)
        v_hi = value.astype(bf16).astype(f32)
        v_mid = (value - v_hi).astype(bf16).astype(f32)
        v_lo = value - v_hi - v_mid
        both = jnp.where(piece == 2, v_lo, 0.0)
        both = jnp.where(piece == 1, v_mid, both)
        qbuf[slot] = jnp.where(piece == 0, v_hi, both).astype(bf16)

    def image_arrived(p):
        image(p).wait_recv()
        to_sibling(p).start()

    def score_copy(slot, s):
        return copy(
            sc_send.at[slot, s], sc_recv.at[slot, s], sc_s.at[slot], sc_r.at[slot],
            group((NX - STEPS[s // 2]) % NX, s % 2),
        )

    def score_part(n, s):
        rows = pl.ds(*PARTED[n])
        return copy(
            sc_send.at[3, s, rows], sc_recv.at[3, s, rows], sc_s.at[3 + n], sc_r.at[3 + n],
            group((NX - STEPS[s // 2]) % NX, s % 2),
        )

    def scores(slot, first, last):
        rows = (last - first) * ROWS
        part = lax.dot_general(
            white[first:last].reshape(rows, W), block_of(slot), NN, preferred_element_type=f32
        )
        part += lax.dot_general(
            xin[first:last, :, W:].reshape(rows, TAG), qbuf[slot], NN, preferred_element_type=f32
        )
        sc_send[slot, first:last] = part.reshape(last - first, ROWS, BLOCK)
        if slot == 3:
            for n in range(2):
                for s in (6, 7, 2, 4, 3, 5, 1):
                    score_part(n, s).start()
            return
        for s in (6, 7, 2, 4, 3, 5, 1):
            if first <= s < last:
                score_copy(slot, s).start()

    def whiten(s):
        inverse = jnp.dot(xin[s, :, W:], inv3[...], preferred_element_type=f32)
        white[s] = (xin[s, :, :W].astype(f32) * inverse).astype(bf16)

    whiten(0)
    columns(0)
    crossed(0)
    crossed(1)
    told(1)
    crossed(2)
    paired(0)
    crossed(3)
    told(2)
    image_arrived(1)
    image_arrived(2)
    paired(1)
    whiten(2)
    whiten(4)
    for s in (1, 3, 5):
        to_sibling(s // 2).wait_recv()
        whiten(s)
    paired(2)
    scores(0, 0, EARLY)
    crossed(4)
    paired(3)
    sided(1)
    crossed(5)
    columns(1)
    image_arrived(3)
    scores(1, 0, EARLY)
    whiten(6)
    paired(4)
    to_sibling(3).wait_recv()
    whiten(7)
    paired(5)
    scores(0, EARLY, 2 * NX)
    scores(1, EARLY, 2 * NX)
    told(3)
    sided(2)
    columns(2)
    scores(2, 0, 2 * NX)
    sided(3)
    told(4)
    columns(3)
    scores(3, 0, 2 * NX)

    def all_scores(slot, n=0):
        ref = sc_recv.at[slot, pl.ds(1, 2 * NX - 1)]
        if slot == 3:
            ref = sc_recv.at[slot, pl.ds(1, 2 * NX - 1), pl.ds(*PARTED[n])]
        return copy(ref, ref, sc_s.at[slot + n], sc_r.at[slot + n], group(1, 0))

    def post_copy(n, s):
        rows = pl.ds(*PARTED[n])
        return copy(
            post_send.at[s % 2, :, rows], post_recv.at[s, :, rows], post_s.at[n], post_r.at[n],
            group(STEPS[s // 2], s % 2),
        )

    def all_posts(n):
        ref = post_recv.at[pl.ds(1, 2 * NX - 1), :, pl.ds(*PARTED[n])]
        return copy(ref, ref, post_s.at[n], post_r.at[n], group(1, 0))

    for slot in range(3):
        all_scores(slot).wait_recv()
    evidences = []
    for n in range(2):
        first, rows = PARTED[n]
        here = slice(first, first + rows)
        all_scores(3, n).wait_recv()
        total = {}
        for slot in range(4):
            for dc in (0, 1):
                terms = [sc_send[slot, 0, here]] if dc == 0 else [sc_recv[slot, 1, here]]
                terms += [sc_recv[slot, 2 * dx + dc, here] for dx in range(1, NX)]
                total[slot, dc] = (terms[0] + terms[1]) + (terms[2] + terms[3])
        peak = None
        for value in total.values():
            peak = value if peak is None else jnp.maximum(peak, value)
        peak = jnp.max(peak, axis=1, keepdims=True)
        mass = None
        for value in total.values():
            term = jnp.exp(value - peak)
            mass = term if mass is None else mass + term
        evidence = peak + jnp.log(jnp.sum(mass, axis=1, keepdims=True))
        evidences.append(evidence)
        for (slot, dc), value in total.items():
            post_send[dc, slot, here] = jnp.exp(value - evidence).astype(bf16)
        for s in (6, 7, 2, 4, 3, 5, 1):
            post_copy(n, s).start()

    evidence = jnp.broadcast_to(jnp.concatenate(evidences, axis=0), (ROWS, TAG))
    ev_ref[...] = jnp.transpose(evidence)[0:1, :]
    store_ev = pltpu.make_async_copy(ev_ref, ev_hbm, load.at[4])
    store_ev.start()
    post_recv[0] = post_send[0]
    for n in range(2):
        all_posts(n).wait_recv()

    for slot in range(4):
        wt[BLOCK * slot : BLOCK * (slot + 1)] = jnp.transpose(post_recv[:, slot].reshape(ALL, BLOCK))

    place = {"z": z, "y": y}
    other = {"z": "y", "y": "z"}

    def along(axis, d):
        at = (place[axis] + d + 8) % 8
        return device(y, at, x, c) if axis == "z" else device(at, z, x, c)

    def near(axis, side):
        return along(axis, side * (1 - 2 * (place[axis] % 2)))

    def stage1(i):
        axis, side = STREAMS[i][:2]
        return copy(
            parts[i].at[1 - place[axis] % 2], in1[i], st_s.at[0, i], st_r.at[0, i], near(axis, side)
        )

    def stage2(i):
        axis, side = STREAMS[i][:2]
        return copy(
            mid1[i].at[1 - place[other[axis]] % 2], in2[i], st_s.at[1, i], st_r.at[1, i],
            near(other[axis], side),
        )

    def stage3(i, d):
        axis = STREAMS[i][0]
        return copy(
            mid2[i].at[(place[axis] // 2 + d) % 4], in3[i].at[d - 1], st_s.at[2, i],
            st_r.at[2, i], along(axis, 2 * d),
        )

    def all3(i):
        return copy(in3[i], in3[i], st_s.at[2, i], st_r.at[2, i], along("z", 2))

    def last(axis, d, e):
        n = "zy".index(axis)
        at = (place[other[axis]] + 2 * d) % 8
        to = device(at, z, (x + e) % NX, c) if axis == "z" else device(y, at, (x + e) % NX, c)
        return copy(
            own[n].at[(place[other[axis]] // 2 + d) % 4, (x + e) % NX], got[n].at[d, x],
            own_s.at[n, d], own_r.at[n, d], to,
        )

    def self_copy(n, axis):
        return pltpu.make_async_copy(
            own[n].at[place[other[axis]] // 2, x], got[n].at[0, x], own_r.at[n, 0]
        )

    def last_in(n, d):
        return copy(got[n].at[d], got[n].at[d], own_s.at[n, d], own_r.at[n, d], group(1, 0))

    order = range(len(STREAMS))
    for i in order:
        axis, _, col, width = STREAMS[i]
        part = jnp.dot(
            wt[...], white[:, :, col : col + width].reshape(ALL, width), preferred_element_type=f32
        ).astype(bf16)
        for slot in range(4):
            y_half = (h + turn[slot]) % 4
            for r in range(2 * NZ):
                low, z_ = r // NZ, r % NZ
                at = BLOCK * slot + OWN * r
                if axis == "z":
                    parts[i][z_ % 2, low, z_ // 2, y_half] = part[at : at + OWN]
                else:
                    parts[i][low, z_ % 2, y_half, z_ // 2] = part[at : at + OWN]
        stage1(i).start()
    for i in order:
        axis = STREAMS[i][0]
        stage1(i).wait_recv()
        total = parts[i][place[axis] % 2].astype(f32) + in1[i][...].astype(f32)
        mid1[i][...] = total.astype(bf16)
        stage2(i).start()
    for i in order:
        axis = STREAMS[i][0]
        stage2(i).wait_recv()
        total = mid1[i][place[other[axis]] % 2].astype(f32) + in2[i][...].astype(f32)
        mid2[i][...] = total.astype(bf16)
        for d in (2, 1, 3):
            stage3(i, d).start()
    far_first = [(d, e) for d in (2, 1, 3, 0) for e in (2, 1, 3, 0) if d or e]
    for i in order:
        axis, _, col, width = STREAMS[i]
        n = "zy".index(axis)
        col -= WA * n
        acc = mid2[i][place[axis] // 2].astype(f32)
        all3(i).wait_recv()
        for d in (1, 3, 2):
            acc += in3[i][d - 1].astype(f32)
        for k in range(NX):
            own[n][:, k, :, col : col + width] = acc[:, 2 * k : 2 * k + 2].astype(bf16)
        if all(t[0] != axis for t in STREAMS[i + 1 :]):
            for d, e in far_first:
                last(axis, d, e).start()
            self_copy(n, axis).start()

    def store_out(n):
        lanes = pl.ds(WA * n, (WA, WB)[n])
        return pltpu.make_async_copy(
            out_ref.at[:, :, lanes], out_hbm.at[:, :, lanes], load.at[5 + n]
        )

    for axis in "zy":
        n = "zy".index(axis)
        for d in (0, 1, 3, 2):
            last_in(n, d).wait_recv()
        acc = got[n][0].astype(f32)
        for d in range(1, 4):
            acc += got[n][d].astype(f32)
        out_ref[:, :, WA * n : WA * n + (WA, WB)[n]] = acc
        store_out(n).start()

    def sent(ref, sem):
        copy(ref, ref, sem, cross_r.at[0], across).wait_send()

    for n in range(4):
        sent(pbuf.at[n, pl.ds(0, 6)], ring_s.at[n])
    sent(xin.at[pl.ds(0, NX - 1)], img_s.at[0])
    sent(xin.at[pl.ds(0, NX)], img_s.at[1])
    for slot in range(3):
        all_scores(slot).wait_send()
    for n in range(2):
        all_scores(3, n).wait_send()
        all_posts(n).wait_send()
    for i in order:
        stage1(i).wait_send()
        stage2(i).wait_send()
        all3(i).wait_send()
    for n in range(2):
        sent(own[n].at[0, pl.ds(0, NX - 1)], own_s.at[n, 0])
        for d in (1, 2, 3):
            sent(own[n].at[d], own_s.at[n, d])
    store_ev.wait()
    store_out(0).wait()
    store_out(1).wait()


def body(images, projections, noise_power, class_logprior, groups, offsets):
    dma = pltpu.SemaphoreType.DMA
    anywhere = pl.BlockSpec(memory_space=pl.ANY)
    out, evidence = pl.pallas_call(
        kernel,
        out_shape=(
            jax.ShapeDtypeStruct((NX, 2, W), f32),
            jax.ShapeDtypeStruct((1, ROWS), f32),
        ),
        in_specs=[anywhere] * 6,
        out_specs=(anywhere, anywhere),
        scratch_shapes=[
            pltpu.SMEM((1, CLASSES), f32),
            pltpu.VMEM((1, ROWS), jnp.int32),
            pltpu.VMEM((1, ROWS), jnp.int32),
            pltpu.VMEM((NX, 2, W), f32),
            pltpu.VMEM((1, ROWS), f32),
            pltpu.VMEM((ROWS, LAST), bf16),
            pltpu.VMEM((GROUPS, F), f32),
            pltpu.VMEM((NX, ROWS, W + TAG), bf16),
            pltpu.VMEM((2 * NX, ROWS, W + TAG), bf16),
            pltpu.VMEM((2 * NX, ROWS, W), bf16),
            pltpu.VMEM((TAG, W), bf16),
            pltpu.VMEM((4, PARTS, CHUNK, BLOCK), bf16),
            pltpu.VMEM((4, TAG, BLOCK), bf16),
            pltpu.VMEM((4, 2 * NX, ROWS, BLOCK), f32),
            pltpu.VMEM((4, 2 * NX, ROWS, BLOCK), f32),
            pltpu.VMEM((2, 4, ROWS, BLOCK), bf16),
            pltpu.VMEM((2 * NX, 4, ROWS, BLOCK), bf16),
            pltpu.VMEM((4 * BLOCK, ALL), bf16),
            [pltpu.VMEM((2, 2, 4, 4, OWN, t[3]), bf16) for t in STREAMS],
            [pltpu.VMEM((2, 4, 4, OWN, t[3]), bf16) for t in STREAMS],
            [pltpu.VMEM((2, 4, 4, OWN, t[3]), bf16) for t in STREAMS],
            [pltpu.VMEM((4, 4, OWN, t[3]), bf16) for t in STREAMS],
            [pltpu.VMEM((4, 4, OWN, t[3]), bf16) for t in STREAMS],
            [pltpu.VMEM((3, 4, OWN, t[3]), bf16) for t in STREAMS],
            [pltpu.VMEM((4, NX, 2, t), bf16) for t in (WA, WB)],
            [pltpu.VMEM((4, NX, 2, t), bf16) for t in (WA, WB)],
            pltpu.SemaphoreType.REGULAR((2, 4)),
            pltpu.SemaphoreType.REGULAR((2, 2)),
            dma((10 + NX,)),
            dma((2,)), dma((2 * NX,)),
            dma((4,)), dma((6,)), dma((6,)), dma((3,)),
            dma((5,)), dma((5,)),
            dma((2,)), dma((2,)),
            dma((3, len(STREAMS))), dma((3, len(STREAMS))),
            dma((2, 4)), dma((2, 4)),
        ],
        compiler_params=pltpu.CompilerParams(
            collective_id=0, has_side_effects=True, vmem_limit_bytes=58 * 1024 * 1024
        ),
        name="estep",
    )(
        images, projections.T.reshape(F // CHUNK, CHUNK, BLOCK), noise_power, class_logprior.reshape(1, CLASSES),
        groups.reshape(1, ROWS), offsets.reshape(1, ROWS),
    )
    out, evidence = pl.pallas_call(
        finish,
        out_shape=(
            jax.ShapeDtypeStruct((2, F), f32),
            jax.ShapeDtypeStruct((1, ROWS), f32),
        ),
        in_specs=[anywhere, anywhere],
        out_specs=(anywhere, anywhere),
        scratch_shapes=[
            pltpu.VMEM((NX, 2, W), f32),
            pltpu.VMEM((1, ROWS), f32),
            pltpu.VMEM((2, F), f32),
            dma((4,)),
        ],
        name="finish",
    )(out, evidence)
    return (out, evidence.reshape(ROWS))


def solution(mesh):
    in_specs = (
        P(("cls", "img"), None),
        P("cls", None),
        P(),
        P(),
        P(("cls", "img")),
        P(("cls", "img")),
    )
    out_specs = (P(("cls", "img"), None), P(("cls", "img")))
    return jax.shard_map(body, mesh=mesh, in_specs=in_specs, out_specs=out_specs, check_vma=False)
```
